32 devices in a mesh: batch: 1 (over z), col: 4 (over y), row: 8 (over x, core).
Axes of the slice: x: 4, y: 4, z: 1, core: 2. Of those that a mesh axis runs over, the one named last changes fastest.
The devices are a block of a 4x4x8 slice.
Arguments:
- lower_cyc: float32 [2048, 2048], P(('batch', 'row'), 'col')
Outputs:
- output: float32 [2048, 2048], P(('batch', 'row'), 'col')
All inputs are finite; a program needn't handle non-finite values.
Results may differ from the reference program's by a relative error of at most 0.001.
Values sent between devices are 32-bit elements.
A program may use at most 768 MiB of HBM per device.

```python
import jax
import jax.numpy as jnp
from jax import lax

N = 2048
DEPTH = 3
BLK = 8
PX = 8
PY = 4


def to_cyclic(matrix):
    blocks6 = matrix.reshape(N // (PX * BLK), PX, BLK, N // (PY * BLK), PY, BLK)
    return blocks6.transpose(1, 0, 2, 4, 3, 5).reshape(N, N)


def to_natural(cyclic):
    blocks6 = cyclic.reshape(PX, N // (PX * BLK), BLK, PY, N // (PY * BLK), BLK)
    return blocks6.transpose(1, 0, 2, 4, 3, 5).reshape(N, N)


def setup_inputs(seed: int = 0, part: int = 0) -> dict:
    base_key = jax.random.fold_in(jax.random.key(seed), part)
    key_diag, key_low = jax.random.split(base_key)
    diag_vals = jax.random.uniform(key_diag, (N,), jnp.float32, 2.0, 4.0)
    low_vals = jax.random.normal(key_low, (N, N), jnp.float32) * (2.0 / N ** 0.5)
    row_ids = jnp.arange(N)[:, None]
    col_ids = jnp.arange(N)[None, :]
    natural = jnp.where(row_ids > col_ids, low_vals, 0.0) + jnp.where(row_ids == col_ids, diag_vals[:, None], 0.0)
    return {"lower_cyc": to_cyclic(natural)}


def highest_dot(left, right):
    return jnp.dot(left, right, precision=lax.Precision.HIGHEST, preferred_element_type=jnp.float32)


def invert_block(mat_block, levels_left):
    block_size = mat_block.shape[0]
    if levels_left == 0:
        identity = jnp.eye(block_size, dtype=jnp.float32)
        return lax.linalg.triangular_solve(mat_block, identity, left_side=True, lower=True)
    half_size = block_size // 2
    inv_upper = invert_block(mat_block[:half_size, :half_size], levels_left - 1)
    inv_lower = invert_block(mat_block[half_size:, half_size:], levels_left - 1)
    temp_prod = highest_dot(mat_block[half_size:, :half_size], inv_upper)
    off_diag = -highest_dot(inv_lower, temp_prod)
    zero_block = jnp.zeros((half_size, half_size), jnp.float32)
    upper_rows = jnp.concatenate([inv_upper, zero_block], axis=1)
    lower_rows = jnp.concatenate([off_diag, inv_lower], axis=1)
    return jnp.concatenate([upper_rows, lower_rows], axis=0)


def reference(lower_cyc):
    return to_cyclic(invert_block(to_natural(lower_cyc), DEPTH))
```

```python
import functools

import jax
import jax.numpy as jnp
from jax import lax
from jax.experimental import pallas as pl
from jax.experimental.pallas import tpu as pltpu
from jax.sharding import PartitionSpec as P

BLK = 8
CORES = 2
LANES = 128
MESH = pl.DeviceIdType.MESH
F32 = jnp.float32


def dot(left, right):
    return jnp.dot(left, right, precision=lax.Precision.HIGHEST, preferred_element_type=F32)


def iota(shape, dim):
    return lax.broadcasted_iota(jnp.int32, shape, dim)


def halves(tiles, half):
    low = iota(tiles[0].shape, 1) < LANES // 2
    out = []
    for first, second in ((tiles[0], tiles[1]), (tiles[2], tiles[3])):
        if half == 0:
            out.append(jnp.where(low, first, pltpu.roll(second, LANES // 2, 1)))
        else:
            out.append(jnp.where(low, pltpu.roll(first, LANES // 2, 1), second))
    return jnp.concatenate(out, axis=1)


class Net:
    def __init__(self, send, recv):
        self.send, self.recv, self.used, self.all = send, recv, 0, []

    def copy(self, src, dst, device):
        slot = self.used
        self.used += 1
        made = pltpu.make_async_remote_copy(
            src_ref=src, dst_ref=dst, send_sem=self.send.at[slot], recv_sem=self.recv.at[slot],
            device_id=device, device_id_type=MESH)
        return made

    def start(self, src, dst, device):
        made = self.copy(src, dst, device)
        made.start()
        self.all.append(made)
        return made


def kernel(rows, cols, l_ref, o_ref, U, G, C0, LF, PK, LI, W, ZM, ZS, TG, send, recv):
    chips = rows // CORES
    row = lax.axis_index("row")
    y = lax.axis_index("col")
    x, core = row // CORES, row % CORES
    spot, hh = row % cols, row // cols
    net = Net(send, recv)

    def at(xx, cc, yy):
        return {"row": xx * CORES + cc, "col": yy}

    def xs(step):
        return lax.rem(x + step + chips, chips)

    def ys(step):
        return lax.rem(y + step + cols, cols)

    partner = at(x, 1 - core, y)
    barrier = pltpu.get_barrier_semaphore()
    peers = [partner] + [at(xs(d), core, y) for d in range(1, chips)] + [at(x, core, ys(d)) for d in range(1, cols)]
    for peer in peers:
        pl.semaphore_signal(barrier, inc=1, device_id=peer, device_id_type=MESH)

    for part in range(2):
        piece = l_ref[part * 128:(part + 1) * 128, part * 256:(part + 1) * 256]
        low = iota((32, LANES), 1) < LANES // 2
        packed = [jnp.where(low, piece[64 * m:64 * m + 32, LANES * m:LANES * (m + 1)],
                            piece[64 * m + 32:64 * m + 64, LANES * m:LANES * (m + 1)]) for m in range(2)]
        packed.append(jnp.where(low, piece[32:64, :LANES], pltpu.roll(piece[96:128, LANES:], LANES // 2, 1)))
        packed += [piece[64:96, :LANES], piece[96:128, :LANES]]

        @pl.when(core == part)
        def _():
            for g in range(5):
                G[y, g, spot, :, hh] = packed[g].reshape(4, BLK, LANES)

        @pl.when(core != part)
        def _():
            for g in range(5):
                U[g] = packed[g].reshape(4, BLK, LANES)

    C0[y] = l_ref[128:256, 0:256]
    pl.semaphore_wait(barrier, len(peers))

    swap = net.start(U, G.at[y, :, spot, :, hh], partner)
    swap.wait_recv()

    def chip_piece(yy, g, xx, ysel=None):
        return G.at[yy if ysel is None else ysel, g, pl.ds(2 * (xx % 2), 2), :, xx // 2]

    axis_first = ["x", "y", "y", "x", "y"]
    first = []
    for g in range(5):
        mine = chip_piece(y, g, x)
        if axis_first[g] == "x":
            first.append([net.start(mine, mine, at(xs(d), core, y)) for d in range(1, chips)])
        else:
            first.append([net.start(mine, mine, at(x, core, ys(d))) for d in range(1, cols)])
    c0_src = l_ref.at[pl.ds(128, 128), pl.ds(0, 256)]

    def bundle(g, step, part=None):
        if axis_first[g] == "x":
            return G.at[ys(step), g] if part is None else G.at[ys(step), g, pl.ds(2 * part, 2)]
        sel = slice(None) if part is None else pl.ds(2 * part, 2)
        return chip_piece(None, g, xs(step), sel)

    def along(g, step):
        return at(x, core, ys(step)) if axis_first[g] == "x" else at(xs(step), core, y)

    second = {}

    def send_second(g):
        for made in first[g]:
            made.wait_recv()
        second[g] = [net.start(bundle(g, 0), bundle(g, 0), along(g, 1)),
                     net.start(bundle(g, 0), bundle(g, 0), along(g, -1))]

    def relay(g):
        up, down = second[g]
        up.wait_recv()
        far_up = net.start(bundle(g, -1, 0), bundle(g, -1, 0), along(g, 1))
        down.wait_recv()
        far_down = net.start(bundle(g, 1, 1), bundle(g, 1, 1), along(g, -1))
        second[g] = [far_up, far_down]

    def arrive(g):
        for made in second[g]:
            made.wait_recv()

    for g in range(5):
        send_second(g)
    c0_copies = [net.start(c0_src, C0.at[y], at(x, core, ys(d))) for d in range(1, cols)]
    for g in range(2):
        relay(g)
    for g in range(2):
        arrive(g)

    lane = iota((BLK, LANES), 1)
    sub = iota((BLK, LANES), 0)
    block_of = (lane // BLK) % BLK
    diag = [[[None] * 4 for _ in range(4)] for _ in range(2)]
    inv = [[[None] * 4 for _ in range(4)] for _ in range(2)]
    for m in range(2):
        for c in range(4):
            for k in range(c + 1):
                total = jnp.zeros((BLK, LANES), F32)
                for b in range(8):
                    total = jnp.where(block_of == b, G[k, m, c, b // 2, b % 2], total)
                diag[m][c][k] = total
                inv[m][c][k] = jnp.where(sub == lane % BLK, 1.0, 0.0) if c == k else jnp.zeros((BLK, LANES), F32)
    for t in range(32):
        ct, jt = t // BLK, t % BLK
        index = (lane // BLK) * BLK + jt
        for m in range(2):
            spread = [jnp.take_along_axis(diag[m][c][ct], index, axis=1) for c in range(ct, 4)]
            pivot = 1.0 / spread[0][jt:jt + 1, :]
            below = jnp.where(sub > jt, spread[0], 0.0)
            for k in range(ct + 1):
                solved = inv[m][ct][k][jt:jt + 1, :] * pivot
                inv[m][ct][k] = jnp.where(sub == jt, solved, inv[m][ct][k] - below * solved)
                for c in range(ct + 1, 4):
                    inv[m][c][k] = inv[m][c][k] - spread[c - ct] * solved
    for m in range(2):
        for c in range(4):
            tiles = [inv[m][c][k] if k <= c else jnp.zeros((BLK, LANES), F32) for k in range(4)]
            for e in range(2):
                PK[2 * m + e, c] = halves(tiles, e)
    wide_block = (iota((BLK, 2 * LANES), 1) % 64) // BLK

    @pl.loop(0, 2)
    def _(m):
        tiles = [G[k, m].reshape(256, LANES) for k in range(4)]
        for e in range(2):
            LF[2 * m + e] = halves(tiles, e).reshape(32, BLK, 256)

    def keep(mask, tile):
        return jnp.where(mask, tile, 0.0)

    def double(leaf, nb):
        group = wide_block // nb
        packed = [PK[leaf, i] for i in range(4 * nb)]
        spread = jnp.concatenate([keep(group == b // nb, packed[(b % nb) * 4 + c]) for c in range(4) for b in range(8)], axis=0)
        coupling = []
        for bb in range(nb):
            for c in range(4):
                total = None
                for s in range(1, 8 // nb, 2):
                    tile = LF[leaf, c * 8 + s * nb + bb]
                    total = keep(group == s - 1, tile if total is None else tile) if total is None else jnp.where(group == s - 1, tile, total)
                coupling.append(total)
        temp = dot(jnp.concatenate(coupling, axis=0), spread)
        zero = jnp.zeros((BLK, 256), F32)
        temp_spread = jnp.concatenate(
            [keep(group == b // nb - 1, temp[((b % nb) * 4 + c) * BLK:((b % nb) * 4 + c + 1) * BLK]) if (b // nb) % 2 else zero
             for c in range(4) for b in range(8)], axis=0)
        corner = dot(jnp.concatenate(packed, axis=0), temp_spread)
        for half in range(2):
            for i in range(4 * nb):
                tile = keep(group % 2 == half, packed[i])
                if half:
                    tile = tile - corner[i * BLK:(i + 1) * BLK]
                if nb < 4:
                    PK[leaf, half * 4 * nb + i] = tile
                else:
                    bb, c = i // 4, i % 4
                    LI[leaf, c * 8 + half * 4 + bb] = tile

    for step, nb in enumerate((1, 2, 4)):
        @pl.loop(0, 2)
        def _(m):
            for e in range(2):
                double(2 * m + e, nb)
        relay(2 + step)

    def leaf_inv(i):
        return LI[i].reshape(256, 256)

    for g in range(2, 5):
        arrive(g)

    def coupling2(m):
        return halves([G[k, 2].reshape(256, LANES) for k in range(4)], m)

    def coupling1(g):
        return jnp.concatenate([G[k, g].reshape(256, LANES) for k in range(4)], axis=1)

    def pick(i):
        r, l = iota((256, 256), 0), iota((256, 256), 1)
        return jnp.where((r // 64 == y) & (l // 64 == i) & (r % 64 == l % 64), 1.0, 0.0)

    send_w = net.copy(W, W, partner)
    send_z = net.copy(ZS, ZM, partner)

    @pl.when(core == 0)
    def _():
        def put(i, val):
            W[i // 2, :, i % 2] = val.reshape(4, 4, 2, BLK, 256)
            return val

        w0 = put(0, dot(leaf_inv(0), pick(0)))
        w1 = put(1, dot(leaf_inv(1), pick(1) - dot(coupling2(0), w0)))
        pair = W[0].reshape(512, 256)
        s2 = pick(2) - dot(coupling1(3), pair)
        s3 = pick(3) - dot(coupling1(4), pair)
        w2 = put(2, dot(leaf_inv(2), s2))
        put(3, dot(leaf_inv(3), s3 - dot(coupling2(1), w2)))
        send_w.start()

    @pl.when(core == 1)
    def _():
        def mine(i):
            r, l = iota((256, 256), 0), iota((256, 256), 1)
            own = CORES * x + r // 128
            return jnp.where(((r // 32) % 4 == i) & (l // 64 == own % cols) & ((l % 64) // BLK == 2 * ((r // BLK) % 4) + own // cols)
                             & (r % BLK == l % BLK), 1.0, 0.0)

        def put(i, val):
            ZS[i] = val[:128]
            ZM[i] = val[128:]
            return val

        z3 = put(3, dot(mine(3), leaf_inv(3)))
        z2 = put(2, dot(mine(2) - dot(z3, coupling2(1)), leaf_inv(2)))
        both = dot(z2, coupling1(3)) + dot(z3, coupling1(4))
        tiles = [both[:, LANES * k:LANES * (k + 1)] for k in range(4)]
        z1 = put(1, dot(mine(1) - halves(tiles, 1), leaf_inv(1)))
        put(0, dot(mine(0) - halves(tiles, 0) - dot(z1, coupling2(0)), leaf_inv(0)))
        send_z.start()

    for made in c0_copies:
        made.wait_recv()

    @pl.when(core == 0)
    def _():
        send_z.wait_recv()

    @pl.when(core == 1)
    def _():
        send_w.wait_recv()

    left = jnp.concatenate([C0[k, :, LANES * n:LANES * (n + 1)] for n in range(2) for k in range(4)], axis=1)
    TG[:, spot, :, hh] = dot(left, W[...].reshape(1024, 256)).reshape(4, 4, BLK, 256)

    def t_piece(xx, cc):
        own = CORES * xx + cc
        return TG.at[:, own % cols, :, own // cols]

    t_out = [net.start(t_piece(x, core), t_piece(x, core), at(xs(d), core, y)) for d in range(1, chips)]
    t_in = [net.start(t_piece(x, core), t_piece(x, core), partner)]

    o_ref[0:128, 256:512] = jnp.zeros((128, 256), F32)
    for i in range(4):
        o_ref[32 * i:32 * (i + 1), 0:256] = W[i // 2, spot, i % 2, :, hh].reshape(32, 256)
    o_ref[128:256, 256:512] = sum(dot(ZM[i], pick(i)) for i in range(4))

    for d, made in enumerate(t_out):
        made.wait_recv()
        there = t_piece(xs(-(d + 1)), core)
        t_in.append(net.start(there, there, partner))
    for made in t_in:
        made.wait_recv()
    o_ref[128:256, 0:256] = -sum(dot(ZM[i], TG[i].reshape(256, 256)) for i in range(4))

    for made in net.all:
        made.wait_send()

    @pl.when(core == 0)
    def _():
        send_w.wait_send()

    @pl.when(core == 1)
    def _():
        send_z.wait_send()


def solution(mesh):
    rows, cols = mesh.shape["row"], mesh.shape["col"]
    block_spec = P(("batch", "row"), "col")

    def device_body(local_l):
        vmem = functools.partial(pltpu.VMEM, dtype=F32)
        slots = 64
        return pl.pallas_call(
            functools.partial(kernel, rows, cols),
            out_shape=jax.ShapeDtypeStruct(local_l.shape, F32),
            in_specs=[pl.BlockSpec(memory_space=pltpu.VMEM)],
            out_specs=pl.BlockSpec(memory_space=pltpu.VMEM),
            scratch_shapes=[
                vmem((5, 4, BLK, LANES)),
                vmem((4, 5, 4, 4, 2, BLK, LANES)),
                vmem((4, 128, 256)),
                vmem((4, 32, BLK, 256)),
                vmem((4, 16, BLK, 256)),
                vmem((4, 32, BLK, 256)),
                vmem((2, 4, 2, 4, 2, BLK, 256)),
                vmem((4, 128, 256)),
                vmem((4, 128, 256)),
                vmem((4, 4, 4, 2, BLK, 256)),
                pltpu.SemaphoreType.DMA((slots,)),
                pltpu.SemaphoreType.DMA((slots,)),
            ],
            compiler_params=pltpu.CompilerParams(collective_id=0, has_side_effects=True),
        )(local_l)

    return jax.shard_map(device_body, mesh=mesh, in_specs=(block_spec,), out_specs=block_spec, check_vma=False)
```

```python
import functools

import jax
import jax.numpy as jnp
from jax import lax
from jax.experimental import pallas as pl
from jax.experimental.pallas import tpu as pltpu
from jax.sharding import PartitionSpec as P

BLK = 8
CORES = 2
LANES = 128
MESH = pl.DeviceIdType.MESH


class Marks:
    def __init__(self):
        self.scope = None

    def __call__(self, name=None):
        if self.scope is not None:
            self.scope.__exit__(None, None, None)
        self.scope = None if name is None else jax.named_scope(name)
        if name is not None:
            self.scope.__enter__()
F32 = jnp.float32


def dot(left, right):
    return jnp.dot(left, right, precision=lax.Precision.HIGHEST, preferred_element_type=F32)


def iota(shape, dim):
    return lax.broadcasted_iota(jnp.int32, shape, dim)


def halves(tiles, half):
    low = iota(tiles[0].shape, 1) < LANES // 2
    out = []
    for first, second in ((tiles[0], tiles[1]), (tiles[2], tiles[3])):
        if half == 0:
            out.append(jnp.where(low, first, pltpu.roll(second, LANES // 2, 1)))
        else:
            out.append(jnp.where(low, pltpu.roll(first, LANES // 2, 1), second))
    return jnp.concatenate(out, axis=1)


class Net:
    def __init__(self, send, recv):
        self.send, self.recv, self.used, self.all = send, recv, 0, []

    def copy(self, src, dst, device):
        slot = self.used
        self.used += 1
        made = pltpu.make_async_remote_copy(
            src_ref=src, dst_ref=dst, send_sem=self.send.at[slot], recv_sem=self.recv.at[slot],
            device_id=device, device_id_type=MESH)
        return made

    def start(self, src, dst, device):
        made = self.copy(src, dst, device)
        made.start()
        self.all.append(made)
        return made


def kernel(rows, cols, hbm_ref, o_ref, l_ref, U, G, C0, LF, PK, LI, W, ZM, ZS, TG, load, send, recv):
    chips = rows // CORES
    row = lax.axis_index("row")
    y = lax.axis_index("col")
    x, core = row // CORES, row % CORES
    spot, hh = row % cols, row // cols
    net = Net(send, recv)

    def at(xx, cc, yy):
        return {"row": xx * CORES + cc, "col": yy}

    def xs(step):
        return lax.rem(x + step + chips, chips)

    def ys(step):
        return lax.rem(y + step + cols, cols)

    windows = [(pl.ds(0, 128), pl.ds(0, 256)), (pl.ds(128, 128), pl.ds(256, 256)), (pl.ds(128, 128), pl.ds(0, 256))]
    loads = [pltpu.make_async_copy(hbm_ref.at[w], l_ref.at[w], load.at[i]) for i, w in enumerate(windows)]
    for made in loads:
        made.start()
    mark = Marks()
    mark("a_signal")
    partner = at(x, 1 - core, y)
    barrier = pltpu.get_barrier_semaphore()
    peers = [partner] + [at(xs(d), core, y) for d in range(1, chips)] + [at(x, core, ys(d)) for d in range(1, cols)]
    for peer in peers:
        pl.semaphore_signal(barrier, inc=1, device_id=peer, device_id_type=MESH)

    mark("a_pack")
    for part in range(2):
        loads[part].wait()
        piece = l_ref[part * 128:(part + 1) * 128, part * 256:(part + 1) * 256]
        low = iota((32, LANES), 1) < LANES // 2
        packed = [jnp.where(low, piece[64 * m:64 * m + 32, LANES * m:LANES * (m + 1)],
                            piece[64 * m + 32:64 * m + 64, LANES * m:LANES * (m + 1)]) for m in range(2)]
        packed.append(jnp.where(low, piece[32:64, :LANES], pltpu.roll(piece[96:128, LANES:], LANES // 2, 1)))
        packed += [piece[64:96, :LANES], piece[96:128, :LANES]]

        @pl.when(core == part)
        def _():
            for g in range(5):
                G[y, g, spot, :, hh] = packed[g].reshape(4, BLK, LANES)

        @pl.when(core != part)
        def _():
            for g in range(5):
                U[g] = packed[g].reshape(4, BLK, LANES)

    loads[2].wait()
    C0[y] = l_ref[128:256, 0:256]
    mark("b_barrier")
    pl.semaphore_wait(barrier, len(peers))

    mark("c_swap")
    swap = net.start(U, G.at[y, :, spot, :, hh], partner)
    swap.wait_recv()

    axis_first = ["x", "y", "y", "x", "y"]

    def source(g, f, s, k=None):
        xx, yy = (xs(f), ys(s)) if axis_first[g] == "x" else (xs(s), ys(f))
        return G.at[yy, g, pl.ds(2 * (xx % 2), 2) if k is None else 2 * (xx % 2) + k, :, xx // 2]

    def toward(g, f, s):
        return at(xs(f), core, ys(s)) if axis_first[g] == "x" else at(xs(s), core, ys(f))

    got = {}

    def first_axis(g, f, k=None):
        if f:
            got[g, f, 0, k].wait_recv()
        if f in (-1, 1):
            half = 0 if f < 0 else 1
            got[g, 2, 0, half] = net.start(source(g, f, 0, half), source(g, f, 0, half), toward(g, -f, 0))
        for s in (1, -1):
            got[g, f, -s, k] = net.start(source(g, f, 0, k), source(g, f, 0, k), toward(g, 0, s))

    def second_axis(g, f, s, k=None):
        got[g, f, s, k].wait_recv()
        half = 0 if s < 0 else 1
        if k is None or k == half:
            got[g, f, 2, half] = net.start(source(g, f, s, half), source(g, f, s, half), toward(g, 0, -s))

    mark("d_own")
    both = range(2)
    for g in both:
        for f in (1, -1):
            got[g, -f, 0, None] = net.start(source(g, 0, 0), source(g, 0, 0), toward(g, f, 0))
    for g in both:
        first_axis(g, 0)
    first = {}
    for g in range(2, 5):
        first[g] = [net.start(source(g, 0, 0), source(g, 0, 0), toward(g, d, 0)) for d in range(1, 4)]
    mark("e_near1")
    for f in (-1, 1):
        for g in both:
            first_axis(g, f)
    mark("f_near2")
    for s in (-1, 1):
        for g in both:
            second_axis(g, 0, s)
    mark("g_far1")
    for k in range(2):
        for g in both:
            first_axis(g, 2, k)
    mark("h_diag")
    for f in (-1, 1):
        for s in (-1, 1):
            for g in both:
                second_axis(g, f, s)
    mark("i_far2")
    for k in range(2):
        for s in (-1, 1):
            for g in both:
                second_axis(g, 2, s, k)

    def bundle(g, step, part=None):
        if axis_first[g] == "x":
            return G.at[ys(step), g] if part is None else G.at[ys(step), g, pl.ds(2 * part, 2)]
        xx = xs(step)
        return G.at[slice(None) if part is None else pl.ds(2 * part, 2), g, pl.ds(2 * (xx % 2), 2), :, xx // 2]

    second = {}

    def send_second(g):
        for made in first[g]:
            made.wait_recv()
        second[g] = [net.start(bundle(g, 0), bundle(g, 0), toward(g, 0, 1)),
                     net.start(bundle(g, 0), bundle(g, 0), toward(g, 0, -1))]

    def relay(g):
        up, down = second[g]
        up.wait_recv()
        far_up = net.start(bundle(g, -1, 0), bundle(g, -1, 0), toward(g, 0, 1))
        down.wait_recv()
        far_down = net.start(bundle(g, 1, 1), bundle(g, 1, 1), toward(g, 0, -1))
        second[g] = [far_up, far_down]

    def arrive(g):
        for made in second[g]:
            made.wait_recv()

    mark("j_second")
    for g in range(2, 5):
        send_second(g)
    c0_src = l_ref.at[pl.ds(128, 128), pl.ds(0, 256)]
    c0_copies = [net.start(c0_src, C0.at[y], at(x, core, ys(d))) for d in range(1, cols)]
    mark("k_leafin")
    for key, made in got.items():
        if key[2] == 2:
            made.wait_recv()

    mark("l_base")
    lane = iota((BLK, LANES), 1)
    sub = iota((BLK, LANES), 0)
    block_of = (lane // BLK) % BLK
    diag = [[[None] * 4 for _ in range(4)] for _ in range(2)]
    inv = [[[None] * 4 for _ in range(4)] for _ in range(2)]
    for m in range(2):
        for c in range(4):
            for k in range(c + 1):
                total = jnp.zeros((BLK, LANES), F32)
                for b in range(8):
                    total = jnp.where(block_of == b, G[k, m, c, b // 2, b % 2], total)
                diag[m][c][k] = total
                inv[m][c][k] = jnp.where(sub == lane % BLK, 1.0, 0.0) if c == k else jnp.zeros((BLK, LANES), F32)
    for t in range(32):
        ct, jt = t // BLK, t % BLK
        index = (lane // BLK) * BLK + jt
        for m in range(2):
            spread = [jnp.take_along_axis(diag[m][c][ct], index, axis=1) for c in range(ct, 4)]
            pivot = 1.0 / spread[0][jt:jt + 1, :]
            below = jnp.where(sub > jt, spread[0], 0.0)
            for k in range(ct + 1):
                solved = inv[m][ct][k][jt:jt + 1, :] * pivot
                inv[m][ct][k] = jnp.where(sub == jt, solved, inv[m][ct][k] - below * solved)
                for c in range(ct + 1, 4):
                    inv[m][c][k] = inv[m][c][k] - spread[c - ct] * solved
    for m in range(2):
        for c in range(4):
            tiles = [inv[m][c][k] if k <= c else jnp.zeros((BLK, LANES), F32) for k in range(4)]
            for e in range(2):
                PK[2 * m + e, c] = halves(tiles, e)
    mark("m_sep")
    wide_block = (iota((BLK, 2 * LANES), 1) % 64) // BLK

    @pl.loop(0, 2)
    def _(m):
        tiles = [G[k, m].reshape(256, LANES) for k in range(4)]
        for e in range(2):
            LF[2 * m + e] = halves(tiles, e).reshape(32, BLK, 256)

    def keep(mask, tile):
        return jnp.where(mask, tile, 0.0)

    def double(leaf, nb):
        group = wide_block // nb
        packed = [PK[leaf, i] for i in range(4 * nb)]
        spread = jnp.concatenate([keep(group == b // nb, packed[(b % nb) * 4 + c]) for c in range(4) for b in range(8)], axis=0)
        coupling = []
        for bb in range(nb):
            for c in range(4):
                total = None
                for s in range(1, 8 // nb, 2):
                    tile = LF[leaf, c * 8 + s * nb + bb]
                    total = keep(group == s - 1, tile if total is None else tile) if total is None else jnp.where(group == s - 1, tile, total)
                coupling.append(total)
        temp = dot(jnp.concatenate(coupling, axis=0), spread)
        zero = jnp.zeros((BLK, 256), F32)
        temp_spread = jnp.concatenate(
            [keep(group == b // nb - 1, temp[((b % nb) * 4 + c) * BLK:((b % nb) * 4 + c + 1) * BLK]) if (b // nb) % 2 else zero
             for c in range(4) for b in range(8)], axis=0)
        corner = dot(jnp.concatenate(packed, axis=0), temp_spread)
        for half in range(2):
            for i in range(4 * nb):
                tile = keep(group % 2 == half, packed[i])
                if half:
                    tile = tile - corner[i * BLK:(i + 1) * BLK]
                if nb < 4:
                    PK[leaf, half * 4 * nb + i] = tile
                else:
                    bb, c = i // 4, i % 4
                    LI[leaf, c * 8 + half * 4 + bb] = tile

    mark("n_dbl")
    for step, nb in enumerate((1, 2, 4)):
        @pl.loop(0, 2)
        def _(m):
            for e in range(2):
                double(2 * m + e, nb)
        relay(2 + step)

    def leaf_inv(i):
        return LI[i].reshape(256, 256)

    mark("o_arrive")
    for g in range(2, 5):
        arrive(g)

    mark("p_chain")
    def coupling2(m):
        return halves([G[k, 2].reshape(256, LANES) for k in range(4)], m)

    def coupling1(g):
        return jnp.concatenate([G[k, g].reshape(256, LANES) for k in range(4)], axis=1)

    def pick(i):
        r, l = iota((256, 256), 0), iota((256, 256), 1)
        return jnp.where((r // 64 == y) & (l // 64 == i) & (r % 64 == l % 64), 1.0, 0.0)

    send_w = [net.copy(W.at[i // 2, :, i % 2], W.at[i // 2, :, i % 2], partner) for i in range(4)]
    send_z = [net.copy(ZS.at[i], ZM.at[i], partner) for i in range(4)]

    @pl.when(core == 0)
    def _():
        def put(i, val):
            W[i // 2, :, i % 2] = val.reshape(4, 4, 2, BLK, 256)
            send_w[i].start()
            return val

        w0 = put(0, dot(leaf_inv(0), pick(0)))
        w1 = put(1, dot(leaf_inv(1), pick(1) - dot(coupling2(0), w0)))
        pair = W[0].reshape(512, 256)
        s2 = pick(2) - dot(coupling1(3), pair)
        s3 = pick(3) - dot(coupling1(4), pair)
        w2 = put(2, dot(leaf_inv(2), s2))
        put(3, dot(leaf_inv(3), s3 - dot(coupling2(1), w2)))

    @pl.when(core == 1)
    def _():
        def mine(i):
            r, l = iota((256, 256), 0), iota((256, 256), 1)
            own = CORES * x + r // 128
            return jnp.where(((r // 32) % 4 == i) & (l // 64 == own % cols) & ((l % 64) // BLK == 2 * ((r // BLK) % 4) + own // cols)
                             & (r % BLK == l % BLK), 1.0, 0.0)

        def put(i, val):
            ZS[i] = val[:128]
            send_z[i].start()
            ZM[i] = val[128:]
            return val

        z3 = put(3, dot(mine(3), leaf_inv(3)))
        z2 = put(2, dot(mine(2) - dot(z3, coupling2(1)), leaf_inv(2)))
        both = dot(z2, coupling1(3)) + dot(z3, coupling1(4))
        tiles = [both[:, LANES * k:LANES * (k + 1)] for k in range(4)]
        z1 = put(1, dot(mine(1) - halves(tiles, 1), leaf_inv(1)))
        put(0, dot(mine(0) - halves(tiles, 0) - dot(z1, coupling2(0)), leaf_inv(0)))

    mark("q_waits")
    for made in c0_copies:
        made.wait_recv()

    @pl.when(core == 0)
    def _():
        for made in send_z:
            made.wait_recv()

    @pl.when(core == 1)
    def _():
        for made in send_w:
            made.wait_recv()

    mark("r_T0")
    left = jnp.concatenate([C0[k, :, LANES * n:LANES * (n + 1)] for n in range(2) for k in range(4)], axis=1)
    TG[:, spot, :, hh] = dot(left, W[...].reshape(1024, 256)).reshape(4, 4, BLK, 256)

    def t_piece(step, part=None):
        own = CORES * xs(step) + core
        return TG.at[slice(None) if part is None else pl.ds(2 * part, 2), own % cols, :, own // cols]

    t_up = net.start(t_piece(0), t_piece(0), at(xs(1), core, y))
    t_down = net.start(t_piece(0), t_piece(0), at(xs(-1), core, y))
    t_in = [net.start(t_piece(0), t_piece(0), partner)]

    mark("s_out")
    o_ref[0:128, 256:512] = jnp.zeros((128, 256), F32)
    for i in range(4):
        o_ref[32 * i:32 * (i + 1), 0:256] = W[i // 2, spot, i % 2, :, hh].reshape(32, 256)
    o_ref[128:256, 256:512] = sum(dot(ZM[i], pick(i)) for i in range(4))

    mark("t_twait")
    t_up.wait_recv()
    far_up = net.start(t_piece(-1, 0), t_piece(-1, 0), at(xs(1), core, y))
    t_in.append(net.start(t_piece(-1), t_piece(-1), partner))
    t_down.wait_recv()
    far_down = net.start(t_piece(1, 1), t_piece(1, 1), at(xs(-1), core, y))
    t_in.append(net.start(t_piece(1), t_piece(1), partner))
    far_up.wait_recv()
    t_in.append(net.start(t_piece(2, 0), t_piece(2, 0), partner))
    far_down.wait_recv()
    t_in.append(net.start(t_piece(2, 1), t_piece(2, 1), partner))
    for made in t_in:
        made.wait_recv()
    mark("u_x21")
    o_ref[128:256, 0:256] = -sum(dot(ZM[i], TG[i].reshape(256, 256)) for i in range(4))

    mark("v_end")
    for made in net.all:
        made.wait_send()

    @pl.when(core == 0)
    def _():
        for made in send_w:
            made.wait_send()

    @pl.when(core == 1)
    def _():
        for made in send_z:
            made.wait_send()
    mark()


def solution(mesh):
    rows, cols = mesh.shape["row"], mesh.shape["col"]
    block_spec = P(("batch", "row"), "col")

    def device_body(local_l):
        vmem = functools.partial(pltpu.VMEM, dtype=F32)
        slots = 160
        return pl.pallas_call(
            functools.partial(kernel, rows, cols),
            out_shape=jax.ShapeDtypeStruct(local_l.shape, F32),
            in_specs=[pl.BlockSpec(memory_space=pl.ANY)],
            out_specs=pl.BlockSpec(memory_space=pltpu.VMEM),
            scratch_shapes=[
                vmem(local_l.shape),
                vmem((5, 4, BLK, LANES)),
                vmem((4, 5, 4, 4, 2, BLK, LANES)),
                vmem((4, 128, 256)),
                vmem((4, 32, BLK, 256)),
                vmem((4, 16, BLK, 256)),
                vmem((4, 32, BLK, 256)),
                vmem((2, 4, 2, 4, 2, BLK, 256)),
                vmem((4, 128, 256)),
                vmem((4, 128, 256)),
                vmem((4, 4, 4, 2, BLK, 256)),
                pltpu.SemaphoreType.DMA((3,)),
                pltpu.SemaphoreType.DMA((slots,)),
                pltpu.SemaphoreType.DMA((slots,)),
            ],
            compiler_params=pltpu.CompilerParams(collective_id=0, has_side_effects=True),
        )(local_l)

    return jax.shard_map(device_body, mesh=mesh, in_specs=(block_spec,), out_specs=block_spec, check_vma=False)
```

```python
import functools

import jax
import jax.numpy as jnp
from jax import lax
from jax.experimental import pallas as pl
from jax.experimental.pallas import tpu as pltpu
from jax.sharding import PartitionSpec as P

BLK = 8
CORES = 2
LANES = 128
HALF = LANES // 2
WIDE = 2 * LANES
TALL = 4
GROUPS = 5
REST = range(2, GROUPS)
LEAVES = range(2)
PAIR = range(2)
SIDES = (-1, 1)
MESH = pl.DeviceIdType.MESH


class Marks:
    def __init__(self):
        self.scope = None

    def __call__(self, name=None):
        if self.scope is not None:
            self.scope.__exit__(None, None, None)
        self.scope = None if name is None else jax.named_scope(name)
        if name is not None:
            self.scope.__enter__()
F32 = jnp.float32


def dot(left, right):
    return jnp.dot(left, right, precision=lax.Precision.HIGHEST, preferred_element_type=F32)


def iota(shape, dim):
    return lax.broadcasted_iota(jnp.int32, shape, dim)


def halves(tiles, half):
    low = iota(tiles[0].shape, 1) < HALF
    out = []
    for first, second in ((tiles[0], tiles[1]), (tiles[2], tiles[3])):
        if half == 0:
            out.append(jnp.where(low, first, pltpu.roll(second, HALF, 1)))
        else:
            out.append(jnp.where(low, pltpu.roll(first, HALF, 1), second))
    return jnp.concatenate(out, axis=1)


class Net:
    def __init__(self, send, recv):
        self.send, self.recv, self.names = send, recv, {}

    def slot(self, side, name):
        held = [key for key in self.names if key[0] == side]
        return self.names.setdefault((side, name), len(held))

    def start(self, src, dst, device, send, recv):
        self.make(src, dst, device, send, recv).start()

    def make(self, src, dst, device, send, recv):
        return pltpu.make_async_remote_copy(
            src_ref=src, dst_ref=dst, send_sem=self.send.at[self.slot("send", send)], recv_sem=self.recv.at[self.slot("recv", recv)],
            device_id=device, device_id_type=MESH)

    def wait(self, name, like, side="recv"):
        sems = self.recv if side == "recv" else self.send
        pltpu.make_async_copy(like, like, sems.at[self.slot(side, name)]).wait()


def shift(val, lanes):
    return jnp.concatenate([pltpu.roll(val[:, LANES * i:LANES * (i + 1)], lanes % LANES, 1) for i in range(2)], axis=1)


def kernel(rows, cols, hbm_ref, o_ref, l_ref, U, G, C0, LF, PK, LI, WL, WR, ZM, ZS, TG, load, send, recv):
    chips = rows // CORES
    row = lax.axis_index("row")
    y = lax.axis_index("col")
    x, core = row // CORES, row % CORES
    spot, hh = row % cols, row // cols
    net = Net(send, recv)
    first_half = core == 1

    def at(xx, cc, yy):
        return {"row": xx * CORES + cc, "col": yy}

    def xs(step):
        return lax.rem(x + step + chips, chips)

    def ys(step):
        return lax.rem(y + step + cols, cols)

    def along(axis, step, cc=core):
        return at(xs(step), cc, y) if axis == "x" else at(x, cc, ys(step))

    mark = Marks()
    mark("a_signal")
    upper, lower, near, far = pl.ds(0, LANES), pl.ds(LANES, LANES), pl.ds(0, WIDE), pl.ds(WIDE, WIDE)
    windows = [(upper, near), (lower, far), (lower, near)]
    loads = [pltpu.make_async_copy(hbm_ref.at[w], l_ref.at[w], load.at[i]) for i, w in enumerate(windows)]
    for made in loads:
        made.start()
    partner = at(x, 1 - core, y)
    barrier = pltpu.get_barrier_semaphore()
    peers = [partner] + [along(axis, d, cc) for axis in "xy" for d in range(1, chips) for cc in range(CORES)]
    for peer in peers:
        pl.semaphore_signal(barrier, inc=1, device_id=peer, device_id_type=MESH)

    mark("a_pack")
    quarter = LANES // TALL
    for part in range(2):
        loads[part].wait()
        piece = l_ref[part * LANES:(part + 1) * LANES, part * WIDE:(part + 1) * WIDE]
        low = iota((quarter, LANES), 1) < HALF
        band = [piece[quarter * i:quarter * (i + 1)] for i in range(TALL)]
        packed = [jnp.where(low, band[2 * m][:, LANES * m:LANES * (m + 1)], band[2 * m + 1][:, LANES * m:LANES * (m + 1)])
                  for m in PAIR]
        packed.append(jnp.where(low, band[1][:, :LANES], pltpu.roll(band[3][:, LANES:], HALF, 1)))
        packed += [band[2][:, :LANES], band[3][:, :LANES]]
        tiles = [val.reshape(TALL, BLK, LANES) for val in packed]
        for g in range(GROUPS):
            U[part, g] = tiles[g]

        @pl.when(core == 1 - part)
        def _():
            for g in range(GROUPS):
                G[y, g, hh, spot] = tiles[g]

    loads[2].wait()
    C0[core, y] = l_ref[lower, near]
    mark("b_barrier")
    pl.semaphore_wait(barrier, len(peers))

    axis_first = ["x", "y", "y", "x", "y"]

    def other(axis):
        return "y" if axis == "x" else "x"

    def source(g, f, s, k=None):
        xx, yy = (xs(f), ys(s)) if axis_first[g] == "x" else (xs(s), ys(f))
        return G.at[yy, g, xx // 2, pl.ds(2 * (xx % 2), 2) if k is None else 2 * (xx % 2) + k]

    def pass_on(g, f, s, k, step, name):
        piece = source(g, f, s, k)
        net.start(piece, piece, along(other(axis_first[g]), step), g, name)

    def pass_leaf(g, f):
        for s in SIDES:
            pass_on(g, f, 0, None, -s, (g, "far") if f == 2 else (g, f, s))
        if f == 2:
            pass_on(g, f, 0, None, 2, (g, "far"))

    def half_on(g, f, s):
        pass_on(g, f, s, 0 if s < 0 else 1, -s, (g, "far"))

    mark("d_own")
    for axis in "xy":
        for step in SIDES:
            for part in range(2):
                net.start(U.at[part, pl.ds(0, 2)], G.at[y, pl.ds(0, 2), hh, spot], along(axis, step, 1 - part), "leaf", (axis, -step))
    for g in LEAVES:
        for part in range(2):
            net.start(U.at[part, g], G.at[y, g, hh, spot], along(axis_first[g], 2, 1 - part), "leaf", (g, "two"))
    net.start(U.at[core], G.at[y, :, hh, spot], partner, "pair", "pair")

    mark("e_near")
    for step in SIDES:
        for axis in "xy":
            net.wait((axis, step), G.at[0, pl.ds(0, 2), 0, pl.ds(0, 2)])
            for g in LEAVES:
                if axis_first[g] == axis:
                    pass_leaf(g, step)
                else:
                    half_on(g, 0, step)
    for g in REST:
        for d in range(1, chips):
            for part in range(2):
                net.start(U.at[part, g], G.at[y, g, hh, spot], along(axis_first[g], d, 1 - part), "rest", (g, "first"))
    mark("f_pair")
    net.wait("pair", U.at[0])
    mark("g_two")
    for g in LEAVES:
        net.wait((g, "two"), G.at[0, 0, 0, pl.ds(0, 2)])
        pass_leaf(g, 2)
    mark("h_diag")
    for f in SIDES:
        for s in SIDES:
            for g in LEAVES:
                net.wait((g, f, s), source(g, f, s))
                half_on(g, f, s)

    def bundle(g, step, part=None):
        if axis_first[g] == "x":
            return G.at[ys(step), g] if part is None else G.at[ys(step), g, part]
        xx = xs(step)
        return G.at[slice(None) if part is None else pl.ds(2 * part, 2), g, xx // 2, pl.ds(2 * (xx % 2), 2)]

    def send_second(g):
        net.wait((g, "first"), G.at[0, pl.ds(0, 3), 0, pl.ds(0, 2)])
        for s in SIDES:
            net.start(bundle(g, 0), bundle(g, 0), along(other(axis_first[g]), -s), g, (g, "near", s))

    def relay(g):
        for s in SIDES:
            net.wait((g, "near", s), G.at[0, g])
            half = bundle(g, s, 0 if s < 0 else 1)
            net.start(half, half, along(other(axis_first[g]), -s), g, (g, "end"))

    def arrive(g):
        net.wait((g, "end"), G.at[0, g])

    mark("j_second")
    for g in REST:
        send_second(g)
    for s in SIDES:
        net.start(l_ref.at[lower, near], C0.at[core, y], along("y", -s, 1), "c0", ("c0", s))

    @pl.when(core == 0)
    def _():
        net.start(l_ref.at[lower, near], C0.at[core, y], partner, "c0pair", "c0pair")

    mark("k_leafin")
    for g in LEAVES:
        net.wait((g, "far"), G.at[pl.ds(0, 3), g, 0])

    mark("l_base")
    lane = iota((BLK, LANES), 1)
    sub = iota((BLK, LANES), 0)
    block_of = (lane // BLK) % BLK
    diag = [[[None] * TALL for _ in range(TALL)] for _ in PAIR]
    inv = [[[None] * TALL for _ in range(TALL)] for _ in PAIR]
    for m in PAIR:
        for c in range(TALL):
            for k in range(c + 1):
                total = jnp.zeros((BLK, LANES), F32)
                for b in range(BLK):
                    total = jnp.where(block_of == b, G[k, m, b % 2, c, b // 2], total)
                diag[m][c][k] = total
                inv[m][c][k] = jnp.where(sub == lane % BLK, 1.0, 0.0) if c == k else jnp.zeros((BLK, LANES), F32)
    for t in range(BLK * TALL):
        ct, jt = t // BLK, t % BLK
        index = (lane // BLK) * BLK + jt
        for m in PAIR:
            spread = [jnp.take_along_axis(diag[m][c][ct], index, axis=1) for c in range(ct, TALL)]
            pivot = 1.0 / spread[0][jt:jt + 1, :]
            below = jnp.where(sub > jt, spread[0], 0.0)
            for k in range(ct + 1):
                solved = inv[m][ct][k][jt:jt + 1, :] * pivot
                inv[m][ct][k] = jnp.where(sub == jt, solved, inv[m][ct][k] - below * solved)
                for c in range(ct + 1, TALL):
                    inv[m][c][k] = inv[m][c][k] - spread[c - ct] * solved
    for m in PAIR:
        for c in range(TALL):
            tiles = [inv[m][c][k] if k <= c else jnp.zeros((BLK, LANES), F32) for k in range(TALL)]
            for e in PAIR:
                PK[2 * m + e, c] = halves(tiles, e)

    def gathered(k, g):
        return jnp.concatenate([G[k, g, b % 2, c, b // 2] for c in range(TALL) for b in range(BLK)], axis=0)

    mark("m_sep")
    for m in PAIR:
        tiles = [gathered(k, m) for k in range(cols)]
        for e in PAIR:
            LF[2 * m + e] = halves(tiles, e).reshape(TALL * BLK, BLK, WIDE)

    def double(m, nb):
        count, lanes = TALL * nb, BLK * nb
        size = BLK * count
        group = ((iota((BLK, WIDE), 1) % HALF) // BLK) // nb
        even = ((iota((size, WIDE), 1) % HALF) // BLK) // nb % 2 == 0

        def coupling(leaf):
            out = []
            for bb in range(nb):
                for c in range(TALL):
                    total = LF[leaf, c * BLK + nb + bb]
                    for s in range(3, BLK // nb, 2):
                        total = jnp.where(group == s - 1, LF[leaf, c * BLK + s * nb + bb], total)
                    out.append(total)
            return jnp.concatenate(out, axis=0)

        def spread(val, flip):
            tiles = val.reshape(count, BLK, WIDE)
            return jnp.concatenate([jnp.where(group == (b // nb) ^ flip, tiles[(b % nb) * TALL + c], 0.0)
                                    for c in range(TALL) for b in range(BLK)], axis=0)

        one, two = (PK[2 * m + e, 0:count].reshape(size, WIDE) for e in PAIR)
        temp = dot(jnp.where(even, coupling(2 * m), shift(coupling(2 * m + 1), lanes)),
                   spread(jnp.where(even, one, shift(two, lanes)), 0))
        corner = dot(jnp.where(even, shift(two, -lanes), one), spread(temp, 1))
        for e, (val, low) in enumerate(((one, corner), (two, shift(corner, -lanes)))):
            parts = (jnp.where(even, val, 0.0), jnp.where(even, -low, val))
            for half in PAIR:
                tiles = parts[half].reshape(count, BLK, WIDE)
                if nb < TALL:
                    PK[2 * m + e, half * count:(half + 1) * count] = tiles
                else:
                    for i in range(count):
                        LI[2 * m + e, (i % TALL) * BLK + half * TALL + i // TALL] = tiles[i]

    mark("n_dbl1")
    for m in PAIR:
        double(m, 1)
    mark("n_rel2")
    relay(2)
    mark("n_dbl2")
    for m in PAIR:
        double(m, 2)
    mark("n_rel34")
    relay(3)
    relay(4)

    @pl.when(first_half)
    def _():
        for s in SIDES:
            net.wait(("c0", s), C0.at[:, 0])
            piece = C0.at[0 if s < 0 else 1, ys(s)]
            net.start(piece, piece, along("y", -s), "c0far", "c0far")

    mark("n_dbl4")
    for m in PAIR:
        double(m, 4)
    mark("o_arr2")
    arrive(2)

    def leaf_inv(i):
        return LI[i].reshape(WIDE, WIDE)

    def coupling2(m):
        return halves([gathered(k, 2) for k in range(cols)], m)

    def coupling1(g):
        return jnp.concatenate([gathered(k, g) for k in range(cols)], axis=1)

    def pick(i, width=WIDE, base=0):
        r, l = iota((WIDE, width), 0), iota((WIDE, width), 1) + base
        return jnp.where((r // HALF == y) & (l // HALF == i) & (r % HALF == l % HALF), 1.0, 0.0)

    def mine(i):
        r, l = iota((WIDE, WIDE), 0), iota((WIDE, WIDE), 1)
        own = CORES * x + r // LANES
        return jnp.where(((r // quarter) % TALL == i) & (l // HALF == own % cols) & (r % BLK == l % BLK)
                         & ((l % HALF) // BLK == 2 * ((r // BLK) % TALL) + own // cols), 1.0, 0.0)

    def put_w(ref, val):
        ref[...] = val.reshape(TALL, TALL, 2, BLK, LANES)
        return val

    def put_z(i, val):
        ZM[i] = val[:LANES]
        ZS[i] = val[LANES:]
        net.start(ZS.at[i], ZM.at[i], partner, "z", "z")
        return val

    def t_piece(side, step, k=None):
        xx = xs(step)
        return TG.at[side, xx // 2, pl.ds(2 * (xx % 2), 2) if k is None else 2 * (xx % 2) + k]

    def t_start(side, step, k, device, name, kind="t"):
        net.start(t_piece(side, step, k), t_piece(side, step, k), device, kind, (side, name))

    def t_send(side, val):
        t_piece(side, 0)[...] = val.reshape(CORES, TALL, TALL, BLK, LANES)
        for i in PAIR:
            for s in SIDES:
                k = i if s < 0 else 1 - i
                t_start(side, 0, k, along("x", -s), (s, i))
        t_start(side, 0, None, partner, "partner", "tpair")

    def t_near(side):
        for i in PAIR:
            for s in SIDES:
                k = i if s < 0 else 1 - i
                net.wait((side, (s, i)), t_piece(side, s, k))
                if i == 0:
                    t_start(side, s, k, along("x", -s), "far")
                t_start(side, s, k, partner, "partner", "tpair")

    def t_far(side):
        net.wait((side, "far"), t_piece(side, 2))
        t_start(side, 2, None, partner, "partner", "tpair")

    def t_left(tiles):
        return jnp.concatenate([jnp.concatenate([C0[k, c, :, LANES * n:LANES * (n + 1)] for n in tiles for c in range(cols)], axis=1)
                                for k in range(CORES)], axis=0)

    def w_rows(ref):
        own = CORES * x
        return ref.at[..., own % cols, :, :, own // cols, :, :]

    mark("p_chain1")

    @pl.when(first_half)
    def _():
        w2 = put_w(WR.at[:, 0], dot(leaf_inv(2), pick(2, LANES, LANES)))
        put_w(WR.at[:, 1], dot(leaf_inv(3), pick(3, LANES, LANES) - dot(coupling2(1), w2)))
        net.wait("c0pair", C0.at[0, 0])
        net.wait("c0far", C0.at[0, pl.ds(0, 2)])
        t_send(1, dot(t_left((1,)), WR[...].reshape(2 * WIDE, LANES)))
        w0 = put_w(WL.at[0, :, 0], dot(leaf_inv(0), pick(0, LANES)))
        put_w(WL.at[0, :, 1], dot(leaf_inv(1), pick(1, LANES) - dot(coupling2(0), w0)))

    @pl.when(core == 0)
    def _():
        z3 = put_z(3, dot(mine(3), leaf_inv(3)))
        put_z(2, dot(mine(2) - dot(z3, coupling2(1)), leaf_inv(2)))

    mark("o_arr34")
    for g in (3, 4):
        arrive(g)

    mark("p_chain2")

    @pl.when(first_half)
    def _():
        pair = WL[0].reshape(2 * WIDE, LANES)
        s2 = -dot(coupling1(3), pair)
        s3 = -dot(coupling1(4), pair)
        w2 = put_w(WL.at[1, :, 0], dot(leaf_inv(2), s2))
        put_w(WL.at[1, :, 1], dot(leaf_inv(3), s3 - dot(coupling2(1), w2)))
        t_near(1)
        t_send(0, dot(t_left(PAIR), WL[...].reshape(4 * WIDE, LANES)))
        net.start(w_rows(WL), w_rows(WL), partner, "w", "w")
        net.start(w_rows(WR), w_rows(WR), partner, "w", "w")

    @pl.when(core == 0)
    def _():
        z3, z2 = (jnp.concatenate([ZM[i], ZS[i]], axis=0) for i in (3, 2))
        both_rows = dot(z2, coupling1(3)) + dot(z3, coupling1(4))
        tiles = [both_rows[:, LANES * k:LANES * (k + 1)] for k in range(cols)]
        z1 = put_z(1, dot(mine(1) - halves(tiles, 1), leaf_inv(1)))
        put_z(0, dot(mine(0) - halves(tiles, 0) - dot(z1, coupling2(0)), leaf_inv(0)))
        net.wait("w", G.at[0, pl.ds(0, 3), 0, pl.ds(0, 2)])

    mark("s_out")

    @pl.when(first_half)
    def _():
        net.wait("z", ZM)

    o_ref[upper, far] = jnp.zeros((LANES, WIDE), F32)
    for i in range(TALL):
        lines = slice(quarter * i, quarter * (i + 1))
        o_ref[lines, :LANES] = WL[i // 2, spot, i % 2, :, hh].reshape(quarter, LANES)
        o_ref[lines, LANES:WIDE] = WR[spot, i % 2, :, hh].reshape(quarter, LANES) if i >= 2 else jnp.zeros((quarter, LANES), F32)
    o_ref[lower, far] = sum(dot(ZM[i], pick(i)) for i in range(TALL))

    mark("t_near")

    @pl.when(first_half)
    def _():
        t_near(0)
        t_far(1)
        t_far(0)

    mark("t_end")

    @pl.when(core == 0)
    def _():
        for side in PAIR:
            net.wait((side, "partner"), TG.at[side])

    def t_rows(i):
        return jnp.concatenate([jnp.concatenate([TG[side, b % 2, c, i, b // 2] for c in range(TALL) for b in range(BLK)], axis=0)
                                for side in PAIR], axis=1)

    mark("u_x21")
    o_ref[lower, near] = -sum(dot(ZM[i], t_rows(i)) for i in range(TALL))

    mark("v_end")
    for name in ("leaf", *LEAVES):
        net.wait(name, G.at[0, :, 0], "send")
    net.wait("rest", G.at[pl.ds(0, 2), pl.ds(0, 3), 0, pl.ds(0, 3)], "send")
    for g in REST:
        net.wait(g, G.at[pl.ds(0, 3), g], "send")
    net.wait("pair", U.at[0], "send")
    net.wait("c0", C0.at[0, pl.ds(0, 2)], "send")

    @pl.when(first_half)
    def _():
        net.wait("c0far", C0.at[0, pl.ds(0, 2)], "send")
        net.wait("t", G.at[:, pl.ds(0, 3), 0], "send")
        net.wait("tpair", TG, "send")
        net.wait("w", G.at[0, pl.ds(0, 3), 0, pl.ds(0, 2)], "send")

    @pl.when(core == 0)
    def _():
        net.wait("c0pair", C0.at[0, 0], "send")
        net.wait("z", ZM, "send")

    mark()
    counts = [len([key for key in net.names if key[0] == side]) for side in ("send", "recv")]
    assert counts == [send.shape[0], recv.shape[0]], counts


def solution(mesh):
    rows, cols = mesh.shape["row"], mesh.shape["col"]
    block_spec = P(("batch", "row"), "col")

    def device_body(local_l):
        vmem = functools.partial(pltpu.VMEM, dtype=F32)
        return pl.pallas_call(
            functools.partial(kernel, rows, cols),
            out_shape=jax.ShapeDtypeStruct(local_l.shape, F32),
            in_specs=[pl.BlockSpec(memory_space=pl.ANY)],
            out_specs=pl.BlockSpec(memory_space=pltpu.VMEM),
            scratch_shapes=[
                vmem(local_l.shape),
                vmem((2, GROUPS, TALL, BLK, LANES)),
                vmem((cols, GROUPS, 2, TALL, TALL, BLK, LANES)),
                vmem((CORES, cols, LANES, WIDE)),
                vmem((TALL, TALL * BLK, BLK, WIDE)),
                vmem((TALL, 2 * BLK, BLK, WIDE)),
                vmem((TALL, TALL * BLK, BLK, WIDE)),
                vmem((2, cols, 2, TALL, 2, BLK, LANES)),
                vmem((cols, 2, TALL, 2, BLK, LANES)),
                vmem((TALL, LANES, WIDE)),
                vmem((TALL, LANES, WIDE)),
                vmem((2, 2, TALL, TALL, TALL, BLK, LANES)),
                pltpu.SemaphoreType.DMA((3,)),
                pltpu.SemaphoreType.DMA((15,)),
                pltpu.SemaphoreType.DMA((45,)),
            ],
            compiler_params=pltpu.CompilerParams(collective_id=0, has_side_effects=True),
        )(local_l)

    return jax.shard_map(device_body, mesh=mesh, in_specs=(block_spec,), out_specs=block_spec, check_vma=False)
```

```python
import functools

import jax
import jax.numpy as jnp
from jax import lax
from jax.experimental import pallas as pl
from jax.experimental.pallas import tpu as pltpu
from jax.sharding import PartitionSpec as P

BLK = 8
CORES = 2
LANES = 128
HALF = LANES // 2
WIDE = 2 * LANES
TALL = 4
GROUPS = 5
REST = range(2, GROUPS)
LEAVES = range(2)
PAIR = range(2)
SIDES = (-1, 1)
MESH = pl.DeviceIdType.MESH


class Marks:
    def __init__(self):
        self.scope = None

    def __call__(self, name=None):
        if self.scope is not None:
            self.scope.__exit__(None, None, None)
        self.scope = None if name is None else jax.named_scope(name)
        if name is not None:
            self.scope.__enter__()
F32 = jnp.float32


def dot(left, right):
    return jnp.dot(left, right, precision=lax.Precision.HIGHEST, preferred_element_type=F32)


def iota(shape, dim):
    return lax.broadcasted_iota(jnp.int32, shape, dim)


def halves(tiles, half):
    low = iota(tiles[0].shape, 1) < HALF
    out = []
    for first, second in ((tiles[0], tiles[1]), (tiles[2], tiles[3])):
        if half == 0:
            out.append(jnp.where(low, first, pltpu.roll(second, HALF, 1)))
        else:
            out.append(jnp.where(low, pltpu.roll(first, HALF, 1), second))
    return jnp.concatenate(out, axis=1)


class Net:
    def __init__(self, send, recv):
        self.send, self.recv, self.names = send, recv, {}

    def slot(self, side, name):
        held = [key for key in self.names if key[0] == side]
        return self.names.setdefault((side, name), len(held))

    def start(self, src, dst, device, send, recv):
        self.make(src, dst, device, send, recv).start()

    def make(self, src, dst, device, send, recv):
        return pltpu.make_async_remote_copy(
            src_ref=src, dst_ref=dst, send_sem=self.send.at[self.slot("send", send)], recv_sem=self.recv.at[self.slot("recv", recv)],
            device_id=device, device_id_type=MESH)

    def wait(self, name, like, side="recv"):
        sems = self.recv if side == "recv" else self.send
        pltpu.make_async_copy(like, like, sems.at[self.slot(side, name)]).wait()


def shift(val, lanes):
    return jnp.concatenate([pltpu.roll(val[:, LANES * i:LANES * (i + 1)], lanes % LANES, 1) for i in range(2)], axis=1)


def kernel(rows, cols, hbm_ref, o_ref, l_ref, U, G, C0, LF, PK, LI, WL, WR, ZM, ZS, TG, VV, SS, TP, load, send, recv):
    chips = rows // CORES
    row = lax.axis_index("row")
    y = lax.axis_index("col")
    x, core = row // CORES, row % CORES
    spot, hh = row % cols, row // cols
    net = Net(send, recv)
    first_half = core == 1

    def at(xx, cc, yy):
        return {"row": xx * CORES + cc, "col": yy}

    def xs(step):
        return lax.rem(x + step + chips, chips)

    def ys(step):
        return lax.rem(y + step + cols, cols)

    def along(axis, step, cc=core):
        return at(xs(step), cc, y) if axis == "x" else at(x, cc, ys(step))

    mark = Marks()
    mark("a_signal")
    upper, lower, near, far = pl.ds(0, LANES), pl.ds(LANES, LANES), pl.ds(0, WIDE), pl.ds(WIDE, WIDE)
    windows = [(upper, near), (lower, far), (lower, near)]
    loads = [pltpu.make_async_copy(hbm_ref.at[w], l_ref.at[w], load.at[i]) for i, w in enumerate(windows)]
    for made in loads:
        made.start()
    partner = at(x, 1 - core, y)
    barrier = pltpu.get_barrier_semaphore()
    peers = [partner] + [along(axis, d, cc) for axis in "xy" for d in range(1, chips) for cc in range(CORES)]
    for peer in peers:
        pl.semaphore_signal(barrier, inc=1, device_id=peer, device_id_type=MESH)

    mark("a_pack")
    quarter = LANES // TALL
    for part in range(2):
        loads[part].wait()
        piece = l_ref[part * LANES:(part + 1) * LANES, part * WIDE:(part + 1) * WIDE]
        low = iota((quarter, LANES), 1) < HALF
        band = [piece[quarter * i:quarter * (i + 1)] for i in range(TALL)]
        packed = [jnp.where(low, band[2 * m][:, LANES * m:LANES * (m + 1)], band[2 * m + 1][:, LANES * m:LANES * (m + 1)])
                  for m in PAIR]
        packed.append(jnp.where(low, band[1][:, :LANES], pltpu.roll(band[3][:, LANES:], HALF, 1)))
        packed += [band[2][:, :LANES], band[3][:, :LANES]]
        tiles = [val.reshape(TALL, BLK, LANES) for val in packed]
        for g in range(GROUPS):
            U[part, g] = tiles[g]

        @pl.when(core == 1 - part)
        def _():
            for g in range(GROUPS):
                G[y, g, hh, spot] = tiles[g]

    loads[2].wait()
    C0[core, y] = l_ref[lower, near]
    mark("b_barrier")
    pl.semaphore_wait(barrier, len(peers))

    axis_first = ["x", "y", "y", "x", "y"]

    def other(axis):
        return "y" if axis == "x" else "x"

    def source(g, f, s, k=None):
        xx, yy = (xs(f), ys(s)) if axis_first[g] == "x" else (xs(s), ys(f))
        return G.at[yy, g, xx // 2, pl.ds(2 * (xx % 2), 2) if k is None else 2 * (xx % 2) + k]

    def pass_on(g, f, s, k, step, name):
        piece = source(g, f, s, k)
        net.start(piece, piece, along(other(axis_first[g]), step), g, name)

    def pass_leaf(g, f):
        for s in SIDES:
            pass_on(g, f, 0, None, -s, (g, "far") if f == 2 else (g, f, s))
        if f == 2:
            pass_on(g, f, 0, None, 2, (g, "far"))

    def half_on(g, f, s):
        pass_on(g, f, s, 0 if s < 0 else 1, -s, (g, "far"))

    mark("d_own")
    for axis in "xy":
        for step in SIDES:
            for part in range(2):
                net.start(U.at[part, pl.ds(0, 2)], G.at[y, pl.ds(0, 2), hh, spot], along(axis, step, 1 - part), "leaf", (axis, -step))
    for g in LEAVES:
        for part in range(2):
            net.start(U.at[part, g], G.at[y, g, hh, spot], along(axis_first[g], 2, 1 - part), "leaf", (g, "two"))
    net.start(U.at[core], G.at[y, :, hh, spot], partner, "pair", "pair")

    mark("e_near")
    for step in SIDES:
        for axis in "xy":
            net.wait((axis, step), G.at[0, pl.ds(0, 2), 0, pl.ds(0, 2)])
            for g in LEAVES:
                if axis_first[g] == axis:
                    pass_leaf(g, step)
                else:
                    half_on(g, 0, step)
    for g in REST:
        for d in range(1, chips):
            for part in range(2):
                net.start(U.at[part, g], G.at[y, g, hh, spot], along(axis_first[g], d, 1 - part), "rest", (g, "first"))
    mark("f_pair")
    net.wait("pair", U.at[0])
    mark("g_two")
    for g in LEAVES:
        net.wait((g, "two"), G.at[0, 0, 0, pl.ds(0, 2)])
        pass_leaf(g, 2)
    mark("h_diag")
    for f in SIDES:
        for s in SIDES:
            for g in LEAVES:
                net.wait((g, f, s), source(g, f, s))
                half_on(g, f, s)

    def bundle(g, step, part=None):
        if axis_first[g] == "x":
            return G.at[ys(step), g] if part is None else G.at[ys(step), g, part]
        xx = xs(step)
        return G.at[slice(None) if part is None else pl.ds(2 * part, 2), g, xx // 2, pl.ds(2 * (xx % 2), 2)]

    def send_second(g):
        net.wait((g, "first"), G.at[0, pl.ds(0, 3), 0, pl.ds(0, 2)])
        for s in SIDES:
            net.start(bundle(g, 0), bundle(g, 0), along(other(axis_first[g]), -s), g, (g, "near", s))

    def relay(g):
        for s in SIDES:
            net.wait((g, "near", s), G.at[0, g])
            half = bundle(g, s, 0 if s < 0 else 1)
            net.start(half, half, along(other(axis_first[g]), -s), g, (g, "end"))

    def arrive(g):
        net.wait((g, "end"), G.at[0, g])

    mark("j_second")
    send_second(2)
    for s in SIDES:
        net.start(l_ref.at[lower, near], C0.at[core, y], along("y", -s, 1), "c0", ("c0", s))

    @pl.when(core == 0)
    def _():
        net.start(l_ref.at[lower, near], C0.at[core, y], partner, "c0pair", "c0pair")

    send_second(3)
    send_second(4)

    mark("k_leafin")
    for g in LEAVES:
        net.wait((g, "far"), G.at[pl.ds(0, 3), g, 0])

    mark("l_base")
    lane = iota((BLK, LANES), 1)
    sub = iota((BLK, LANES), 0)
    block_of = (lane // BLK) % BLK
    diag = [[[None] * TALL for _ in range(TALL)] for _ in PAIR]
    inv = [[[None] * TALL for _ in range(TALL)] for _ in PAIR]
    for m in PAIR:
        for c in range(TALL):
            for k in range(c + 1):
                total = jnp.zeros((BLK, LANES), F32)
                for b in range(BLK):
                    total = jnp.where(block_of == b, G[k, m, b % 2, c, b // 2], total)
                diag[m][c][k] = total
                inv[m][c][k] = jnp.where(sub == lane % BLK, 1.0, 0.0) if c == k else jnp.zeros((BLK, LANES), F32)
    for t in range(BLK * TALL):
        ct, jt = t // BLK, t % BLK
        index = (lane // BLK) * BLK + jt
        for m in PAIR:
            spread = [jnp.take_along_axis(diag[m][c][ct], index, axis=1) for c in range(ct, TALL)]
            pivot = 1.0 / spread[0][jt:jt + 1, :]
            below = jnp.where(sub > jt, spread[0], 0.0)
            for k in range(ct + 1):
                solved = inv[m][ct][k][jt:jt + 1, :] * pivot
                inv[m][ct][k] = jnp.where(sub == jt, solved, inv[m][ct][k] - below * solved)
                for c in range(ct + 1, TALL):
                    inv[m][c][k] = inv[m][c][k] - spread[c - ct] * solved
    for m in PAIR:
        for c in range(TALL):
            tiles = [inv[m][c][k] if k <= c else jnp.zeros((BLK, LANES), F32) for k in range(TALL)]
            for e in PAIR:
                PK[2 * m + e, c] = halves(tiles, e)

    def gathered(k, g):
        return jnp.concatenate([G[k, g, b % 2, c, b // 2] for c in range(TALL) for b in range(BLK)], axis=0)

    mark("m_sep")
    for m in PAIR:
        tiles = [gathered(k, m) for k in range(cols)]
        for e in PAIR:
            LF[2 * m + e] = halves(tiles, e).reshape(TALL * BLK, BLK, WIDE)

    def double(m, nb):
        count, lanes = TALL * nb, BLK * nb
        size = BLK * count
        group = ((iota((BLK, WIDE), 1) % HALF) // BLK) // nb
        even = ((iota((size, WIDE), 1) % HALF) // BLK) // nb % 2 == 0

        def coupling(leaf):
            out = []
            for bb in range(nb):
                for c in range(TALL):
                    total = LF[leaf, c * BLK + nb + bb]
                    for s in range(3, BLK // nb, 2):
                        total = jnp.where(group == s - 1, LF[leaf, c * BLK + s * nb + bb], total)
                    out.append(total)
            return jnp.concatenate(out, axis=0)

        def spread(val, flip):
            tiles = val.reshape(count, BLK, WIDE)
            return jnp.concatenate([jnp.where(group == (b // nb) ^ flip, tiles[(b % nb) * TALL + c], 0.0)
                                    for c in range(TALL) for b in range(BLK)], axis=0)

        one, two = (PK[2 * m + e, 0:count].reshape(size, WIDE) for e in PAIR)
        temp = dot(jnp.where(even, coupling(2 * m), shift(coupling(2 * m + 1), lanes)),
                   spread(jnp.where(even, one, shift(two, lanes)), 0))
        corner = dot(jnp.where(even, shift(two, -lanes), one), spread(temp, 1))
        for e, (val, low) in enumerate(((one, corner), (two, shift(corner, -lanes)))):
            parts = (jnp.where(even, val, 0.0), jnp.where(even, -low, val))
            for half in PAIR:
                tiles = parts[half].reshape(count, BLK, WIDE)
                if nb < TALL:
                    PK[2 * m + e, half * count:(half + 1) * count] = tiles
                else:
                    for i in range(count):
                        LI[2 * m + e, (i % TALL) * BLK + half * TALL + i // TALL] = tiles[i]

    mark("n_dbl1")
    for m in PAIR:
        double(m, 1)
    mark("n_rel2")
    relay(2)
    mark("n_dbl2")
    for m in PAIR:
        double(m, 2)
    mark("n_dbl4")
    for m in PAIR:
        double(m, 4)
    mark("o_arr2")
    arrive(2)

    def leaf_inv(i):
        return LI[i].reshape(WIDE, WIDE)

    def coupling2(m):
        return halves([gathered(k, 2) for k in range(cols)], m)

    def coupling1(g):
        return jnp.concatenate([gathered(k, g) for k in range(cols)], axis=1)

    def mine(i):
        r, l = iota((WIDE, WIDE), 0), iota((WIDE, WIDE), 1)
        own = CORES * x + r // LANES
        return jnp.where(((r // quarter) % TALL == i) & (l // HALF == own % cols) & (r % BLK == l % BLK)
                         & ((l % HALF) // BLK == 2 * ((r // BLK) % TALL) + own // cols), 1.0, 0.0)

    def put_w(ref, val):
        ref[...] = val.reshape(TALL, TALL, 2, BLK, LANES)
        return val

    def put_z(i, val):
        ZM[i] = val[:LANES]
        ZS[i] = val[LANES:]
        net.start(ZS.at[i], ZM.at[i], partner, "z", "z")
        return val

    def t_piece(side, step, k=None):
        xx = xs(step)
        return TG.at[side, xx // 2, pl.ds(2 * (xx % 2), 2) if k is None else 2 * (xx % 2) + k]

    def t_start(side, step, k, device, name, kind="t"):
        net.start(t_piece(side, step, k), t_piece(side, step, k), device, kind, (side, name))

    def t_send(side, val):
        t_piece(side, 0)[...] = val.reshape(CORES, TALL, TALL, BLK, LANES)
        for i in PAIR:
            for s in SIDES:
                k = i if s < 0 else 1 - i
                t_start(side, 0, k, along("x", -s), (s, i))
        t_start(side, 0, None, partner, "partner", "tpair")

    def t_near(side):
        for i in PAIR:
            for s in SIDES:
                k = i if s < 0 else 1 - i
                net.wait((side, (s, i)), t_piece(side, s, k))
                if i == 0:
                    t_start(side, s, k, along("x", -s), "far")
                t_start(side, s, k, partner, "partner", "tpair")

    def t_far(side):
        net.wait((side, "far"), t_piece(side, 2))
        t_start(side, 2, None, partner, "partner", "tpair")

    def c0_pair(n):
        return [jnp.concatenate([C0[k, c, :, LANES * n:LANES * (n + 1)] for k in range(CORES)], axis=0) for c in range(cols)]

    def own_columns(first, second):
        low = iota((first.shape[0], LANES), 1) < HALF
        out = []
        for val in (first, second):
            tile = jnp.where(y // 2 == 0, val[:, :LANES], val[:, LANES:])
            moved = pltpu.roll(tile, HALF, 1)
            out.append(jnp.where(y % 2 == 0, tile, moved) if val is first else jnp.where(y % 2 == 0, moved, tile))
        return jnp.where(low, out[0], out[1])

    def w_rows(ref):
        own = CORES * x
        return ref.at[..., own % cols, :, :, own // cols, :, :]

    mark("p_chain1")
    low_half = iota((WIDE, LANES), 1) < HALF
    blank = jnp.zeros((WIDE, WIDE), F32)

    def two_columns(one, two, coupling):
        head = own_columns(one, blank)
        return head, jnp.where(low_half, -dot(two, dot(coupling, head)), own_columns(blank, two))

    @pl.when(first_half)
    def _():
        head, tail = two_columns(leaf_inv(0), leaf_inv(1), coupling2(0))
        put_w(WL.at[0, :, 0], head)
        put_w(WL.at[0, :, 1], tail)

    @pl.when(core == 0)
    def _():
        z3 = put_z(3, dot(mine(3), leaf_inv(3)))
        put_z(2, dot(mine(2) - dot(z3, coupling2(1)), leaf_inv(2)))

    mark("q_rel3")
    relay(3)

    @pl.when(first_half)
    def _():
        for s in SIDES:
            net.wait(("c0", s), C0.at[:, 0])
            piece = C0.at[0 if s < 0 else 1, ys(s)]
            net.start(piece, piece, along("y", -s), "c0far", "c0far")

    mark("q_rel4")
    relay(4)
    mark("q_c0")

    @pl.when(first_half)
    def _():
        net.wait("c0pair", C0.at[0, 0])
        net.wait("c0far", C0.at[0, pl.ds(0, 2)])

    mark("r_V")

    @pl.when(first_half)
    def _():
        right = c0_pair(1)
        v3 = dot(halves(right, 1), leaf_inv(3))
        v2 = dot(halves(right, 0) - dot(v3, coupling2(1)), leaf_inv(2))
        VV[:, :WIDE] = v2
        VV[:, WIDE:] = v3
        t_send(1, own_columns(v2, v3))
        TP[...] = dot(jnp.concatenate(c0_pair(0), axis=1), WL[0].reshape(2 * WIDE, LANES))

    mark("o_arr34")
    for g in (3, 4):
        arrive(g)

    mark("p_chain2")

    @pl.when(first_half)
    def _():
        couplings = jnp.concatenate([coupling1(3), coupling1(4)], axis=0)
        SS[...] = dot(couplings, WL[0].reshape(2 * WIDE, LANES))
        t_send(0, TP[...] - dot(VV[...], SS[...]))
        t_near(1)
        w2 = put_w(WL.at[1, :, 0], -dot(leaf_inv(2), SS[:WIDE]))
        put_w(WL.at[1, :, 1], -dot(leaf_inv(3), SS[WIDE:] + dot(coupling2(1), w2)))
        head, tail = two_columns(leaf_inv(2), leaf_inv(3), coupling2(1))
        put_w(WR.at[:, 0], head)
        put_w(WR.at[:, 1], tail)
        net.start(w_rows(WL), w_rows(WL), partner, "w", "w")
        net.start(w_rows(WR), w_rows(WR), partner, "w", "w")
        t_near(0)

    @pl.when(core == 0)
    def _():
        z3, z2 = (jnp.concatenate([ZM[i], ZS[i]], axis=0) for i in (3, 2))
        both_rows = dot(z2, coupling1(3)) + dot(z3, coupling1(4))
        tiles = [both_rows[:, LANES * k:LANES * (k + 1)] for k in range(cols)]
        z1 = put_z(1, dot(mine(1) - halves(tiles, 1), leaf_inv(1)))
        put_z(0, dot(mine(0) - halves(tiles, 0) - dot(z1, coupling2(0)), leaf_inv(0)))
        net.wait("w", G.at[0, pl.ds(0, 3), 0, pl.ds(0, 2)])

    mark("s_out")

    @pl.when(first_half)
    def _():
        net.wait("z", ZM)

    o_ref[upper, far] = jnp.zeros((LANES, WIDE), F32)
    for i in range(TALL):
        lines = slice(quarter * i, quarter * (i + 1))
        o_ref[lines, :LANES] = WL[i // 2, spot, i % 2, :, hh].reshape(quarter, LANES)
        o_ref[lines, LANES:WIDE] = WR[spot, i % 2, :, hh].reshape(quarter, LANES) if i >= 2 else jnp.zeros((quarter, LANES), F32)
    o_ref[lower, far] = jnp.concatenate([own_columns(ZM[2 * n], ZM[2 * n + 1]) for n in PAIR], axis=1)

    mark("t_near")

    @pl.when(first_half)
    def _():
        t_far(1)
        t_far(0)

    mark("t_end")

    @pl.when(core == 0)
    def _():
        for side in PAIR:
            net.wait((side, "partner"), TG.at[side])

    def t_rows(i):
        return jnp.concatenate([jnp.concatenate([TG[side, b % 2, c, i, b // 2] for c in range(TALL) for b in range(BLK)], axis=0)
                                for side in PAIR], axis=1)

    mark("u_x21")
    o_ref[lower, near] = -sum(dot(ZM[i], t_rows(i)) for i in range(TALL))

    mark("v_end")
    for name in ("leaf", *LEAVES):
        net.wait(name, G.at[0, :, 0], "send")
    net.wait("rest", G.at[pl.ds(0, 2), pl.ds(0, 3), 0, pl.ds(0, 3)], "send")
    for g in REST:
        net.wait(g, G.at[pl.ds(0, 3), g], "send")
    net.wait("pair", U.at[0], "send")
    net.wait("c0", C0.at[0, pl.ds(0, 2)], "send")

    @pl.when(first_half)
    def _():
        net.wait("c0far", C0.at[0, pl.ds(0, 2)], "send")
        net.wait("t", G.at[:, pl.ds(0, 3), 0], "send")
        net.wait("tpair", TG, "send")
        net.wait("w", G.at[0, pl.ds(0, 3), 0, pl.ds(0, 2)], "send")

    @pl.when(core == 0)
    def _():
        net.wait("c0pair", C0.at[0, 0], "send")
        net.wait("z", ZM, "send")

    mark()
    counts = [len([key for key in net.names if key[0] == side]) for side in ("send", "recv")]
    assert counts == [send.shape[0], recv.shape[0]], counts


def solution(mesh):
    rows, cols = mesh.shape["row"], mesh.shape["col"]
    block_spec = P(("batch", "row"), "col")

    def device_body(local_l):
        vmem = functools.partial(pltpu.VMEM, dtype=F32)
        return pl.pallas_call(
            functools.partial(kernel, rows, cols),
            out_shape=jax.ShapeDtypeStruct(local_l.shape, F32),
            in_specs=[pl.BlockSpec(memory_space=pl.ANY)],
            out_specs=pl.BlockSpec(memory_space=pltpu.VMEM),
            scratch_shapes=[
                vmem(local_l.shape),
                vmem((2, GROUPS, TALL, BLK, LANES)),
                vmem((cols, GROUPS, 2, TALL, TALL, BLK, LANES)),
                vmem((CORES, cols, LANES, WIDE)),
                vmem((TALL, TALL * BLK, BLK, WIDE)),
                vmem((TALL, 2 * BLK, BLK, WIDE)),
                vmem((TALL, TALL * BLK, BLK, WIDE)),
                vmem((2, cols, 2, TALL, 2, BLK, LANES)),
                vmem((cols, 2, TALL, 2, BLK, LANES)),
                vmem((TALL, LANES, WIDE)),
                vmem((TALL, LANES, WIDE)),
                vmem((2, 2, TALL, TALL, TALL, BLK, LANES)),
                vmem((WIDE, 2 * WIDE)),
                vmem((2 * WIDE, LANES)),
                vmem((WIDE, LANES)),
                pltpu.SemaphoreType.DMA((3,)),
                pltpu.SemaphoreType.DMA((15,)),
                pltpu.SemaphoreType.DMA((45,)),
            ],
            compiler_params=pltpu.CompilerParams(collective_id=0, has_side_effects=True),
        )(local_l)

    return jax.shard_map(device_body, mesh=mesh, in_specs=(block_spec,), out_specs=block_spec, check_vma=False)
```

```python
import functools

import jax
import jax.numpy as jnp
from jax import lax
from jax.experimental import pallas as pl
from jax.experimental.pallas import tpu as pltpu
from jax.sharding import PartitionSpec as P

BLK = 8
CORES = 2
LANES = 128
HALF = LANES // 2
WIDE = 2 * LANES
TALL = 4
GROUPS = 5
LEAVES = range(2)
PAIR = range(2)
SIDES = (-1, 1)
MESH = pl.DeviceIdType.MESH


class Marks:
    def __init__(self):
        self.scope = None

    def __call__(self, name=None):
        if self.scope is not None:
            self.scope.__exit__(None, None, None)
        self.scope = None if name is None else jax.named_scope(name)
        if name is not None:
            self.scope.__enter__()
F32 = jnp.float32


def dot(left, right):
    return jnp.dot(left, right, precision=lax.Precision.HIGHEST, preferred_element_type=F32)


def iota(shape, dim):
    return lax.broadcasted_iota(jnp.int32, shape, dim)


def halves(tiles, half):
    low = iota(tiles[0].shape, 1) < HALF
    out = []
    for first, second in ((tiles[0], tiles[1]), (tiles[2], tiles[3])):
        if half == 0:
            out.append(jnp.where(low, first, pltpu.roll(second, HALF, 1)))
        else:
            out.append(jnp.where(low, pltpu.roll(first, HALF, 1), second))
    return jnp.concatenate(out, axis=1)


class Net:
    def __init__(self, send, recv):
        self.send, self.recv, self.names = send, recv, {}

    def slot(self, side, name):
        held = [key for key in self.names if key[0] == side]
        return self.names.setdefault((side, name), len(held))

    def start(self, src, dst, device, send, recv):
        self.make(src, dst, device, send, recv).start()

    def make(self, src, dst, device, send, recv):
        return pltpu.make_async_remote_copy(
            src_ref=src, dst_ref=dst, send_sem=self.send.at[self.slot("send", send)], recv_sem=self.recv.at[self.slot("recv", recv)],
            device_id=device, device_id_type=MESH)

    def wait(self, name, like, side="recv"):
        sems = self.recv if side == "recv" else self.send
        pltpu.make_async_copy(like, like, sems.at[self.slot(side, name)]).wait()


def shift(val, lanes):
    return jnp.concatenate([pltpu.roll(val[:, LANES * i:LANES * (i + 1)], lanes % LANES, 1) for i in range(2)], axis=1)


def kernel(rows, cols, hbm_ref, o_ref, l_ref, U, G, C0, LF, PK, LI, WL, WR, ZM, ZS, TG, SX, YX, VV, SS, TP, load, send, recv):
    chips = rows // CORES
    row = lax.axis_index("row")
    y = lax.axis_index("col")
    x, core = row // CORES, row % CORES
    spot, hh = row % cols, row // cols
    net = Net(send, recv)
    first_half = core == 1

    def at(xx, cc, yy):
        return {"row": xx * CORES + cc, "col": yy}

    def xs(step):
        return lax.rem(x + step + chips, chips)

    def ys(step):
        return lax.rem(y + step + cols, cols)

    def along(axis, step, cc=core):
        return at(xs(step), cc, y) if axis == "x" else at(x, cc, ys(step))

    mark = Marks()
    mark("a_signal")
    upper, lower, near, far = pl.ds(0, LANES), pl.ds(LANES, LANES), pl.ds(0, WIDE), pl.ds(WIDE, WIDE)
    windows = [(upper, near), (lower, far), (lower, near)]
    loads = [pltpu.make_async_copy(hbm_ref.at[w], l_ref.at[w], load.at[i]) for i, w in enumerate(windows)]
    for made in loads:
        made.start()
    partner = at(x, 1 - core, y)
    barrier = pltpu.get_barrier_semaphore()
    peers = [partner] + [along(axis, d, cc) for axis in "xy" for d in range(1, chips) for cc in range(CORES)]
    for peer in peers:
        pl.semaphore_signal(barrier, inc=1, device_id=peer, device_id_type=MESH)

    mark("a_pack")
    quarter = LANES // TALL
    for part in range(2):
        loads[part].wait()
        piece = l_ref[part * LANES:(part + 1) * LANES, part * WIDE:(part + 1) * WIDE]
        low = iota((quarter, LANES), 1) < HALF
        band = [piece[quarter * i:quarter * (i + 1)] for i in range(TALL)]
        packed = [jnp.where(low, band[2 * m][:, LANES * m:LANES * (m + 1)], band[2 * m + 1][:, LANES * m:LANES * (m + 1)])
                  for m in PAIR]
        packed.append(jnp.where(low, band[1][:, :LANES], pltpu.roll(band[3][:, LANES:], HALF, 1)))
        packed += [band[2][:, :LANES], band[3][:, :LANES]]
        tiles = [val.reshape(TALL, BLK, LANES) for val in packed]
        for g in range(GROUPS):
            U[part, g] = tiles[g]

        @pl.when(core == 1 - part)
        def _():
            for g in range(GROUPS):
                G[y, g, hh, spot] = tiles[g]

    loads[2].wait()
    C0[core, y] = l_ref[lower, near]
    mark("b_barrier")
    pl.semaphore_wait(barrier, len(peers))

    axis_first = ["x", "y", "y"]

    def other(axis):
        return "y" if axis == "x" else "x"

    def source(g, f, s, k=None):
        xx, yy = (xs(f), ys(s)) if axis_first[g] == "x" else (xs(s), ys(f))
        return G.at[yy, g, xx // 2, pl.ds(2 * (xx % 2), 2) if k is None else 2 * (xx % 2) + k]

    def pass_on(g, f, s, k, step, name):
        piece = source(g, f, s, k)
        net.start(piece, piece, along(other(axis_first[g]), step), g, name)

    def pass_leaf(g, f):
        for s in SIDES:
            pass_on(g, f, 0, None, -s, (g, "far") if f == 2 else (g, f, s))
        if f == 2:
            pass_on(g, f, 0, None, 2, (g, "far"))

    def half_on(g, f, s):
        pass_on(g, f, s, 0 if s < 0 else 1, -s, (g, "far"))

    mark("d_own")
    for axis in "xy":
        for step in SIDES:
            for part in range(2):
                net.start(U.at[part, pl.ds(0, 2)], G.at[y, pl.ds(0, 2), hh, spot], along(axis, step, 1 - part), "leaf", (axis, -step))
    for g in LEAVES:
        for part in range(2):
            net.start(U.at[part, g], G.at[y, g, hh, spot], along(axis_first[g], 2, 1 - part), "leaf", (g, "two"))
    net.start(U.at[core], G.at[y, :, hh, spot], partner, "pair", "pair")

    mark("e_near")
    for step in SIDES:
        for axis in "xy":
            net.wait((axis, step), G.at[0, pl.ds(0, 2), 0, pl.ds(0, 2)])
            for g in LEAVES:
                if axis_first[g] == axis:
                    pass_leaf(g, step)
                else:
                    half_on(g, 0, step)
    for d in range(1, chips):
        for part in range(2):
            net.start(U.at[part, 2], G.at[y, 2, hh, spot], along(axis_first[2], d, 1 - part), "rest", (2, "first"))
    mark("f_pair")
    net.wait("pair", U.at[0])
    mark("g_two")
    for g in LEAVES:
        net.wait((g, "two"), G.at[0, 0, 0, pl.ds(0, 2)])
        pass_leaf(g, 2)
    mark("h_diag")
    for f in SIDES:
        for s in SIDES:
            for g in LEAVES:
                net.wait((g, f, s), source(g, f, s))
                half_on(g, f, s)

    def bundle(g, step, part=None):
        if axis_first[g] == "x":
            return G.at[ys(step), g] if part is None else G.at[ys(step), g, part]
        xx = xs(step)
        return G.at[slice(None) if part is None else pl.ds(2 * part, 2), g, xx // 2, pl.ds(2 * (xx % 2), 2)]

    def send_second(g):
        net.wait((g, "first"), G.at[0, pl.ds(0, 3), 0, pl.ds(0, 2)])
        for s in SIDES:
            net.start(bundle(g, 0), bundle(g, 0), along(other(axis_first[g]), -s), g, (g, "near", s))

    def relay(g):
        for s in SIDES:
            net.wait((g, "near", s), G.at[0, g])
            half = bundle(g, s, 0 if s < 0 else 1)
            net.start(half, half, along(other(axis_first[g]), -s), g, (g, "end"))

    def arrive(g):
        net.wait((g, "end"), G.at[0, g])

    mark("j_second")
    for s in SIDES:
        net.start(l_ref.at[lower, near], C0.at[core, y], along("y", -s, 1), "c0", ("c0", s))

    @pl.when(core == 0)
    def _():
        net.start(l_ref.at[lower, near], C0.at[core, y], partner, "c0pair", "c0pair")

    for d in range(1, chips):
        for part, axis in enumerate("yx"):
            net.start(U.at[part, pl.ds(3, 2)], G.at[y, pl.ds(3, 2), hh, spot], along(axis, d, 1 - part), "rest", "c1")
    send_second(2)

    mark("k_leafin")
    for g in LEAVES:
        net.wait((g, "far"), G.at[pl.ds(0, 3), g, 0])

    mark("l_base")
    lane = iota((BLK, LANES), 1)
    sub = iota((BLK, LANES), 0)
    block_of = (lane // BLK) % BLK
    diag = [[[None] * TALL for _ in range(TALL)] for _ in PAIR]
    inv = [[[None] * TALL for _ in range(TALL)] for _ in PAIR]
    for m in PAIR:
        for c in range(TALL):
            for k in range(c + 1):
                total = jnp.zeros((BLK, LANES), F32)
                for b in range(BLK):
                    total = jnp.where(block_of == b, G[k, m, b % 2, c, b // 2], total)
                diag[m][c][k] = total
                inv[m][c][k] = jnp.where(sub == lane % BLK, 1.0, 0.0) if c == k else jnp.zeros((BLK, LANES), F32)
    for t in range(BLK * TALL):
        ct, jt = t // BLK, t % BLK
        index = (lane // BLK) * BLK + jt
        for m in PAIR:
            spread = [jnp.take_along_axis(diag[m][c][ct], index, axis=1) for c in range(ct, TALL)]
            pivot = 1.0 / spread[0][jt:jt + 1, :]
            below = jnp.where(sub > jt, spread[0], 0.0)
            for k in range(ct + 1):
                solved = inv[m][ct][k][jt:jt + 1, :] * pivot
                inv[m][ct][k] = jnp.where(sub == jt, solved, inv[m][ct][k] - below * solved)
                for c in range(ct + 1, TALL):
                    inv[m][c][k] = inv[m][c][k] - spread[c - ct] * solved
    for m in PAIR:
        for c in range(TALL):
            tiles = [inv[m][c][k] if k <= c else jnp.zeros((BLK, LANES), F32) for k in range(TALL)]
            for e in PAIR:
                PK[2 * m + e, c] = halves(tiles, e)

    def gathered(k, g):
        return jnp.concatenate([G[k, g, b % 2, c, b // 2] for c in range(TALL) for b in range(BLK)], axis=0)

    mark("m_sep")
    for m in PAIR:
        tiles = [gathered(k, m) for k in range(cols)]
        for e in PAIR:
            LF[2 * m + e] = halves(tiles, e).reshape(TALL * BLK, BLK, WIDE)

    def double(m, nb):
        count, lanes = TALL * nb, BLK * nb
        size = BLK * count
        group = ((iota((BLK, WIDE), 1) % HALF) // BLK) // nb
        even = ((iota((size, WIDE), 1) % HALF) // BLK) // nb % 2 == 0

        def coupling(leaf):
            out = []
            for bb in range(nb):
                for c in range(TALL):
                    total = LF[leaf, c * BLK + nb + bb]
                    for s in range(3, BLK // nb, 2):
                        total = jnp.where(group == s - 1, LF[leaf, c * BLK + s * nb + bb], total)
                    out.append(total)
            return jnp.concatenate(out, axis=0)

        def spread(val, flip):
            tiles = val.reshape(count, BLK, WIDE)
            return jnp.concatenate([jnp.where(group == (b // nb) ^ flip, tiles[(b % nb) * TALL + c], 0.0)
                                    for c in range(TALL) for b in range(BLK)], axis=0)

        one, two = (PK[2 * m + e, 0:count].reshape(size, WIDE) for e in PAIR)
        temp = dot(jnp.where(even, coupling(2 * m), shift(coupling(2 * m + 1), lanes)),
                   spread(jnp.where(even, one, shift(two, lanes)), 0))
        corner = dot(jnp.where(even, shift(two, -lanes), one), spread(temp, 1))
        for e, (val, low) in enumerate(((one, corner), (two, shift(corner, -lanes)))):
            parts = (jnp.where(even, val, 0.0), jnp.where(even, -low, val))
            for half in PAIR:
                tiles = parts[half].reshape(count, BLK, WIDE)
                if nb < TALL:
                    PK[2 * m + e, half * count:(half + 1) * count] = tiles
                else:
                    for i in range(count):
                        LI[2 * m + e, (i % TALL) * BLK + half * TALL + i // TALL] = tiles[i]

    mark("n_dbl1")
    for m in PAIR:
        double(m, 1)
    mark("n_rel2")
    relay(2)
    mark("n_dbl2")
    for m in PAIR:
        double(m, 2)
    mark("n_relc0")

    @pl.when(first_half)
    def _():
        for s in SIDES:
            net.wait(("c0", s), C0.at[:, 0])
            piece = C0.at[0 if s < 0 else 1, ys(s)]
            net.start(piece, piece, along("y", -s), "c0far", "c0far")

    mark("n_dbl4")
    for m in PAIR:
        double(m, 4)
    mark("o_arr2")
    arrive(2)

    def leaf_inv(i):
        return LI[i].reshape(WIDE, WIDE)

    def coupling2(m):
        return halves([gathered(k, 2) for k in range(cols)], m)

    def mine(i):
        r, l = iota((WIDE, WIDE), 0), iota((WIDE, WIDE), 1)
        own = CORES * x + r // LANES
        return jnp.where(((r // quarter) % TALL == i) & (l // HALF == own % cols) & (r % BLK == l % BLK)
                         & ((l % HALF) // BLK == 2 * ((r // BLK) % TALL) + own // cols), 1.0, 0.0)

    def put_w(ref, val):
        ref[...] = val.reshape(TALL, TALL, 2, BLK, LANES)
        return val

    def put_z(i, val):
        ZM[i] = val[:LANES]
        ZS[i] = val[LANES:]
        net.start(ZS.at[i], ZM.at[i], partner, "z", "z")
        return val

    def t_piece(side, step, k=None):
        xx = xs(step)
        return TG.at[side, xx // 2, pl.ds(2 * (xx % 2), 2) if k is None else 2 * (xx % 2) + k]

    def t_start(side, step, k, device, name, kind="t"):
        net.start(t_piece(side, step, k), t_piece(side, step, k), device, kind, (side, name))

    def t_send(side, val):
        t_piece(side, 0)[...] = val.reshape(CORES, TALL, TALL, BLK, LANES)
        for i in PAIR:
            for s in SIDES:
                k = i if s < 0 else 1 - i
                t_start(side, 0, k, along("x", -s), (s, i))
        t_start(side, 0, None, partner, "partner", "tpair")

    def t_near(side):
        for i in PAIR:
            for s in SIDES:
                k = i if s < 0 else 1 - i
                net.wait((side, (s, i)), t_piece(side, s, k))
                if i == 0:
                    t_start(side, s, k, along("x", -s), "far")
                t_start(side, s, k, partner, "partner", "tpair")

    def t_far(side):
        net.wait((side, "far"), t_piece(side, 2))
        t_start(side, 2, None, partner, "partner", "tpair")

    def c0_pair(n):
        return [jnp.concatenate([C0[k, c, :, LANES * n:LANES * (n + 1)] for k in range(CORES)], axis=0) for c in range(cols)]

    def own_columns(first, second):
        low = iota((first.shape[0], LANES), 1) < HALF
        out = []
        for val in (first, second):
            tile = jnp.where(y // 2 == 0, val[:, :LANES], val[:, LANES:])
            moved = pltpu.roll(tile, HALF, 1)
            out.append(jnp.where(y % 2 == 0, tile, moved) if val is first else jnp.where(y % 2 == 0, moved, tile))
        return jnp.where(low, out[0], out[1])

    def w_rows(ref):
        own = CORES * x
        return ref.at[..., own % cols, :, :, own // cols, :, :]

    mark("p_chain1")
    low_half = iota((WIDE, LANES), 1) < HALF
    blank = jnp.zeros((WIDE, WIDE), F32)

    def two_columns(one, two, coupling):
        head = own_columns(one, blank)
        return head, jnp.where(low_half, -dot(two, dot(coupling, head)), own_columns(blank, two))

    @pl.when(first_half)
    def _():
        head, tail = two_columns(leaf_inv(0), leaf_inv(1), coupling2(0))
        put_w(WL.at[0, :, 0], head)
        put_w(WL.at[0, :, 1], tail)

    @pl.when(core == 0)
    def _():
        z3 = put_z(3, dot(mine(3), leaf_inv(3)))
        put_z(2, dot(mine(2) - dot(z3, coupling2(1)), leaf_inv(2)))

    mark("q_c1")
    net.wait("c1", G.at[pl.ds(0, 3), 0, 0])

    def x_piece(step):
        xx = xs(step)
        return SX.at[xx // 2, pl.ds(2 * (xx % 2), 2)]

    @pl.when(first_half)
    def _():
        def own_rows(k):
            return jnp.concatenate(
                [G[k, g, x // 2, 2 * (x % 2) + kk, a] for kk in range(CORES) for g in (3, 4) for a in range(TALL)], axis=0)

        product = dot(jnp.concatenate([own_rows(k) for k in range(cols)], axis=1), WL[0].reshape(2 * WIDE, LANES))
        x_piece(0)[...] = product.reshape(CORES, 2, TALL, BLK, LANES)
        for d in range(1, chips):
            net.start(x_piece(0), x_piece(0), along("x", d), "share", "share")

    @pl.when(core == 0)
    def _():
        lhs = [jnp.concatenate([ZM[i, HALF:], ZS[i, HALF:]], axis=0) for i in (2, 3)]
        YX[y] = sum(dot(lhs[i], gathered(y, 3 + i)) for i in PAIR)
        for d in range(1, cols):
            net.start(YX.at[y], YX.at[y], along("y", d), "share", "share")

    mark("q_c0")

    @pl.when(first_half)
    def _():
        net.wait("c0pair", C0.at[0, 0])
        net.wait("c0far", C0.at[0, pl.ds(0, 2)])

    mark("r_V")

    @pl.when(first_half)
    def _():
        right = c0_pair(1)
        v3 = dot(halves(right, 1), leaf_inv(3))
        v2 = dot(halves(right, 0) - dot(v3, coupling2(1)), leaf_inv(2))
        VV[:, :WIDE] = v2
        VV[:, WIDE:] = v3
        t_send(1, own_columns(v2, v3))
        TP[...] = dot(jnp.concatenate(c0_pair(0), axis=1), WL[0].reshape(2 * WIDE, LANES))

    mark("o_share")
    net.wait("share", G.at[pl.ds(0, 3), 0, 0])
    mark("p_chain2")

    @pl.when(first_half)
    def _():
        for g in PAIR:
            for c in range(TALL):
                for i in range(BLK):
                    SS[(g * TALL + c) * BLK + i] = SX[i % 2, c, g, i // 2]
        shared = SS[...].reshape(2 * WIDE, LANES)
        t_send(0, TP[...] - dot(VV[...], shared))
        t_near(1)
        w2 = put_w(WL.at[1, :, 0], -dot(leaf_inv(2), shared[:WIDE]))
        put_w(WL.at[1, :, 1], -dot(leaf_inv(3), shared[WIDE:] + dot(coupling2(1), w2)))
        head, tail = two_columns(leaf_inv(2), leaf_inv(3), coupling2(1))
        put_w(WR.at[:, 0], head)
        put_w(WR.at[:, 1], tail)
        net.start(w_rows(WL), w_rows(WL), partner, "w", "w")
        net.start(w_rows(WR), w_rows(WR), partner, "w", "w")
        t_near(0)

    @pl.when(core == 0)
    def _():
        none = jnp.zeros((HALF, LANES), F32)
        tiles = [jnp.concatenate([none, YX[k, :HALF], none, YX[k, HALF:]], axis=0) for k in range(cols)]
        z1 = put_z(1, dot(mine(1) - halves(tiles, 1), leaf_inv(1)))
        put_z(0, dot(mine(0) - halves(tiles, 0) - dot(z1, coupling2(0)), leaf_inv(0)))
        net.wait("w", G.at[0, pl.ds(0, 3), 0, pl.ds(0, 2)])

    mark("s_out")

    @pl.when(first_half)
    def _():
        net.wait("z", ZM)

    o_ref[upper, far] = jnp.zeros((LANES, WIDE), F32)
    for i in range(TALL):
        lines = slice(quarter * i, quarter * (i + 1))
        o_ref[lines, :LANES] = WL[i // 2, spot, i % 2, :, hh].reshape(quarter, LANES)
        o_ref[lines, LANES:WIDE] = WR[spot, i % 2, :, hh].reshape(quarter, LANES) if i >= 2 else jnp.zeros((quarter, LANES), F32)
    o_ref[lower, far] = jnp.concatenate([own_columns(ZM[2 * n], ZM[2 * n + 1]) for n in PAIR], axis=1)

    mark("t_near")

    @pl.when(first_half)
    def _():
        t_far(1)
        t_far(0)

    mark("t_end")

    @pl.when(core == 0)
    def _():
        for side in PAIR:
            net.wait((side, "partner"), TG.at[side])

    def t_rows(i):
        return jnp.concatenate([jnp.concatenate([TG[side, b % 2, c, i, b // 2] for c in range(TALL) for b in range(BLK)], axis=0)
                                for side in PAIR], axis=1)

    mark("u_x21")
    o_ref[lower, near] = -sum(dot(ZM[i], t_rows(i)) for i in range(TALL))

    mark("v_end")
    for name in ("leaf", *LEAVES):
        net.wait(name, G.at[0, :, 0], "send")
    net.wait("rest", G.at[pl.ds(0, 2), pl.ds(0, 3), 0, pl.ds(0, 3)], "send")
    net.wait(2, G.at[pl.ds(0, 3), 2], "send")
    net.wait("share", G.at[pl.ds(0, 3), 0, 0], "send")
    net.wait("pair", U.at[0], "send")
    net.wait("c0", C0.at[0, pl.ds(0, 2)], "send")

    @pl.when(first_half)
    def _():
        net.wait("c0far", C0.at[0, pl.ds(0, 2)], "send")
        net.wait("t", G.at[:, pl.ds(0, 3), 0], "send")
        net.wait("tpair", TG, "send")
        net.wait("w", G.at[0, pl.ds(0, 3), 0, pl.ds(0, 2)], "send")

    @pl.when(core == 0)
    def _():
        net.wait("c0pair", C0.at[0, 0], "send")
        net.wait("z", ZM, "send")

    mark()
    counts = [len([key for key in net.names if key[0] == side]) for side in ("send", "recv")]
    assert counts == [send.shape[0], recv.shape[0]], counts


def solution(mesh):
    rows, cols = mesh.shape["row"], mesh.shape["col"]
    block_spec = P(("batch", "row"), "col")

    def device_body(local_l):
        vmem = functools.partial(pltpu.VMEM, dtype=F32)
        return pl.pallas_call(
            functools.partial(kernel, rows, cols),
            out_shape=jax.ShapeDtypeStruct(local_l.shape, F32),
            in_specs=[pl.BlockSpec(memory_space=pl.ANY)],
            out_specs=pl.BlockSpec(memory_space=pltpu.VMEM),
            scratch_shapes=[
                vmem(local_l.shape),
                vmem((2, GROUPS, TALL, BLK, LANES)),
                vmem((cols, GROUPS, 2, TALL, TALL, BLK, LANES)),
                vmem((CORES, cols, LANES, WIDE)),
                vmem((TALL, TALL * BLK, BLK, WIDE)),
                vmem((TALL, 2 * BLK, BLK, WIDE)),
                vmem((TALL, TALL * BLK, BLK, WIDE)),
                vmem((2, cols, 2, TALL, 2, BLK, LANES)),
                vmem((cols, 2, TALL, 2, BLK, LANES)),
                vmem((TALL, LANES, WIDE)),
                vmem((TALL, LANES, WIDE)),
                vmem((2, 2, TALL, TALL, TALL, BLK, LANES)),
                vmem((2, TALL, 2, TALL, BLK, LANES)),
                vmem((cols, LANES, LANES)),
                vmem((WIDE, 2 * WIDE)),
                vmem((2 * TALL * BLK, BLK, LANES)),
                vmem((WIDE, LANES)),
                pltpu.SemaphoreType.DMA((3,)),
                pltpu.SemaphoreType.DMA((14,)),
                pltpu.SemaphoreType.DMA((39,)),
            ],
            compiler_params=pltpu.CompilerParams(collective_id=0, has_side_effects=True),
        )(local_l)

    return jax.shard_map(device_body, mesh=mesh, in_specs=(block_spec,), out_specs=block_spec, check_vma=False)
```

```python
import functools

import jax
import jax.numpy as jnp
from jax import lax
from jax.experimental import pallas as pl
from jax.experimental.pallas import tpu as pltpu
from jax.sharding import PartitionSpec as P

BLK = 8
CORES = 2
LANES = 128
HALF = LANES // 2
WIDE = 2 * LANES
TALL = 4
GROUPS = 10
LEAD = (0, 1)
REST = (4, 5, 2, 3)
PAIR = range(2)
SIDES = (-1, 1)
MESH = pl.DeviceIdType.MESH


class Marks:
    def __init__(self):
        self.scope = None

    def __call__(self, name=None):
        if self.scope is not None:
            self.scope.__exit__(None, None, None)
        self.scope = None if name is None else jax.named_scope(name)
        if name is not None:
            self.scope.__enter__()
F32 = jnp.float32


def dot(left, right):
    return jnp.dot(left, right, precision=lax.Precision.HIGHEST, preferred_element_type=F32)


def iota(shape, dim):
    return lax.broadcasted_iota(jnp.int32, shape, dim)


def halves(tiles, half):
    low = iota(tiles[0].shape, 1) < HALF
    out = []
    for first, second in ((tiles[0], tiles[1]), (tiles[2], tiles[3])):
        if half == 0:
            out.append(jnp.where(low, first, pltpu.roll(second, HALF, 1)))
        else:
            out.append(jnp.where(low, pltpu.roll(first, HALF, 1), second))
    return jnp.concatenate(out, axis=1)


class Net:
    def __init__(self, send, recv):
        self.send, self.recv, self.names = send, recv, {}

    def slot(self, side, name):
        held = [key for key in self.names if key[0] == side]
        return self.names.setdefault((side, name), len(held))

    def start(self, src, dst, device, send, recv):
        self.make(src, dst, device, send, recv).start()

    def make(self, src, dst, device, send, recv):
        return pltpu.make_async_remote_copy(
            src_ref=src, dst_ref=dst, send_sem=self.send.at[self.slot("send", send)], recv_sem=self.recv.at[self.slot("recv", recv)],
            device_id=device, device_id_type=MESH)

    def wait(self, name, like, side="recv"):
        sems = self.recv if side == "recv" else self.send
        pltpu.make_async_copy(like, like, sems.at[self.slot(side, name)]).wait()


def shift(val, lanes):
    return jnp.concatenate([pltpu.roll(val[:, LANES * i:LANES * (i + 1)], lanes % LANES, 1) for i in range(2)], axis=1)


def kernel(rows, cols, hbm_ref, o_ref, l_ref, U, G, C0, LF, PK, LI, WL, WR, ZM, ZS, TG, SX, YX, VV, SS, TP, load, send, recv):
    chips = rows // CORES
    row = lax.axis_index("row")
    y = lax.axis_index("col")
    x, core = row // CORES, row % CORES
    spot, hh = row % cols, row // cols
    net = Net(send, recv)
    first_half = core == 1

    def at(xx, cc, yy):
        return {"row": xx * CORES + cc, "col": yy}

    def xs(step):
        return lax.rem(x + step + chips, chips)

    def ys(step):
        return lax.rem(y + step + cols, cols)

    def along(axis, step, cc=core):
        return at(xs(step), cc, y) if axis == "x" else at(x, cc, ys(step))

    mark = Marks()
    mark("a_signal")
    upper, lower, near, far = pl.ds(0, LANES), pl.ds(LANES, LANES), pl.ds(0, WIDE), pl.ds(WIDE, WIDE)
    windows = [(upper, near), (lower, far), (lower, near)]
    loads = [pltpu.make_async_copy(hbm_ref.at[w], l_ref.at[w], load.at[i]) for i, w in enumerate(windows)]
    for made in loads:
        made.start()
    partner = at(x, 1 - core, y)
    barrier = pltpu.get_barrier_semaphore()
    peers = [partner] + [along(axis, d, cc) for axis in "xy" for d in range(1, chips) for cc in range(CORES)]
    for peer in peers:
        pl.semaphore_signal(barrier, inc=1, device_id=peer, device_id_type=MESH)

    mark("a_pack")
    quarter = LANES // TALL
    for part in range(2):
        loads[part].wait()
        piece = l_ref[part * LANES:(part + 1) * LANES, part * WIDE:(part + 1) * WIDE]
        low = iota((quarter, LANES), 1) < HALF
        band = [piece[quarter * i:quarter * (i + 1)] for i in range(TALL)]
        packed = [jnp.where(low, band[2 * m][:, LANES * m:LANES * (m + 1)], band[2 * m + 1][:, LANES * m:LANES * (m + 1)])
                  for m in PAIR]
        packed.append(jnp.where(low, band[1][:, :LANES], pltpu.roll(band[3][:, LANES:], HALF, 1)))
        packed += [band[2][:, :LANES], band[3][:, :LANES]]
        if part:
            packed[:2] = packed[1::-1]
        tiles = [val.reshape(2, 2, BLK, LANES)[i] for val in packed for i in PAIR]
        for g in range(GROUPS):
            U[part, g] = tiles[g]

        @pl.when(core == 1 - part)
        def _():
            for g in range(GROUPS):
                G[y, g, hh, spot] = tiles[g]

    loads[2].wait()
    C0[core, y] = l_ref[lower, near]
    mark("b_barrier")
    pl.semaphore_wait(barrier, len(peers))

    axis_first = "xy" * 3

    def other(axis):
        return "y" if axis == "x" else "x"

    def source(g, f, s, k=None):
        xx, yy = (xs(f), ys(s)) if axis_first[g] == "x" else (xs(s), ys(f))
        return G.at[yy, g, xx // 2, pl.ds(2 * (xx % 2), 2) if k is None else 2 * (xx % 2) + k]

    def pass_on(g, f, s, k, step, name):
        piece = source(g, f, s, k)
        net.start(piece, piece, along(other(axis_first[g]), step), "on", name)

    def pass_leaf(g, f):
        for s in SIDES:
            pass_on(g, f, 0, None, -s, (g, "far") if f == 2 else (g, f, s))
        if f == 2:
            pass_on(g, f, 0, None, 2, (g, "far"))

    def half_on(g, f, s):
        pass_on(g, f, s, 0 if s < 0 else 1, -s, (g, "far"))

    def own(groups, name):
        lo, count = min(groups), len(groups)
        for axis in "xy":
            for step in SIDES:
                for part in range(2):
                    net.start(U.at[part, pl.ds(lo, count)], G.at[y, pl.ds(lo, count), hh, spot], along(axis, step, 1 - part),
                              name, (name, axis, -step))
        for g in groups:
            for part in range(2):
                net.start(U.at[part, g], G.at[y, g, hh, spot], along(axis_first[g], 2, 1 - part), name, (g, "two"))

    def near_by(groups, name):
        for step in SIDES:
            for axis in "xy":
                net.wait((name, axis, step), G.at[0, pl.ds(0, len(groups)), 0, pl.ds(0, 2)])
                for g in groups:
                    if axis_first[g] == axis:
                        pass_leaf(g, step)
                    else:
                        half_on(g, 0, step)

    def two_away(groups):
        for g in groups:
            net.wait((g, "two"), G.at[0, 0, 0, pl.ds(0, 2)])
            pass_leaf(g, 2)

    def across(groups):
        for f in SIDES:
            for s in SIDES:
                for g in groups:
                    net.wait((g, f, s), source(g, f, s))
                    half_on(g, f, s)

    def arrive(groups):
        for g in groups:
            net.wait((g, "far"), G.at[pl.ds(0, 3), g, 0])

    mark("d_own")
    own(LEAD, "lead")
    net.start(U.at[core], G.at[y, :, hh, spot], partner, "pair", "pair")
    mark("e_near")
    near_by(LEAD, "lead")
    own(REST, "rest")
    mark("g_two")
    two_away(LEAD)
    mark("h_diag")
    across(LEAD)
    net.wait("pair", U.at[0])
    mark("i_near2")
    near_by(REST, "rest")
    mark("j_more")
    for d in range(1, chips):
        for part, axis in enumerate("yx"):
            net.start(U.at[part, pl.ds(6, TALL)], G.at[y, pl.ds(6, TALL), hh, spot], along(axis, d, 1 - part), "c1", "c1")
    for s in SIDES:
        net.start(l_ref.at[lower, near], C0.at[core, y], along("y", -s, 1), "c0", ("c0", s))

    @pl.when(core == 0)
    def _():
        net.start(l_ref.at[lower, near], C0.at[core, y], partner, "c0pair", "c0pair")

    mark("k_leafin")
    arrive(LEAD)

    lane = iota((BLK, LANES), 1)
    sub = iota((BLK, LANES), 0)
    block_of = (lane // BLK) % BLK

    def tile_of(k, q, c, b):
        return G[k, 2 * q + b // TALL, b % 2, c, (b // 2) % 2]

    def gathered(k, q):
        return jnp.concatenate([tile_of(k, q, c, b) for c in range(TALL) for b in range(BLK)], axis=0)

    def start_leaves(m):
        zero = jnp.zeros((BLK, LANES), F32)
        diag = [[None] * TALL for _ in range(TALL)]
        inv = [[zero] * TALL for _ in range(TALL)]
        for c in range(TALL):
            inv[c][c] = jnp.where(sub == lane % BLK, 1.0, 0.0)
            for k in range(c + 1):
                total = zero
                for b in range(BLK):
                    total = jnp.where(block_of == b, tile_of(k, m, c, b), total)
                diag[c][k] = total
        for t in range(BLK * TALL):
            ct, jt = t // BLK, t % BLK
            index = (lane // BLK) * BLK + jt
            spread = [jnp.take_along_axis(diag[c][ct], index, axis=1) for c in range(ct, TALL)]
            pivot = 1.0 / spread[0][jt:jt + 1, :]
            below = jnp.where(sub > jt, spread[0], 0.0)
            for k in range(ct + 1):
                solved = inv[ct][k][jt:jt + 1, :] * pivot
                inv[ct][k] = jnp.where(sub == jt, solved, inv[ct][k] - below * solved)
                for c in range(ct + 1, TALL):
                    inv[c][k] = inv[c][k] - spread[c - ct] * solved
        full = [gathered(k, m) for k in range(cols)]
        for e in PAIR:
            LF[2 * m + e] = halves(full, e).reshape(TALL * BLK, BLK, WIDE)
            for c in range(TALL):
                PK[2 * m + e, c] = halves(inv[c], e)

    def double(m, nb):
        count, lanes = TALL * nb, BLK * nb
        size = BLK * count
        group = ((iota((BLK, WIDE), 1) % HALF) // BLK) // nb
        even = ((iota((size, WIDE), 1) % HALF) // BLK) // nb % 2 == 0

        def coupling(leaf):
            out = []
            for bb in range(nb):
                for c in range(TALL):
                    total = LF[leaf, c * BLK + nb + bb]
                    for s in range(3, BLK // nb, 2):
                        total = jnp.where(group == s - 1, LF[leaf, c * BLK + s * nb + bb], total)
                    out.append(total)
            return jnp.concatenate(out, axis=0)

        def spread(val, flip):
            tiles = val.reshape(count, BLK, WIDE)
            return jnp.concatenate([jnp.where(group == (b // nb) ^ flip, tiles[(b % nb) * TALL + c], 0.0)
                                    for c in range(TALL) for b in range(BLK)], axis=0)

        one, two = (PK[2 * m + e, 0:count].reshape(size, WIDE) for e in PAIR)
        temp = dot(jnp.where(even, coupling(2 * m), shift(coupling(2 * m + 1), lanes)),
                   spread(jnp.where(even, one, shift(two, lanes)), 0))
        corner = dot(jnp.where(even, shift(two, -lanes), one), spread(temp, 1))
        for e, (val, low) in enumerate(((one, corner), (two, shift(corner, -lanes)))):
            parts = (jnp.where(even, val, 0.0), jnp.where(even, -low, val))
            for half in PAIR:
                tiles = parts[half].reshape(count, BLK, WIDE)
                if nb < TALL:
                    PK[2 * m + e, half * count:(half + 1) * count] = tiles
                else:
                    for i in range(count):
                        LI[2 * m + e, (i % TALL) * BLK + half * TALL + i // TALL] = tiles[i]

    mark("l_base")
    start_leaves(0)
    mark("n_dbl1")
    double(0, 1)
    mark("n_two2")
    two_away(REST)
    mark("n_dbl2")
    double(0, 2)
    mark("n_diag2")
    across(REST)
    mark("n_dbl4")
    double(0, TALL)
    mark("o_arr2")
    arrive(REST[:2])

    def leaf_inv(i):
        return LI[i].reshape(WIDE, WIDE)

    def turned(i):
        return leaf_inv((i + 2) % TALL)

    def coupling2(m):
        return halves([gathered(k, 2) for k in range(cols)], m)

    def mine(i):
        r, l = iota((WIDE, WIDE), 0), iota((WIDE, WIDE), 1)
        own = CORES * x + r // LANES
        return jnp.where(((r // quarter) % TALL == i) & (l // HALF == own % cols) & (r % BLK == l % BLK)
                         & ((l % HALF) // BLK == 2 * ((r // BLK) % TALL) + own // cols), 1.0, 0.0)

    def put_w(ref, val):
        ref[...] = val.reshape(TALL, TALL, 2, BLK, LANES)
        return val

    def put_z(i, val):
        ZM[i] = val[:LANES]
        ZS[i] = val[LANES:]
        net.start(ZS.at[i], ZM.at[i], partner, "z", "z")
        return val

    def t_piece(side, step, k=None):
        xx = xs(step)
        return TG.at[side, xx // 2, pl.ds(2 * (xx % 2), 2) if k is None else 2 * (xx % 2) + k]

    def t_start(side, step, k, device, name, kind="t"):
        net.start(t_piece(side, step, k), t_piece(side, step, k), device, kind, (side, name))

    def t_send(side, val):
        t_piece(side, 0)[...] = val.reshape(CORES, TALL, TALL, BLK, LANES)
        for i in PAIR:
            for s in SIDES:
                k = i if s < 0 else 1 - i
                t_start(side, 0, k, along("x", -s), (s, i))
        t_start(side, 0, None, partner, "partner", "tpair")

    def t_near(side):
        for i in PAIR:
            for s in SIDES:
                k = i if s < 0 else 1 - i
                net.wait((side, (s, i)), t_piece(side, s, k))
                if i == 0:
                    t_start(side, s, k, along("x", -s), "far")
                t_start(side, s, k, partner, "partner", "tpair")

    def t_far(side):
        net.wait((side, "far"), t_piece(side, 2))
        t_start(side, 2, None, partner, "partner", "tpair")

    def c0_pair(n):
        return [jnp.concatenate([C0[k, c, :, LANES * n:LANES * (n + 1)] for k in range(CORES)], axis=0) for c in range(cols)]

    def own_columns(first, second):
        low = iota((first.shape[0], LANES), 1) < HALF
        out = []
        for val in (first, second):
            tile = jnp.where(y // 2 == 0, val[:, :LANES], val[:, LANES:])
            moved = pltpu.roll(tile, HALF, 1)
            out.append(jnp.where(y % 2 == 0, tile, moved) if val is first else jnp.where(y % 2 == 0, moved, tile))
        return jnp.where(low, out[0], out[1])

    def w_rows(ref):
        own = CORES * x
        return ref.at[..., own % cols, :, :, own // cols, :, :]

    mark("p_chain1")
    low_half = iota((WIDE, LANES), 1) < HALF
    blank = jnp.zeros((WIDE, WIDE), F32)

    def two_columns(one, two, coupling):
        head = own_columns(one, blank)
        return head, jnp.where(low_half, -dot(two, dot(coupling, head)), own_columns(blank, two))

    @pl.when(first_half)
    def _():
        head, tail = two_columns(leaf_inv(0), leaf_inv(1), coupling2(0))
        put_w(WL.at[0, :, 0], head)
        put_w(WL.at[0, :, 1], tail)

    @pl.when(core == 0)
    def _():
        z3 = put_z(3, dot(mine(3), turned(3)))
        put_z(2, dot(mine(2) - dot(z3, coupling2(1)), turned(2)))

    mark("q_c1")
    net.wait("c1", G.at[pl.ds(0, 3), pl.ds(0, 2), 0])

    def x_piece(step):
        xx = xs(step)
        return SX.at[xx // 2, pl.ds(2 * (xx % 2), 2)]

    @pl.when(first_half)
    def _():
        def own_rows(k):
            return jnp.concatenate(
                [G[k, 6 + i // 2, x // 2, 2 * (x % 2) + kk, i % 2] for kk in range(CORES) for i in range(BLK)], axis=0)

        product = dot(jnp.concatenate([own_rows(k) for k in range(cols)], axis=1), WL[0].reshape(2 * WIDE, LANES))
        x_piece(0)[...] = product.reshape(CORES, 2, TALL, BLK, LANES)
        for d in range(1, chips):
            net.start(x_piece(0), x_piece(0), along("x", d), "share", "share")

    @pl.when(core == 0)
    def _():
        lhs = [jnp.concatenate([ZM[i, HALF:], ZS[i, HALF:]], axis=0) for i in (2, 3)]
        YX[y] = sum(dot(lhs[i], gathered(y, 3 + i)) for i in PAIR)
        for d in range(1, cols):
            net.start(YX.at[y], YX.at[y], along("y", d), "share", "share")

    mark("s_other")
    arrive(REST[2:])
    start_leaves(1)
    double(1, 1)
    mark("s_relc0")

    @pl.when(first_half)
    def _():
        for s in SIDES:
            net.wait(("c0", s), C0.at[:, 0])
            piece = C0.at[0 if s < 0 else 1, ys(s)]
            net.start(piece, piece, along("y", -s), "c0far", "c0far")

    mark("s_dbl")
    double(1, 2)
    double(1, TALL)
    mark("t_c0")

    @pl.when(first_half)
    def _():
        net.wait("c0pair", C0.at[0, 0])
        net.wait("c0far", C0.at[0, pl.ds(0, 2)])

    mark("t_V")

    @pl.when(first_half)
    def _():
        right = c0_pair(1)
        v3 = dot(halves(right, 1), leaf_inv(3))
        v2 = dot(halves(right, 0) - dot(v3, coupling2(1)), leaf_inv(2))
        VV[:, :WIDE] = v2
        VV[:, WIDE:] = v3
        t_send(1, own_columns(v2, v3))
        TP[...] = dot(jnp.concatenate(c0_pair(0), axis=1), WL[0].reshape(2 * WIDE, LANES))

    mark("t_share")
    net.wait("share", G.at[pl.ds(0, 3), pl.ds(0, 2), 0])
    mark("u_chain2")

    @pl.when(first_half)
    def _():
        for g in PAIR:
            for c in range(TALL):
                for i in range(BLK):
                    SS[(g * TALL + c) * BLK + i] = SX[i % 2, c, g, i // 2]
        shared = SS[...].reshape(2 * WIDE, LANES)
        t_send(0, TP[...] - dot(VV[...], shared))
        t_near(1)
        w2 = put_w(WL.at[1, :, 0], -dot(leaf_inv(2), shared[:WIDE]))
        put_w(WL.at[1, :, 1], -dot(leaf_inv(3), shared[WIDE:] + dot(coupling2(1), w2)))
        head, tail = two_columns(leaf_inv(2), leaf_inv(3), coupling2(1))
        put_w(WR.at[:, 0], head)
        put_w(WR.at[:, 1], tail)
        net.start(w_rows(WL), w_rows(WL), partner, "w", "w")
        net.start(w_rows(WR), w_rows(WR), partner, "w", "w")
        t_near(0)

    @pl.when(core == 0)
    def _():
        none = jnp.zeros((HALF, LANES), F32)
        tiles = [jnp.concatenate([none, YX[k, :HALF], none, YX[k, HALF:]], axis=0) for k in range(cols)]
        z1 = put_z(1, dot(mine(1) - halves(tiles, 1), turned(1)))
        put_z(0, dot(mine(0) - halves(tiles, 0) - dot(z1, coupling2(0)), turned(0)))
        net.wait("w", G.at[pl.ds(0, 3), 0, 0])

    mark("v_out")

    @pl.when(first_half)
    def _():
        net.wait("z", ZM)

    o_ref[upper, far] = jnp.zeros((LANES, WIDE), F32)
    for i in range(TALL):
        lines = slice(quarter * i, quarter * (i + 1))
        o_ref[lines, :LANES] = WL[i // 2, spot, i % 2, :, hh].reshape(quarter, LANES)
        o_ref[lines, LANES:WIDE] = WR[spot, i % 2, :, hh].reshape(quarter, LANES) if i >= 2 else jnp.zeros((quarter, LANES), F32)
    o_ref[lower, far] = jnp.concatenate([own_columns(ZM[2 * n], ZM[2 * n + 1]) for n in PAIR], axis=1)

    mark("v_near")

    @pl.when(first_half)
    def _():
        t_far(1)
        t_far(0)

    mark("v_tend")

    @pl.when(core == 0)
    def _():
        for side in PAIR:
            net.wait((side, "partner"), TG.at[side])

    def t_rows(i):
        return jnp.concatenate([jnp.concatenate([TG[side, b % 2, c, i, b // 2] for c in range(TALL) for b in range(BLK)], axis=0)
                                for side in PAIR], axis=1)

    mark("w_x21")
    o_ref[lower, near] = -sum(dot(ZM[i], t_rows(i)) for i in range(TALL))

    mark("x_end")
    net.wait("lead", G.at[0, pl.ds(0, 5), 0], "send")
    net.wait("rest", G.at[0, :, 0], "send")
    net.wait("c1", G.at[pl.ds(0, 3), pl.ds(0, 2), 0], "send")
    net.wait("on", G.at[pl.ds(0, 3), :, 0], "send")
    net.wait("share", G.at[pl.ds(0, 3), pl.ds(0, 2), 0], "send")
    net.wait("pair", U.at[0], "send")
    net.wait("c0", C0.at[0, pl.ds(0, 2)], "send")

    @pl.when(first_half)
    def _():
        net.wait("c0far", C0.at[0, pl.ds(0, 2)], "send")
        net.wait("t", G.at[pl.ds(0, 3), pl.ds(0, 8), 0], "send")
        net.wait("tpair", TG, "send")
        net.wait("w", G.at[pl.ds(0, 3), 0, 0], "send")

    @pl.when(core == 0)
    def _():
        net.wait("c0pair", C0.at[0, 0], "send")
        net.wait("z", ZM, "send")

    mark()
    counts = [len([key for key in net.names if key[0] == side]) for side in ("send", "recv")]
    assert counts == [send.shape[0], recv.shape[0]], counts


def solution(mesh):
    rows, cols = mesh.shape["row"], mesh.shape["col"]
    block_spec = P(("batch", "row"), "col")

    def device_body(local_l):
        vmem = functools.partial(pltpu.VMEM, dtype=F32)
        return pl.pallas_call(
            functools.partial(kernel, rows, cols),
            out_shape=jax.ShapeDtypeStruct(local_l.shape, F32),
            in_specs=[pl.BlockSpec(memory_space=pl.ANY)],
            out_specs=pl.BlockSpec(memory_space=pltpu.VMEM),
            scratch_shapes=[
                vmem(local_l.shape),
                vmem((2, GROUPS, 2, BLK, LANES)),
                vmem((cols, GROUPS, 2, TALL, 2, BLK, LANES)),
                vmem((CORES, cols, LANES, WIDE)),
                vmem((TALL, TALL * BLK, BLK, WIDE)),
                vmem((TALL, 2 * BLK, BLK, WIDE)),
                vmem((TALL, TALL * BLK, BLK, WIDE)),
                vmem((2, cols, 2, TALL, 2, BLK, LANES)),
                vmem((cols, 2, TALL, 2, BLK, LANES)),
                vmem((TALL, LANES, WIDE)),
                vmem((TALL, LANES, WIDE)),
                vmem((2, 2, TALL, TALL, TALL, BLK, LANES)),
                vmem((2, TALL, 2, TALL, BLK, LANES)),
                vmem((cols, LANES, LANES)),
                vmem((WIDE, 2 * WIDE)),
                vmem((2 * TALL * BLK, BLK, LANES)),
                vmem((WIDE, LANES)),
                pltpu.SemaphoreType.DMA((3,)),
                pltpu.SemaphoreType.DMA((13,)),
                pltpu.SemaphoreType.DMA((63,)),
            ],
            compiler_params=pltpu.CompilerParams(collective_id=0, has_side_effects=True),
        )(local_l)

    return jax.shard_map(device_body, mesh=mesh, in_specs=(block_spec,), out_specs=block_spec, check_vma=False)
```

```python
import functools

import jax
import jax.numpy as jnp
from jax import lax
from jax.experimental import pallas as pl
from jax.experimental.pallas import tpu as pltpu
from jax.sharding import PartitionSpec as P

BLK = 8
CORES = 2
LANES = 128
HALF = LANES // 2
WIDE = 2 * LANES
TALL = 4
GROUPS = 10
LEAD = (0, 1, 2)
REST = (3, 4, 5)
PAIR = range(2)
SIDES = (-1, 1)
MESH = pl.DeviceIdType.MESH


class Marks:
    def __init__(self):
        self.scope = None

    def __call__(self, name=None):
        if self.scope is not None:
            self.scope.__exit__(None, None, None)
        self.scope = None if name is None else jax.named_scope(name)
        if name is not None:
            self.scope.__enter__()
F32 = jnp.float32


def dot(left, right):
    return jnp.dot(left, right, precision=lax.Precision.HIGHEST, preferred_element_type=F32)


def iota(shape, dim):
    return lax.broadcasted_iota(jnp.int32, shape, dim)


def halves(tiles, half):
    low = iota(tiles[0].shape, 1) < HALF
    out = []
    for first, second in ((tiles[0], tiles[1]), (tiles[2], tiles[3])):
        if half == 0:
            out.append(jnp.where(low, first, pltpu.roll(second, HALF, 1)))
        else:
            out.append(jnp.where(low, pltpu.roll(first, HALF, 1), second))
    return jnp.concatenate(out, axis=1)


class Net:
    def __init__(self, send, recv):
        self.send, self.recv, self.names = send, recv, {}

    def slot(self, side, name):
        held = [key for key in self.names if key[0] == side]
        return self.names.setdefault((side, name), len(held))

    def start(self, src, dst, device, send, recv):
        self.make(src, dst, device, send, recv).start()

    def make(self, src, dst, device, send, recv):
        return pltpu.make_async_remote_copy(
            src_ref=src, dst_ref=dst, send_sem=self.send.at[self.slot("send", send)], recv_sem=self.recv.at[self.slot("recv", recv)],
            device_id=device, device_id_type=MESH)

    def wait(self, name, like, side="recv"):
        sems = self.recv if side == "recv" else self.send
        pltpu.make_async_copy(like, like, sems.at[self.slot(side, name)]).wait()


def shift(val, lanes):
    return jnp.concatenate([pltpu.roll(val[:, LANES * i:LANES * (i + 1)], lanes % LANES, 1) for i in range(2)], axis=1)


def kernel(rows, cols, hbm_ref, o_ref, l_ref, U, G, C0, LF, PK, LI, WL, WR, ZM, ZS, TG, SX, YX, VV, SS, TP, load, send, recv):
    chips = rows // CORES
    row = lax.axis_index("row")
    y = lax.axis_index("col")
    x, core = row // CORES, row % CORES
    spot, hh = row % cols, row // cols
    net = Net(send, recv)
    first_half = core == 1

    def at(xx, cc, yy):
        return {"row": xx * CORES + cc, "col": yy}

    def xs(step):
        return lax.rem(x + step + chips, chips)

    def ys(step):
        return lax.rem(y + step + cols, cols)

    def along(axis, step, cc=core):
        return at(xs(step), cc, y) if axis == "x" else at(x, cc, ys(step))

    mark = Marks()
    mark("a_signal")
    upper, lower, near, far = pl.ds(0, LANES), pl.ds(LANES, LANES), pl.ds(0, WIDE), pl.ds(WIDE, WIDE)
    windows = [(upper, near), (lower, far), (lower, near)]
    loads = [pltpu.make_async_copy(hbm_ref.at[w], l_ref.at[w], load.at[i]) for i, w in enumerate(windows)]
    for made in loads:
        made.start()
    partner = at(x, 1 - core, y)
    barrier = pltpu.get_barrier_semaphore()
    peers = [partner] + [along(axis, d, cc) for axis in "xy" for d in range(1, chips) for cc in range(CORES)]
    for peer in peers:
        pl.semaphore_signal(barrier, inc=1, device_id=peer, device_id_type=MESH)

    mark("a_pack")
    quarter = LANES // TALL
    for part in range(2):
        loads[part].wait()
        piece = l_ref[part * LANES:(part + 1) * LANES, part * WIDE:(part + 1) * WIDE]
        low = iota((quarter, LANES), 1) < HALF
        band = [piece[quarter * i:quarter * (i + 1)] for i in range(TALL)]
        packed = [jnp.where(low, band[2 * m][:, LANES * m:LANES * (m + 1)], band[2 * m + 1][:, LANES * m:LANES * (m + 1)])
                  for m in PAIR]
        links = (band[1][:, :LANES], band[3][:, LANES:])
        links = [jnp.where(low[:2 * BLK], val[:2 * BLK], pltpu.roll(val[2 * BLK:], HALF, 1)) for val in links]
        tiles = []
        for m in (part, 1 - part):
            tiles += [packed[m].reshape(2, 2, BLK, LANES)[i] for i in PAIR] + [links[m].reshape(2, BLK, LANES)]
        for i in (2, 3):
            tiles += [band[i][:, :LANES].reshape(2, 2, BLK, LANES)[h] for h in PAIR]
        for g in range(GROUPS):
            U[part, g] = tiles[g]

        @pl.when(core == 1 - part)
        def _():
            for g in range(GROUPS):
                G[y, g, hh, spot] = tiles[g]

    loads[2].wait()
    C0[core, y] = l_ref[lower, near]
    mark("b_barrier")
    pl.semaphore_wait(barrier, len(peers))

    axis_first = "xyyxyx"

    def other(axis):
        return "y" if axis == "x" else "x"

    def source(g, f, s, k=None):
        xx, yy = (xs(f), ys(s)) if axis_first[g] == "x" else (xs(s), ys(f))
        return G.at[yy, g, xx // 2, pl.ds(2 * (xx % 2), 2) if k is None else 2 * (xx % 2) + k]

    def pass_on(g, f, s, k, step, name):
        piece = source(g, f, s, k)
        net.start(piece, piece, along(other(axis_first[g]), step), "on", name)

    def pass_leaf(g, f):
        for s in SIDES:
            pass_on(g, f, 0, None, -s, (g, "far") if f == 2 else (g, f, s))
        if f == 2:
            pass_on(g, f, 0, None, 2, (g, "far"))

    def half_on(g, f, s):
        pass_on(g, f, s, 0 if s < 0 else 1, -s, (g, "far"))

    def own(groups, name):
        lo, count = min(groups), len(groups)
        for axis in "xy":
            for step in SIDES:
                for part in range(2):
                    net.start(U.at[part, pl.ds(lo, count)], G.at[y, pl.ds(lo, count), hh, spot], along(axis, step, 1 - part),
                              name, (name, axis, -step))
        for g in groups:
            for part in range(2):
                net.start(U.at[part, g], G.at[y, g, hh, spot], along(axis_first[g], 2, 1 - part), name, (g, "two"))

    def near_by(groups, name):
        for step in SIDES:
            for axis in "xy":
                net.wait((name, axis, step), G.at[0, pl.ds(0, len(groups)), 0, pl.ds(0, 2)])
                for g in groups:
                    if axis_first[g] == axis:
                        pass_leaf(g, step)
                    else:
                        half_on(g, 0, step)

    def two_away(groups):
        for g in groups:
            net.wait((g, "two"), G.at[0, 0, 0, pl.ds(0, 2)])
            pass_leaf(g, 2)

    def across(groups):
        for f in SIDES:
            for s in SIDES:
                for g in groups:
                    net.wait((g, f, s), source(g, f, s))
                    half_on(g, f, s)

    def arrive(groups):
        for g in groups:
            net.wait((g, "far"), G.at[pl.ds(0, 3), g, 0])

    mark("d_own")
    own(LEAD, "lead")
    net.start(U.at[core], G.at[y, :, hh, spot], partner, "pair", "pair")
    for s in SIDES:
        net.start(l_ref.at[lower, near], C0.at[core, y], along("y", -s, 1), "c0", ("c0", s))

    @pl.when(core == 0)
    def _():
        net.start(l_ref.at[lower, near], C0.at[core, y], partner, "c0pair", "c0pair")

    mark("e_near")
    near_by(LEAD, "lead")
    own(REST, "rest")
    mark("g_two")
    two_away(LEAD)
    mark("h_diag")
    across(LEAD)
    net.wait("pair", U.at[0])
    mark("i_near2")
    near_by(REST, "rest")
    mark("j_more")
    for d in range(1, chips):
        for part, axis in enumerate("yx"):
            net.start(U.at[part, pl.ds(6, TALL)], G.at[y, pl.ds(6, TALL), hh, spot], along(axis, d, 1 - part), "c1", "c1")

    @pl.when(first_half)
    def _():
        for s in SIDES:
            net.wait(("c0", s), C0.at[:, 0])
            piece = C0.at[0 if s < 0 else 1, ys(s)]
            net.start(piece, piece, along("y", -s), "c0far", "c0far")

    mark("k_leafin")
    arrive(LEAD)

    lane = iota((BLK, LANES), 1)
    sub = iota((BLK, LANES), 0)
    block_of = (lane // BLK) % BLK

    def tile_of(k, q, c, b):
        return G[k, q + b // TALL, b % 2, c, (b // 2) % 2]

    def gathered(k, q):
        return jnp.concatenate([tile_of(k, q, c, b) for c in range(TALL) for b in range(BLK)], axis=0)

    def start_leaves(m):
        zero = jnp.zeros((BLK, LANES), F32)
        diag = [[None] * TALL for _ in range(TALL)]
        inv = [[zero] * TALL for _ in range(TALL)]
        for c in range(TALL):
            inv[c][c] = jnp.where(sub == lane % BLK, 1.0, 0.0)
            for k in range(c + 1):
                total = zero
                for b in range(BLK):
                    total = jnp.where(block_of == b, tile_of(k, 3 * m, c, b), total)
                diag[c][k] = total
        for t in range(BLK * TALL):
            ct, jt = t // BLK, t % BLK
            index = (lane // BLK) * BLK + jt
            spread = [jnp.take_along_axis(diag[c][ct], index, axis=1) for c in range(ct, TALL)]
            pivot = 1.0 / spread[0][jt:jt + 1, :]
            below = jnp.where(sub > jt, spread[0], 0.0)
            for k in range(ct + 1):
                solved = inv[ct][k][jt:jt + 1, :] * pivot
                inv[ct][k] = jnp.where(sub == jt, solved, inv[ct][k] - below * solved)
                for c in range(ct + 1, TALL):
                    inv[c][k] = inv[c][k] - spread[c - ct] * solved
        full = [gathered(k, 3 * m) for k in range(cols)]
        for e in PAIR:
            LF[2 * m + e] = halves(full, e).reshape(TALL * BLK, BLK, WIDE)
            for c in range(TALL):
                PK[2 * m + e, c] = halves(inv[c], e)

    def double(m, nb):
        count, lanes = TALL * nb, BLK * nb
        size = BLK * count
        group = ((iota((BLK, WIDE), 1) % HALF) // BLK) // nb
        even = ((iota((size, WIDE), 1) % HALF) // BLK) // nb % 2 == 0

        def coupling(leaf):
            out = []
            for bb in range(nb):
                for c in range(TALL):
                    total = LF[leaf, c * BLK + nb + bb]
                    for s in range(3, BLK // nb, 2):
                        total = jnp.where(group == s - 1, LF[leaf, c * BLK + s * nb + bb], total)
                    out.append(total)
            return jnp.concatenate(out, axis=0)

        def spread(val, flip):
            tiles = val.reshape(count, BLK, WIDE)
            return jnp.concatenate([jnp.where(group == (b // nb) ^ flip, tiles[(b % nb) * TALL + c], 0.0)
                                    for c in range(TALL) for b in range(BLK)], axis=0)

        one, two = (PK[2 * m + e, 0:count].reshape(size, WIDE) for e in PAIR)
        temp = dot(jnp.where(even, coupling(2 * m), shift(coupling(2 * m + 1), lanes)),
                   spread(jnp.where(even, one, shift(two, lanes)), 0))
        corner = dot(jnp.where(even, shift(two, -lanes), one), spread(temp, 1))
        for e, (val, low) in enumerate(((one, corner), (two, shift(corner, -lanes)))):
            parts = (jnp.where(even, val, 0.0), jnp.where(even, -low, val))
            for half in PAIR:
                tiles = parts[half].reshape(count, BLK, WIDE)
                if nb < TALL:
                    PK[2 * m + e, half * count:(half + 1) * count] = tiles
                else:
                    for i in range(count):
                        LI[2 * m + e, (i % TALL) * BLK + half * TALL + i // TALL] = tiles[i]

    mark("l_base")
    start_leaves(0)
    mark("n_dbl1")
    double(0, 1)
    mark("n_two2")
    two_away(REST)
    mark("n_dbl2")
    double(0, 2)
    mark("n_diag2")
    across(REST)
    mark("n_dbl4")
    double(0, TALL)
    mark("o_arr2")

    def leaf_inv(i):
        return LI[i].reshape(WIDE, WIDE)

    def turned(i):
        return leaf_inv((i + 2) % TALL)

    def coupling2(m):
        stacked = [jnp.concatenate([G[k, 3 * m + 2, b % 2, c, b // 2] for c in range(TALL) for b in range(TALL)], axis=0)
                   for k in range(cols)]
        top, bottom = halves(stacked, 0), halves(stacked, 1)
        return jnp.concatenate([val[quarter * c:quarter * (c + 1)] for c in range(TALL) for val in (top, bottom)], axis=0)

    def mine(i):
        r, l = iota((WIDE, WIDE), 0), iota((WIDE, WIDE), 1)
        own = CORES * x + r // LANES
        return jnp.where(((r // quarter) % TALL == i) & (l // HALF == own % cols) & (r % BLK == l % BLK)
                         & ((l % HALF) // BLK == 2 * ((r // BLK) % TALL) + own // cols), 1.0, 0.0)

    def put_w(ref, val):
        ref[...] = val.reshape(TALL, TALL, 2, BLK, LANES)
        return val

    def put_z(i, val):
        ZM[i] = val[:LANES]
        ZS[i] = val[LANES:]
        net.start(ZS.at[i], ZM.at[i], partner, "z", "z")
        return val

    def t_piece(side, step, k=None):
        xx = xs(step)
        return TG.at[side, xx // 2, pl.ds(2 * (xx % 2), 2) if k is None else 2 * (xx % 2) + k]

    def t_start(side, step, k, device, name, kind="t"):
        net.start(t_piece(side, step, k), t_piece(side, step, k), device, kind, (side, name))

    def t_send(side, val):
        t_piece(side, 0)[...] = val.reshape(CORES, TALL, TALL, BLK, LANES)
        for i in PAIR:
            for s in SIDES:
                k = i if s < 0 else 1 - i
                t_start(side, 0, k, along("x", -s), (s, i))
        t_start(side, 0, None, partner, "partner", "tpair")

    def t_near(side):
        for i in PAIR:
            for s in SIDES:
                k = i if s < 0 else 1 - i
                net.wait((side, (s, i)), t_piece(side, s, k))
                if i == 0:
                    t_start(side, s, k, along("x", -s), "far")
                t_start(side, s, k, partner, "partner", "tpair")

    def t_far(side):
        net.wait((side, "far"), t_piece(side, 2))
        t_start(side, 2, None, partner, "partner", "tpair")

    def c0_pair(n):
        return [jnp.concatenate([C0[k, c, :, LANES * n:LANES * (n + 1)] for k in range(CORES)], axis=0) for c in range(cols)]

    def own_columns(first, second):
        low = iota((first.shape[0], LANES), 1) < HALF
        out = []
        for val in (first, second):
            tile = jnp.where(y // 2 == 0, val[:, :LANES], val[:, LANES:])
            moved = pltpu.roll(tile, HALF, 1)
            out.append(jnp.where(y % 2 == 0, tile, moved) if val is first else jnp.where(y % 2 == 0, moved, tile))
        return jnp.where(low, out[0], out[1])

    def w_rows(ref):
        own = CORES * x
        return ref.at[..., own % cols, :, :, own // cols, :, :]

    mark("p_chain1")
    low_half = iota((WIDE, LANES), 1) < HALF
    blank = jnp.zeros((WIDE, WIDE), F32)

    def two_columns(one, two, coupling):
        head = own_columns(one, blank)
        return head, jnp.where(low_half, -dot(two, dot(coupling, head)), own_columns(blank, two))

    @pl.when(first_half)
    def _():
        head, tail = two_columns(leaf_inv(0), leaf_inv(1), coupling2(0))
        put_w(WL.at[0, :, 0], head)
        put_w(WL.at[0, :, 1], tail)

    @pl.when(core == 0)
    def _():
        z3 = put_z(3, dot(mine(3), turned(3)))
        put_z(2, dot(mine(2) - dot(z3, coupling2(0)), turned(2)))

    mark("q_c1")
    net.wait("c1", G.at[pl.ds(0, 3), pl.ds(0, 2), 0])

    def x_piece(step):
        xx = xs(step)
        return SX.at[xx // 2, pl.ds(2 * (xx % 2), 2)]

    @pl.when(first_half)
    def _():
        def own_rows(k):
            return jnp.concatenate(
                [G[k, 6 + i // 2, x // 2, 2 * (x % 2) + kk, i % 2] for kk in range(CORES) for i in range(BLK)], axis=0)

        product = dot(jnp.concatenate([own_rows(k) for k in range(cols)], axis=1), WL[0].reshape(2 * WIDE, LANES))
        x_piece(0)[...] = product.reshape(CORES, 2, TALL, BLK, LANES)
        for d in range(1, chips):
            net.start(x_piece(0), x_piece(0), along("x", d), "share", "share")

    @pl.when(core == 0)
    def _():
        lhs = [jnp.concatenate([ZM[i, HALF:], ZS[i, HALF:]], axis=0) for i in (2, 3)]
        YX[y] = sum(dot(lhs[i], gathered(y, 6 + 2 * i)) for i in PAIR)
        for d in range(1, cols):
            net.start(YX.at[y], YX.at[y], along("y", d), "share", "share")

    mark("s_other")
    arrive(REST)
    start_leaves(1)
    double(1, 1)
    mark("s_dbl")
    double(1, 2)
    double(1, TALL)
    mark("t_c0")

    @pl.when(first_half)
    def _():
        net.wait("c0pair", C0.at[0, 0])
        net.wait("c0far", C0.at[0, pl.ds(0, 2)])

    mark("t_V")

    @pl.when(first_half)
    def _():
        right = c0_pair(1)
        v3 = dot(halves(right, 1), leaf_inv(3))
        v2 = dot(halves(right, 0) - dot(v3, coupling2(1)), leaf_inv(2))
        VV[:, :WIDE] = v2
        VV[:, WIDE:] = v3
        t_send(1, own_columns(v2, v3))
        TP[...] = dot(jnp.concatenate(c0_pair(0), axis=1), WL[0].reshape(2 * WIDE, LANES))

    mark("t_share")
    net.wait("share", G.at[pl.ds(0, 3), pl.ds(0, 2), 0])
    mark("u_chain2")

    @pl.when(first_half)
    def _():
        for g in PAIR:
            for c in range(TALL):
                for i in range(BLK):
                    SS[(g * TALL + c) * BLK + i] = SX[i % 2, c, g, i // 2]
        shared = SS[...].reshape(2 * WIDE, LANES)
        t_send(0, TP[...] - dot(VV[...], shared))
        t_near(1)
        w2 = put_w(WL.at[1, :, 0], -dot(leaf_inv(2), shared[:WIDE]))
        put_w(WL.at[1, :, 1], -dot(leaf_inv(3), shared[WIDE:] + dot(coupling2(1), w2)))
        head, tail = two_columns(leaf_inv(2), leaf_inv(3), coupling2(1))
        put_w(WR.at[:, 0], head)
        put_w(WR.at[:, 1], tail)
        net.start(w_rows(WL), w_rows(WL), partner, "w", "w")
        net.start(w_rows(WR), w_rows(WR), partner, "w", "w")
        t_near(0)

    @pl.when(core == 0)
    def _():
        none = jnp.zeros((HALF, LANES), F32)
        tiles = [jnp.concatenate([none, YX[k, :HALF], none, YX[k, HALF:]], axis=0) for k in range(cols)]
        z1 = put_z(1, dot(mine(1) - halves(tiles, 1), turned(1)))
        put_z(0, dot(mine(0) - halves(tiles, 0) - dot(z1, coupling2(1)), turned(0)))
        net.wait("w", G.at[pl.ds(0, 3), 0, 0])

    mark("v_out")

    @pl.when(first_half)
    def _():
        net.wait("z", ZM)

    o_ref[upper, far] = jnp.zeros((LANES, WIDE), F32)
    for i in range(TALL):
        lines = slice(quarter * i, quarter * (i + 1))
        o_ref[lines, :LANES] = WL[i // 2, spot, i % 2, :, hh].reshape(quarter, LANES)
        o_ref[lines, LANES:WIDE] = WR[spot, i % 2, :, hh].reshape(quarter, LANES) if i >= 2 else jnp.zeros((quarter, LANES), F32)
    o_ref[lower, far] = jnp.concatenate([own_columns(ZM[2 * n], ZM[2 * n + 1]) for n in PAIR], axis=1)

    mark("v_near")

    @pl.when(first_half)
    def _():
        t_far(1)
        t_far(0)

    mark("v_tend")

    @pl.when(core == 0)
    def _():
        for side in PAIR:
            net.wait((side, "partner"), TG.at[side])

    def t_rows(i):
        return jnp.concatenate([jnp.concatenate([TG[side, b % 2, c, i, b // 2] for c in range(TALL) for b in range(BLK)], axis=0)
                                for side in PAIR], axis=1)

    mark("w_x21")
    o_ref[lower, near] = -sum(dot(ZM[i], t_rows(i)) for i in range(TALL))

    mark("x_end")
    for name in ("lead", "rest"):
        net.wait(name, G.at[pl.ds(0, 3), pl.ds(0, 5), 0, pl.ds(0, 2)], "send")
    net.wait("c1", G.at[pl.ds(0, 3), pl.ds(0, 2), 0], "send")
    net.wait("on", G.at[pl.ds(0, 3), :, 0], "send")
    net.wait("share", G.at[pl.ds(0, 3), pl.ds(0, 2), 0], "send")
    net.wait("pair", U.at[0], "send")
    net.wait("c0", C0.at[0, pl.ds(0, 2)], "send")

    @pl.when(first_half)
    def _():
        net.wait("c0far", C0.at[0, pl.ds(0, 2)], "send")
        net.wait("t", G.at[pl.ds(0, 3), pl.ds(0, 8), 0], "send")
        net.wait("tpair", TG, "send")
        net.wait("w", G.at[pl.ds(0, 3), 0, 0], "send")

    @pl.when(core == 0)
    def _():
        net.wait("c0pair", C0.at[0, 0], "send")
        net.wait("z", ZM, "send")

    mark()
    counts = [len([key for key in net.names if key[0] == side]) for side in ("send", "recv")]
    assert counts == [send.shape[0], recv.shape[0]], counts


def solution(mesh):
    rows, cols = mesh.shape["row"], mesh.shape["col"]
    block_spec = P(("batch", "row"), "col")

    def device_body(local_l):
        vmem = functools.partial(pltpu.VMEM, dtype=F32)
        return pl.pallas_call(
            functools.partial(kernel, rows, cols),
            out_shape=jax.ShapeDtypeStruct(local_l.shape, F32),
            in_specs=[pl.BlockSpec(memory_space=pl.ANY)],
            out_specs=pl.BlockSpec(memory_space=pltpu.VMEM),
            scratch_shapes=[
                vmem(local_l.shape),
                vmem((2, GROUPS, 2, BLK, LANES)),
                vmem((cols, GROUPS, 2, TALL, 2, BLK, LANES)),
                vmem((CORES, cols, LANES, WIDE)),
                vmem((TALL, TALL * BLK, BLK, WIDE)),
                vmem((TALL, 2 * BLK, BLK, WIDE)),
                vmem((TALL, TALL * BLK, BLK, WIDE)),
                vmem((2, cols, 2, TALL, 2, BLK, LANES)),
                vmem((cols, 2, TALL, 2, BLK, LANES)),
                vmem((TALL, LANES, WIDE)),
                vmem((TALL, LANES, WIDE)),
                vmem((2, 2, TALL, TALL, TALL, BLK, LANES)),
                vmem((2, TALL, 2, TALL, BLK, LANES)),
                vmem((cols, LANES, LANES)),
                vmem((WIDE, 2 * WIDE)),
                vmem((2 * TALL * BLK, BLK, LANES)),
                vmem((WIDE, LANES)),
                pltpu.SemaphoreType.DMA((3,)),
                pltpu.SemaphoreType.DMA((13,)),
                pltpu.SemaphoreType.DMA((63,)),
            ],
            compiler_params=pltpu.CompilerParams(collective_id=0, has_side_effects=True),
        )(local_l)

    return jax.shard_map(device_body, mesh=mesh, in_specs=(block_spec,), out_specs=block_spec, check_vma=False)
```

```python
import functools

import jax
import jax.numpy as jnp
from jax import lax
from jax.experimental import pallas as pl
from jax.experimental.pallas import tpu as pltpu
from jax.sharding import PartitionSpec as P

BLK = 8
CORES = 2
LANES = 128
HALF = LANES // 2
WIDE = 2 * LANES
TALL = 4
GROUPS = 10
LEAD = (0, 1, 2)
REST = (3, 4, 5)
PAIR = range(2)
SIDES = (-1, 1)
STEPS = (1, -1, 2)
MESH = pl.DeviceIdType.MESH


class Marks:
    def __init__(self):
        self.scope = None

    def __call__(self, name=None):
        if self.scope is not None:
            self.scope.__exit__(None, None, None)
        self.scope = None if name is None else jax.named_scope(name)
        if name is not None:
            self.scope.__enter__()
F32 = jnp.float32


def dot(left, right):
    return jnp.dot(left, right, precision=lax.Precision.HIGHEST, preferred_element_type=F32)


def iota(shape, dim):
    return lax.broadcasted_iota(jnp.int32, shape, dim)


def halves(tiles, half):
    low = iota(tiles[0].shape, 1) < HALF
    out = []
    for first, second in ((tiles[0], tiles[1]), (tiles[2], tiles[3])):
        if half == 0:
            out.append(jnp.where(low, first, pltpu.roll(second, HALF, 1)))
        else:
            out.append(jnp.where(low, pltpu.roll(first, HALF, 1), second))
    return jnp.concatenate(out, axis=1)


class Net:
    def __init__(self, send, recv):
        self.send, self.recv, self.names = send, recv, {}

    def slot(self, side, name):
        held = [key for key in self.names if key[0] == side]
        return self.names.setdefault((side, name), len(held))

    def start(self, src, dst, device, send, recv):
        self.make(src, dst, device, send, recv).start()

    def make(self, src, dst, device, send, recv):
        return pltpu.make_async_remote_copy(
            src_ref=src, dst_ref=dst, send_sem=self.send.at[self.slot("send", send)], recv_sem=self.recv.at[self.slot("recv", recv)],
            device_id=device, device_id_type=MESH)

    def wait(self, name, like, side="recv"):
        sems = self.recv if side == "recv" else self.send
        pltpu.make_async_copy(like, like, sems.at[self.slot(side, name)]).wait()


def shift(val, lanes):
    return jnp.concatenate([pltpu.roll(val[:, LANES * i:LANES * (i + 1)], lanes % LANES, 1) for i in range(2)], axis=1)


def kernel(rows, cols, hbm_ref, o_ref, l_ref, U, G, C0, LF, PK, LI, WL, WR, ZM, ZS, TG, SX, YX, VV, SS, TP, load, send, recv):
    chips = rows // CORES
    row = lax.axis_index("row")
    y = lax.axis_index("col")
    x, core = row // CORES, row % CORES
    spot, hh = row % cols, row // cols
    net = Net(send, recv)
    first_half = core == 1

    def at(xx, cc, yy):
        return {"row": xx * CORES + cc, "col": yy}

    def xs(step):
        return lax.rem(x + step + chips, chips)

    def ys(step):
        return lax.rem(y + step + cols, cols)

    def along(axis, step, cc=core):
        return at(xs(step), cc, y) if axis == "x" else at(x, cc, ys(step))

    mark = Marks()
    mark("a_signal")
    upper, lower, near, far = pl.ds(0, LANES), pl.ds(LANES, LANES), pl.ds(0, WIDE), pl.ds(WIDE, WIDE)
    windows = [(upper, near), (lower, far), (lower, near)]
    loads = [pltpu.make_async_copy(hbm_ref.at[w], l_ref.at[w], load.at[i]) for i, w in enumerate(windows)]
    for made in loads:
        made.start()
    partner = at(x, 1 - core, y)
    barrier = pltpu.get_barrier_semaphore()
    peers = [partner] + [along(axis, d, cc) for axis in "xy" for d in range(1, chips) for cc in range(CORES)]
    for peer in peers:
        pl.semaphore_signal(barrier, inc=1, device_id=peer, device_id_type=MESH)

    mark("a_pack")
    quarter = LANES // TALL
    for part in range(2):
        loads[part].wait()
        piece = l_ref[part * LANES:(part + 1) * LANES, part * WIDE:(part + 1) * WIDE]
        low = iota((quarter, LANES), 1) < HALF
        band = [piece[quarter * i:quarter * (i + 1)] for i in range(TALL)]
        packed = [jnp.where(low, band[2 * m][:, LANES * m:LANES * (m + 1)], band[2 * m + 1][:, LANES * m:LANES * (m + 1)])
                  for m in PAIR]
        links = (band[1][:, :LANES], band[3][:, LANES:])
        links = [jnp.where(low[:2 * BLK], val[:2 * BLK], pltpu.roll(val[2 * BLK:], HALF, 1)) for val in links]
        tiles = []
        for m in (part, 1 - part):
            tiles += [packed[m].reshape(2, 2, BLK, LANES)[i] for i in PAIR] + [links[m].reshape(2, BLK, LANES)]
        for i in (2, 3):
            tiles += [band[i][:, :LANES].reshape(2, 2, BLK, LANES)[h] for h in PAIR]
        for g in range(GROUPS):
            U[part, g] = tiles[g]

        @pl.when(core == 1 - part)
        def _():
            for g in range(GROUPS):
                G[y, g, hh, spot] = tiles[g]

    loads[2].wait()
    C0[core, y] = l_ref[lower, near]
    mark("b_barrier")
    pl.semaphore_wait(barrier, len(peers))

    axis_first = "xyyxyx"

    def other(axis):
        return "y" if axis == "x" else "x"

    def source(g, f, s, k=None):
        xx, yy = (xs(f), ys(s)) if axis_first[g] == "x" else (xs(s), ys(f))
        return G.at[yy, g, xx // 2, pl.ds(2 * (xx % 2), 2) if k is None else 2 * (xx % 2) + k]

    def pass_on(g, f, s, k, step, name):
        piece = source(g, f, s, k)
        net.start(piece, piece, along(other(axis_first[g]), step), "on", name)

    def own(groups, name):
        lo, count = min(groups), len(groups)
        for step in STEPS:
            for axis in "xy":
                for part in range(2):
                    net.start(U.at[part, pl.ds(lo, count)], G.at[y, pl.ds(lo, count), hh, spot], along(axis, step, 1 - part),
                              name, (name, axis, -step if step < 2 else step))

    def forward(groups, name, steps):
        for step in steps:
            for axis in "xy":
                net.wait((name, axis, step), G.at[0, pl.ds(0, len(groups)), 0, pl.ds(0, 2)])
                for g in groups:
                    if axis_first[g] == axis:
                        for away in STEPS:
                            pass_on(g, step, 0, None, away, (g, "far"))

    def arrive(groups):
        for g in groups:
            net.wait((g, "far"), G.at[pl.ds(0, 3), g, :, pl.ds(0, 3)])

    mark("d_own")
    own(LEAD, "lead")
    own(REST, "rest")
    net.start(U.at[core], G.at[y, :, hh, spot], partner, "pair", "pair")
    mark("e_near")
    forward(LEAD, "lead", SIDES)
    mark("g_two")
    forward(LEAD, "lead", (2,))
    mark("i_near2")
    forward(REST, "rest", SIDES)
    mark("i_two2")
    forward(REST, "rest", (2,))
    mark("j_more")
    net.wait("pair", U.at[0])
    for s in SIDES:
        net.start(l_ref.at[lower, near], C0.at[core, y], along("y", -s, 1), "c0", ("c0", s))

    @pl.when(core == 0)
    def _():
        net.start(l_ref.at[lower, near], C0.at[core, y], partner, "c0pair", "c0pair")

    for d in range(1, chips):
        for part, axis in enumerate("yx"):
            net.start(U.at[part, pl.ds(6, TALL)], G.at[y, pl.ds(6, TALL), hh, spot], along(axis, d, 1 - part), "c1", "c1")

    mark("k_leafin")
    arrive(LEAD)

    lane = iota((BLK, LANES), 1)
    sub = iota((BLK, LANES), 0)
    block_of = (lane // BLK) % BLK

    def tile_of(k, q, c, b):
        return G[k, q + b // TALL, b % 2, c, (b // 2) % 2]

    def gathered(k, q):
        return jnp.concatenate([tile_of(k, q, c, b) for c in range(TALL) for b in range(BLK)], axis=0)

    def start_leaves(m):
        zero = jnp.zeros((BLK, LANES), F32)
        diag = [[None] * TALL for _ in range(TALL)]
        inv = [[zero] * TALL for _ in range(TALL)]
        for c in range(TALL):
            inv[c][c] = jnp.where(sub == lane % BLK, 1.0, 0.0)
            for k in range(c + 1):
                total = zero
                for b in range(BLK):
                    total = jnp.where(block_of == b, tile_of(k, 3 * m, c, b), total)
                diag[c][k] = total
        for t in range(BLK * TALL):
            ct, jt = t // BLK, t % BLK
            index = (lane // BLK) * BLK + jt
            spread = [jnp.take_along_axis(diag[c][ct], index, axis=1) for c in range(ct, TALL)]
            pivot = 1.0 / spread[0][jt:jt + 1, :]
            below = jnp.where(sub > jt, spread[0], 0.0)
            for k in range(ct + 1):
                solved = inv[ct][k][jt:jt + 1, :] * pivot
                inv[ct][k] = jnp.where(sub == jt, solved, inv[ct][k] - below * solved)
                for c in range(ct + 1, TALL):
                    inv[c][k] = inv[c][k] - spread[c - ct] * solved
        full = [gathered(k, 3 * m) for k in range(cols)]
        for e in PAIR:
            LF[2 * m + e] = halves(full, e).reshape(TALL * BLK, BLK, WIDE)
            for c in range(TALL):
                PK[2 * m + e, c] = halves(inv[c], e)

    def double(m, nb):
        count, lanes = TALL * nb, BLK * nb
        size = BLK * count
        group = ((iota((BLK, WIDE), 1) % HALF) // BLK) // nb
        even = ((iota((size, WIDE), 1) % HALF) // BLK) // nb % 2 == 0

        def coupling(leaf):
            out = []
            for bb in range(nb):
                for c in range(TALL):
                    total = LF[leaf, c * BLK + nb + bb]
                    for s in range(3, BLK // nb, 2):
                        total = jnp.where(group == s - 1, LF[leaf, c * BLK + s * nb + bb], total)
                    out.append(total)
            return jnp.concatenate(out, axis=0)

        def spread(val, flip):
            tiles = val.reshape(count, BLK, WIDE)
            return jnp.concatenate([jnp.where(group == (b // nb) ^ flip, tiles[(b % nb) * TALL + c], 0.0)
                                    for c in range(TALL) for b in range(BLK)], axis=0)

        one, two = (PK[2 * m + e, 0:count].reshape(size, WIDE) for e in PAIR)
        temp = dot(jnp.where(even, coupling(2 * m), shift(coupling(2 * m + 1), lanes)),
                   spread(jnp.where(even, one, shift(two, lanes)), 0))
        corner = dot(jnp.where(even, shift(two, -lanes), one), spread(temp, 1))
        for e, (val, low) in enumerate(((one, corner), (two, shift(corner, -lanes)))):
            parts = (jnp.where(even, val, 0.0), jnp.where(even, -low, val))
            for half in PAIR:
                tiles = parts[half].reshape(count, BLK, WIDE)
                if nb < TALL:
                    PK[2 * m + e, half * count:(half + 1) * count] = tiles
                else:
                    for i in range(count):
                        LI[2 * m + e, (i % TALL) * BLK + half * TALL + i // TALL] = tiles[i]

    mark("l_base")
    start_leaves(0)
    mark("n_dbl1")
    double(0, 1)
    mark("n_c0")

    @pl.when(first_half)
    def _():
        for s in SIDES:
            net.wait(("c0", s), C0.at[:, 0])
            piece = C0.at[0 if s < 0 else 1, ys(s)]
            net.start(piece, piece, along("y", -s), "c0far", "c0far")

    mark("n_dbl2")
    double(0, 2)
    mark("n_dbl4")
    double(0, TALL)
    mark("o_arr2")

    def leaf_inv(i):
        return LI[i].reshape(WIDE, WIDE)

    def turned(i):
        return leaf_inv((i + 2) % TALL)

    def coupling2(m):
        stacked = [jnp.concatenate([G[k, 3 * m + 2, b % 2, c, b // 2] for c in range(TALL) for b in range(TALL)], axis=0)
                   for k in range(cols)]
        top, bottom = halves(stacked, 0), halves(stacked, 1)
        return jnp.concatenate([val[quarter * c:quarter * (c + 1)] for c in range(TALL) for val in (top, bottom)], axis=0)

    def mine(i):
        r, l = iota((WIDE, WIDE), 0), iota((WIDE, WIDE), 1)
        own = CORES * x + r // LANES
        return jnp.where(((r // quarter) % TALL == i) & (l // HALF == own % cols) & (r % BLK == l % BLK)
                         & ((l % HALF) // BLK == 2 * ((r // BLK) % TALL) + own // cols), 1.0, 0.0)

    def put_w(ref, val):
        ref[...] = val.reshape(TALL, TALL, 2, BLK, LANES)
        return val

    def put_z(i, val):
        ZM[i] = val[:LANES]
        ZS[i] = val[LANES:]
        net.start(ZS.at[i], ZM.at[i], partner, "z", "z")
        return val

    def t_piece(side, step, k=None):
        xx = xs(step)
        return TG.at[side, xx // 2, pl.ds(2 * (xx % 2), 2) if k is None else 2 * (xx % 2) + k]

    def t_start(side, step, k, device, name, kind="t"):
        net.start(t_piece(side, step, k), t_piece(side, step, k), device, kind, (side, name))

    def t_send(side, val):
        t_piece(side, 0)[...] = val.reshape(CORES, TALL, TALL, BLK, LANES)
        for i in PAIR:
            for s in SIDES:
                k = i if s < 0 else 1 - i
                t_start(side, 0, k, along("x", -s), (s, i))
        t_start(side, 0, None, partner, "partner", "tpair")

    def t_near(side):
        for i in PAIR:
            for s in SIDES:
                k = i if s < 0 else 1 - i
                net.wait((side, (s, i)), t_piece(side, s, k))
                if i == 0:
                    t_start(side, s, k, along("x", -s), "far")
                t_start(side, s, k, partner, "partner", "tpair")

    def t_far(side):
        net.wait((side, "far"), t_piece(side, 2))
        t_start(side, 2, None, partner, "partner", "tpair")

    def c0_pair(n):
        return [jnp.concatenate([C0[k, c, :, LANES * n:LANES * (n + 1)] for k in range(CORES)], axis=0) for c in range(cols)]

    def own_columns(first, second):
        low = iota((first.shape[0], LANES), 1) < HALF
        out = []
        for val in (first, second):
            tile = jnp.where(y // 2 == 0, val[:, :LANES], val[:, LANES:])
            moved = pltpu.roll(tile, HALF, 1)
            out.append(jnp.where(y % 2 == 0, tile, moved) if val is first else jnp.where(y % 2 == 0, moved, tile))
        return jnp.where(low, out[0], out[1])

    def w_rows(ref):
        own = CORES * x
        return ref.at[..., own % cols, :, :, own // cols, :, :]

    mark("p_chain1")
    low_half = iota((WIDE, LANES), 1) < HALF
    blank = jnp.zeros((WIDE, WIDE), F32)

    def two_columns(one, two, coupling):
        head = own_columns(one, blank)
        return head, jnp.where(low_half, -dot(two, dot(coupling, head)), own_columns(blank, two))

    @pl.when(first_half)
    def _():
        head, tail = two_columns(leaf_inv(0), leaf_inv(1), coupling2(0))
        put_w(WL.at[0, :, 0], head)
        put_w(WL.at[0, :, 1], tail)

    @pl.when(core == 0)
    def _():
        z3 = put_z(3, dot(mine(3), turned(3)))
        put_z(2, dot(mine(2) - dot(z3, coupling2(0)), turned(2)))

    mark("q_c1")
    net.wait("c1", G.at[pl.ds(0, 3), pl.ds(0, 2), 0])

    def x_piece(step):
        xx = xs(step)
        return SX.at[xx // 2, pl.ds(2 * (xx % 2), 2)]

    @pl.when(first_half)
    def _():
        def own_rows(k):
            return jnp.concatenate(
                [G[k, 6 + i // 2, x // 2, 2 * (x % 2) + kk, i % 2] for kk in range(CORES) for i in range(BLK)], axis=0)

        product = dot(jnp.concatenate([own_rows(k) for k in range(cols)], axis=1), WL[0].reshape(2 * WIDE, LANES))
        x_piece(0)[...] = product.reshape(CORES, 2, TALL, BLK, LANES)
        for d in range(1, chips):
            net.start(x_piece(0), x_piece(0), along("x", d), "share", "share")

    @pl.when(core == 0)
    def _():
        lhs = [jnp.concatenate([ZM[i, HALF:], ZS[i, HALF:]], axis=0) for i in (2, 3)]
        YX[y] = sum(dot(lhs[i], gathered(y, 6 + 2 * i)) for i in PAIR)
        for d in range(1, cols):
            net.start(YX.at[y], YX.at[y], along("y", d), "share", "share")

    mark("s_c0")

    @pl.when(first_half)
    def _():
        net.wait("c0pair", C0.at[0, 0])
        net.wait("c0far", C0.at[0, pl.ds(0, 2)])
        TP[...] = dot(jnp.concatenate(c0_pair(0), axis=1), WL[0].reshape(2 * WIDE, LANES))

    mark("s_arr")
    arrive(REST)
    mark("s_other")
    start_leaves(1)
    double(1, 1)
    mark("s_dbl")
    double(1, 2)
    double(1, TALL)
    mark("t_V")

    @pl.when(first_half)
    def _():
        right = c0_pair(1)
        v3 = dot(halves(right, 1), leaf_inv(3))
        v2 = dot(halves(right, 0) - dot(v3, coupling2(1)), leaf_inv(2))
        VV[:, :WIDE] = v2
        VV[:, WIDE:] = v3
        t_send(1, own_columns(v2, v3))

    mark("t_share")
    net.wait("share", G.at[pl.ds(0, 3), pl.ds(0, 2), 0])
    mark("u_chain2")

    @pl.when(first_half)
    def _():
        for g in PAIR:
            for c in range(TALL):
                for i in range(BLK):
                    SS[(g * TALL + c) * BLK + i] = SX[i % 2, c, g, i // 2]
        shared = SS[...].reshape(2 * WIDE, LANES)
        t_send(0, TP[...] - dot(VV[...], shared))
        t_near(1)
        w2 = put_w(WL.at[1, :, 0], -dot(leaf_inv(2), shared[:WIDE]))
        put_w(WL.at[1, :, 1], -dot(leaf_inv(3), shared[WIDE:] + dot(coupling2(1), w2)))
        head, tail = two_columns(leaf_inv(2), leaf_inv(3), coupling2(1))
        put_w(WR.at[:, 0], head)
        put_w(WR.at[:, 1], tail)
        net.start(w_rows(WL), w_rows(WL), partner, "w", "w")
        net.start(w_rows(WR), w_rows(WR), partner, "w", "w")
        t_near(0)

    @pl.when(core == 0)
    def _():
        none = jnp.zeros((HALF, LANES), F32)
        tiles = [jnp.concatenate([none, YX[k, :HALF], none, YX[k, HALF:]], axis=0) for k in range(cols)]
        z1 = put_z(1, dot(mine(1) - halves(tiles, 1), turned(1)))
        put_z(0, dot(mine(0) - halves(tiles, 0) - dot(z1, coupling2(1)), turned(0)))
        net.wait("w", G.at[pl.ds(0, 3), 0, 0])

    mark("v_out")

    @pl.when(first_half)
    def _():
        net.wait("z", ZM)

    o_ref[upper, far] = jnp.zeros((LANES, WIDE), F32)
    for i in range(TALL):
        lines = slice(quarter * i, quarter * (i + 1))
        o_ref[lines, :LANES] = WL[i // 2, spot, i % 2, :, hh].reshape(quarter, LANES)
        o_ref[lines, LANES:WIDE] = WR[spot, i % 2, :, hh].reshape(quarter, LANES) if i >= 2 else jnp.zeros((quarter, LANES), F32)
    o_ref[lower, far] = jnp.concatenate([own_columns(ZM[2 * n], ZM[2 * n + 1]) for n in PAIR], axis=1)

    mark("v_near")

    @pl.when(first_half)
    def _():
        t_far(1)
        t_far(0)

    mark("v_tend")

    @pl.when(core == 0)
    def _():
        for side in PAIR:
            net.wait((side, "partner"), TG.at[side])

    def t_rows(i):
        return jnp.concatenate([jnp.concatenate([TG[side, b % 2, c, i, b // 2] for c in range(TALL) for b in range(BLK)], axis=0)
                                for side in PAIR], axis=1)

    mark("w_x21")
    o_ref[lower, near] = -sum(dot(ZM[i], t_rows(i)) for i in range(TALL))

    mark("x_end")
    for name in ("lead", "rest"):
        net.wait(name, G.at[pl.ds(0, 3), pl.ds(0, 3), 0], "send")
    net.wait("c1", G.at[pl.ds(0, 3), pl.ds(0, 2), 0], "send")
    net.wait("on", G.at[pl.ds(0, 3), pl.ds(0, 9), 0], "send")
    net.wait("share", G.at[pl.ds(0, 3), pl.ds(0, 2), 0], "send")
    net.wait("pair", U.at[0], "send")
    net.wait("c0", C0.at[0, pl.ds(0, 2)], "send")

    @pl.when(first_half)
    def _():
        net.wait("c0far", C0.at[0, pl.ds(0, 2)], "send")
        net.wait("t", G.at[pl.ds(0, 3), pl.ds(0, 8), 0], "send")
        net.wait("tpair", TG, "send")
        net.wait("w", G.at[pl.ds(0, 3), 0, 0], "send")

    @pl.when(core == 0)
    def _():
        net.wait("c0pair", C0.at[0, 0], "send")
        net.wait("z", ZM, "send")

    mark()
    counts = [len([key for key in net.names if key[0] == side]) for side in ("send", "recv")]
    assert counts == [send.shape[0], recv.shape[0]], counts


def solution(mesh):
    rows, cols = mesh.shape["row"], mesh.shape["col"]
    block_spec = P(("batch", "row"), "col")

    def device_body(local_l):
        vmem = functools.partial(pltpu.VMEM, dtype=F32)
        return pl.pallas_call(
            functools.partial(kernel, rows, cols),
            out_shape=jax.ShapeDtypeStruct(local_l.shape, F32),
            in_specs=[pl.BlockSpec(memory_space=pl.ANY)],
            out_specs=pl.BlockSpec(memory_space=pltpu.VMEM),
            scratch_shapes=[
                vmem(local_l.shape),
                vmem((2, GROUPS, 2, BLK, LANES)),
                vmem((cols, GROUPS, 2, TALL, 2, BLK, LANES)),
                vmem((CORES, cols, LANES, WIDE)),
                vmem((TALL, TALL * BLK, BLK, WIDE)),
                vmem((TALL, 2 * BLK, BLK, WIDE)),
                vmem((TALL, TALL * BLK, BLK, WIDE)),
                vmem((2, cols, 2, TALL, 2, BLK, LANES)),
                vmem((cols, 2, TALL, 2, BLK, LANES)),
                vmem((TALL, LANES, WIDE)),
                vmem((TALL, LANES, WIDE)),
                vmem((2, 2, TALL, TALL, TALL, BLK, LANES)),
                vmem((2, TALL, 2, TALL, BLK, LANES)),
                vmem((cols, LANES, LANES)),
                vmem((WIDE, 2 * WIDE)),
                vmem((2 * TALL * BLK, BLK, LANES)),
                vmem((WIDE, LANES)),
                pltpu.SemaphoreType.DMA((3,)),
                pltpu.SemaphoreType.DMA((13,)),
                pltpu.SemaphoreType.DMA((37,)),
            ],
            compiler_params=pltpu.CompilerParams(collective_id=0, has_side_effects=True),
        )(local_l)

    return jax.shard_map(device_body, mesh=mesh, in_specs=(block_spec,), out_specs=block_spec, check_vma=False)
```

```python
import functools

import jax
import jax.numpy as jnp
from jax import lax
from jax.experimental import pallas as pl
from jax.experimental.pallas import tpu as pltpu
from jax.sharding import PartitionSpec as P

BLK = 8
CORES = 2
LANES = 128
HALF = LANES // 2
WIDE = 2 * LANES
TALL = 4
GROUPS = 10
LEAD = (0, 1, 2)
REST = (3, 4, 5)
PAIR = range(2)
SIDES = (-1, 1)
STEPS = (1, -1, 2)
MESH = pl.DeviceIdType.MESH


class Marks:
    def __init__(self):
        self.scope = None

    def __call__(self, name=None):
        if self.scope is not None:
            self.scope.__exit__(None, None, None)
        self.scope = None if name is None else jax.named_scope(name)
        if name is not None:
            self.scope.__enter__()
F32 = jnp.float32


def dot(left, right):
    return jnp.dot(left, right, precision=lax.Precision.HIGHEST, preferred_element_type=F32)


def iota(shape, dim):
    return lax.broadcasted_iota(jnp.int32, shape, dim)


def halves(tiles, half):
    low = iota(tiles[0].shape, 1) < HALF
    out = []
    for first, second in ((tiles[0], tiles[1]), (tiles[2], tiles[3])):
        if half == 0:
            out.append(jnp.where(low, first, pltpu.roll(second, HALF, 1)))
        else:
            out.append(jnp.where(low, pltpu.roll(first, HALF, 1), second))
    return jnp.concatenate(out, axis=1)


class Net:
    def __init__(self, send, recv):
        self.send, self.recv, self.names = send, recv, {}

    def slot(self, side, name):
        held = [key for key in self.names if key[0] == side]
        return self.names.setdefault((side, name), len(held))

    def start(self, src, dst, device, send, recv):
        self.make(src, dst, device, send, recv).start()

    def make(self, src, dst, device, send, recv):
        return pltpu.make_async_remote_copy(
            src_ref=src, dst_ref=dst, send_sem=self.send.at[self.slot("send", send)], recv_sem=self.recv.at[self.slot("recv", recv)],
            device_id=device, device_id_type=MESH)

    def wait(self, name, like, side="recv"):
        sems = self.recv if side == "recv" else self.send
        pltpu.make_async_copy(like, like, sems.at[self.slot(side, name)]).wait()


def shift(val, lanes):
    return jnp.concatenate([pltpu.roll(val[:, LANES * i:LANES * (i + 1)], lanes % LANES, 1) for i in range(2)], axis=1)


def kernel(rows, cols, hbm_ref, o_ref, l_ref, U, G, C0, LF, PK, LI, WL, WR, ZM, ZS, TG, SX, YX, VV, SS, TP, load, send, recv):
    chips = rows // CORES
    row = lax.axis_index("row")
    y = lax.axis_index("col")
    x, core = row // CORES, row % CORES
    spot, hh = row % cols, row // cols
    net = Net(send, recv)
    first_half = core == 1

    def at(xx, cc, yy):
        return {"row": xx * CORES + cc, "col": yy}

    def xs(step):
        return lax.rem(x + step + chips, chips)

    def ys(step):
        return lax.rem(y + step + cols, cols)

    def along(axis, step, cc=core):
        return at(xs(step), cc, y) if axis == "x" else at(x, cc, ys(step))

    mark = Marks()
    mark("a_signal")
    upper, lower, near, far = pl.ds(0, LANES), pl.ds(LANES, LANES), pl.ds(0, WIDE), pl.ds(WIDE, WIDE)
    windows = [(upper, near), (lower, far), (lower, near)]
    loads = [pltpu.make_async_copy(hbm_ref.at[w], l_ref.at[w], load.at[i]) for i, w in enumerate(windows)]
    for made in loads:
        made.start()
    partner = at(x, 1 - core, y)
    barrier = pltpu.get_barrier_semaphore()
    peers = [partner] + [along(axis, d, cc) for axis in "xy" for d in range(1, chips) for cc in range(CORES)]
    for peer in peers:
        pl.semaphore_signal(barrier, inc=1, device_id=peer, device_id_type=MESH)

    mark("a_pack")
    quarter = LANES // TALL
    for part in range(2):
        loads[part].wait()
        piece = l_ref[part * LANES:(part + 1) * LANES, part * WIDE:(part + 1) * WIDE]
        low = iota((quarter, LANES), 1) < HALF
        band = [piece[quarter * i:quarter * (i + 1)] for i in range(TALL)]
        packed = [jnp.where(low, band[2 * m][:, LANES * m:LANES * (m + 1)], band[2 * m + 1][:, LANES * m:LANES * (m + 1)])
                  for m in PAIR]
        links = (band[1][:, :LANES], band[3][:, LANES:])
        links = [jnp.where(low[:2 * BLK], val[:2 * BLK], pltpu.roll(val[2 * BLK:], HALF, 1)) for val in links]
        tiles = []
        for m in (part, 1 - part):
            tiles += [packed[m].reshape(2, 2, BLK, LANES)[i] for i in PAIR] + [links[m].reshape(2, BLK, LANES)]
        for i in (2, 3):
            tiles += [band[i][:, :LANES].reshape(2, 2, BLK, LANES)[h] for h in PAIR]
        for g in range(GROUPS):
            U[part, g] = tiles[g]

        @pl.when(core == 1 - part)
        def _():
            for g in range(GROUPS):
                G[y, g, hh, spot] = tiles[g]

    loads[2].wait()
    C0[core, y] = l_ref[lower, near]
    mark("b_barrier")
    pl.semaphore_wait(barrier, len(peers))

    axis_first = "xyyxyx"

    def other(axis):
        return "y" if axis == "x" else "x"

    def source(g, f, s, k=None):
        xx, yy = (xs(f), ys(s)) if axis_first[g] == "x" else (xs(s), ys(f))
        return G.at[yy, g, xx // 2, pl.ds(2 * (xx % 2), 2) if k is None else 2 * (xx % 2) + k]

    def pass_on(g, f, s, k, step, name):
        piece = source(g, f, s, k)
        net.start(piece, piece, along(other(axis_first[g]), step), "on", name)

    def own(groups, name):
        lo, count = min(groups), len(groups)
        for step in STEPS:
            for axis in "xy":
                for part in range(2):
                    net.start(U.at[part, pl.ds(lo, count)], G.at[y, pl.ds(lo, count), hh, spot], along(axis, step, 1 - part),
                              name, (name, axis, -step if step < 2 else step))

    def forward(groups, name, steps):
        for step in steps:
            for axis in "xy":
                net.wait((name, axis, step), G.at[0, pl.ds(0, len(groups)), 0, pl.ds(0, 2)])
                for g in groups:
                    if axis_first[g] == axis:
                        for away in STEPS:
                            pass_on(g, step, 0, None, away, (g, "far"))

    def arrive(groups):
        for g in groups:
            net.wait((g, "far"), G.at[pl.ds(0, 3), g, :, pl.ds(0, 3)])

    mark("d_own")
    own(LEAD, "lead")
    own(REST, "rest")
    net.start(U.at[core], G.at[y, :, hh, spot], partner, "pair", "pair")
    for s in SIDES:
        net.start(l_ref.at[lower, near], C0.at[core, y], along("y", -s, 1), "c0", ("c0", s))

    @pl.when(core == 0)
    def _():
        net.start(l_ref.at[lower, near], C0.at[core, y], partner, "c0pair", "c0pair")

    mark("e_near")
    forward(LEAD, "lead", SIDES)
    mark("g_two")
    forward(LEAD, "lead", (2,))
    mark("i_near2")
    forward(REST, "rest", SIDES)
    mark("i_two2")
    forward(REST, "rest", (2,))
    mark("j_more")
    net.wait("pair", U.at[0])
    for d in range(1, chips):
        for part, axis in enumerate("yx"):
            net.start(U.at[part, pl.ds(6, TALL)], G.at[y, pl.ds(6, TALL), hh, spot], along(axis, d, 1 - part), "c1", "c1")

    mark("j_c0")

    @pl.when(first_half)
    def _():
        for s in SIDES:
            net.wait(("c0", s), C0.at[:, 0])
            piece = C0.at[0 if s < 0 else 1, ys(s)]
            net.start(piece, piece, along("y", -s), "c0far", "c0far")

    mark("k_leafin")
    arrive(LEAD)

    lane = iota((BLK, LANES), 1)
    sub = iota((BLK, LANES), 0)
    block_of = (lane // BLK) % BLK

    def tile_of(k, q, c, b):
        return G[k, q + b // TALL, b % 2, c, (b // 2) % 2]

    def gathered(k, q):
        return jnp.concatenate([tile_of(k, q, c, b) for c in range(TALL) for b in range(BLK)], axis=0)

    def start_leaves(m):
        zero = jnp.zeros((BLK, LANES), F32)
        diag = [[None] * TALL for _ in range(TALL)]
        inv = [[zero] * TALL for _ in range(TALL)]
        for c in range(TALL):
            inv[c][c] = jnp.where(sub == lane % BLK, 1.0, 0.0)
            for k in range(c + 1):
                total = zero
                for b in range(BLK):
                    total = jnp.where(block_of == b, tile_of(k, 3 * m, c, b), total)
                diag[c][k] = total
        for t in range(BLK * TALL):
            ct, jt = t // BLK, t % BLK
            index = (lane // BLK) * BLK + jt
            spread = [jnp.take_along_axis(diag[c][ct], index, axis=1) for c in range(ct, TALL)]
            pivot = 1.0 / spread[0][jt:jt + 1, :]
            below = jnp.where(sub > jt, spread[0], 0.0)
            for k in range(ct + 1):
                solved = inv[ct][k][jt:jt + 1, :] * pivot
                inv[ct][k] = jnp.where(sub == jt, solved, inv[ct][k] - below * solved)
                for c in range(ct + 1, TALL):
                    inv[c][k] = inv[c][k] - spread[c - ct] * solved
        full = [gathered(k, 3 * m) for k in range(cols)]
        for e in PAIR:
            LF[2 * m + e] = halves(full, e).reshape(TALL * BLK, BLK, WIDE)
            for c in range(TALL):
                PK[2 * m + e, c] = halves(inv[c], e)

    def double(m, nb):
        count, lanes = TALL * nb, BLK * nb
        size = BLK * count
        group = ((iota((BLK, WIDE), 1) % HALF) // BLK) // nb
        even = ((iota((size, WIDE), 1) % HALF) // BLK) // nb % 2 == 0

        def coupling(leaf):
            out = []
            for bb in range(nb):
                for c in range(TALL):
                    total = LF[leaf, c * BLK + nb + bb]
                    for s in range(3, BLK // nb, 2):
                        total = jnp.where(group == s - 1, LF[leaf, c * BLK + s * nb + bb], total)
                    out.append(total)
            return jnp.concatenate(out, axis=0)

        def spread(val, flip):
            tiles = val.reshape(count, BLK, WIDE)
            return jnp.concatenate([jnp.where(group == (b // nb) ^ flip, tiles[(b % nb) * TALL + c], 0.0)
                                    for c in range(TALL) for b in range(BLK)], axis=0)

        one, two = (PK[2 * m + e, 0:count].reshape(size, WIDE) for e in PAIR)
        temp = dot(jnp.where(even, coupling(2 * m), shift(coupling(2 * m + 1), lanes)),
                   spread(jnp.where(even, one, shift(two, lanes)), 0))
        corner = dot(jnp.where(even, shift(two, -lanes), one), spread(temp, 1))
        for e, (val, low) in enumerate(((one, corner), (two, shift(corner, -lanes)))):
            parts = (jnp.where(even, val, 0.0), jnp.where(even, -low, val))
            for half in PAIR:
                tiles = parts[half].reshape(count, BLK, WIDE)
                if nb < TALL:
                    PK[2 * m + e, half * count:(half + 1) * count] = tiles
                else:
                    for i in range(count):
                        LI[2 * m + e, (i % TALL) * BLK + half * TALL + i // TALL] = tiles[i]

    mark("l_base")
    start_leaves(0)
    mark("n_dbl1")
    double(0, 1)
    mark("n_dbl2")
    double(0, 2)
    mark("n_dbl4")
    double(0, TALL)
    mark("o_arr2")

    def leaf_inv(i):
        return LI[i].reshape(WIDE, WIDE)

    def turned(i):
        return leaf_inv((i + 2) % TALL)

    def coupling2(m):
        stacked = [jnp.concatenate([G[k, 3 * m + 2, b % 2, c, b // 2] for c in range(TALL) for b in range(TALL)], axis=0)
                   for k in range(cols)]
        top, bottom = halves(stacked, 0), halves(stacked, 1)
        return jnp.concatenate([val[quarter * c:quarter * (c + 1)] for c in range(TALL) for val in (top, bottom)], axis=0)

    def mine(i):
        r, l = iota((WIDE, WIDE), 0), iota((WIDE, WIDE), 1)
        own = CORES * x + r // LANES
        return jnp.where(((r // quarter) % TALL == i) & (l // HALF == own % cols) & (r % BLK == l % BLK)
                         & ((l % HALF) // BLK == 2 * ((r // BLK) % TALL) + own // cols), 1.0, 0.0)

    def put_w(ref, val):
        ref[...] = val.reshape(TALL, TALL, 2, BLK, LANES)
        return val

    def put_z(i, val):
        ZM[i] = val[:LANES]
        ZS[i] = val[LANES:]
        net.start(ZS.at[i], ZM.at[i], partner, "z", "z")
        return val

    def t_piece(side, step, k=None):
        xx = xs(step)
        return TG.at[side, xx // 2, pl.ds(2 * (xx % 2), 2) if k is None else 2 * (xx % 2) + k]

    def t_start(side, step, k, device, name, kind="t"):
        net.start(t_piece(side, step, k), t_piece(side, step, k), device, kind, (side, name))

    def t_send(side, val):
        t_piece(side, 0)[...] = val.reshape(CORES, TALL, TALL, BLK, LANES)
        for i in PAIR:
            for s in SIDES:
                k = i if s < 0 else 1 - i
                t_start(side, 0, k, along("x", -s), (s, i))
        t_start(side, 0, None, partner, "partner", "tpair")

    def t_near(side):
        for i in PAIR:
            for s in SIDES:
                k = i if s < 0 else 1 - i
                net.wait((side, (s, i)), t_piece(side, s, k))
                if i == 0:
                    t_start(side, s, k, along("x", -s), "far")
                t_start(side, s, k, partner, "partner", "tpair")

    def t_far(side):
        net.wait((side, "far"), t_piece(side, 2))
        t_start(side, 2, None, partner, "partner", "tpair")

    def c0_pair(n):
        return [jnp.concatenate([C0[k, c, :, LANES * n:LANES * (n + 1)] for k in range(CORES)], axis=0) for c in range(cols)]

    def own_columns(first, second):
        low = iota((first.shape[0], LANES), 1) < HALF
        out = []
        for val in (first, second):
            tile = jnp.where(y // 2 == 0, val[:, :LANES], val[:, LANES:])
            moved = pltpu.roll(tile, HALF, 1)
            out.append(jnp.where(y % 2 == 0, tile, moved) if val is first else jnp.where(y % 2 == 0, moved, tile))
        return jnp.where(low, out[0], out[1])

    def w_rows(ref):
        own = CORES * x
        return ref.at[..., own % cols, :, :, own // cols, :, :]

    mark("p_chain1")
    low_half = iota((WIDE, LANES), 1) < HALF
    blank = jnp.zeros((WIDE, WIDE), F32)

    def two_columns(one, two, coupling):
        head = own_columns(one, blank)
        return head, jnp.where(low_half, -dot(two, dot(coupling, head)), own_columns(blank, two))

    @pl.when(first_half)
    def _():
        head, tail = two_columns(leaf_inv(0), leaf_inv(1), coupling2(0))
        put_w(WL.at[0, :, 0], head)
        put_w(WL.at[0, :, 1], tail)

    @pl.when(core == 0)
    def _():
        z3 = put_z(3, dot(mine(3), turned(3)))
        put_z(2, dot(mine(2) - dot(z3, coupling2(0)), turned(2)))

    mark("q_c1")
    net.wait("c1", G.at[pl.ds(0, 3), pl.ds(0, 2), 0])

    def x_piece(step):
        xx = xs(step)
        return SX.at[xx // 2, pl.ds(2 * (xx % 2), 2)]

    @pl.when(first_half)
    def _():
        def own_rows(k):
            return jnp.concatenate(
                [G[k, 6 + i // 2, x // 2, 2 * (x % 2) + kk, i % 2] for kk in range(CORES) for i in range(BLK)], axis=0)

        product = dot(jnp.concatenate([own_rows(k) for k in range(cols)], axis=1), WL[0].reshape(2 * WIDE, LANES))
        x_piece(0)[...] = product.reshape(CORES, 2, TALL, BLK, LANES)
        for d in range(1, chips):
            net.start(x_piece(0), x_piece(0), along("x", d), "share", "share")

    @pl.when(core == 0)
    def _():
        lhs = [jnp.concatenate([ZM[i, HALF:], ZS[i, HALF:]], axis=0) for i in (2, 3)]
        YX[y] = sum(dot(lhs[i], gathered(y, 6 + 2 * i)) for i in PAIR)
        for d in range(1, cols):
            net.start(YX.at[y], YX.at[y], along("y", d), "share", "share")

    mark("s_c0")

    @pl.when(first_half)
    def _():
        net.wait("c0pair", C0.at[0, 0])
        net.wait("c0far", C0.at[0, pl.ds(0, 2)])
        TP[...] = dot(jnp.concatenate(c0_pair(0), axis=1), WL[0].reshape(2 * WIDE, LANES))

    mark("s_arr")
    arrive(REST)
    mark("s_other")
    start_leaves(1)
    double(1, 1)
    mark("s_dbl")
    double(1, 2)
    double(1, TALL)
    mark("t_V")

    @pl.when(first_half)
    def _():
        right = c0_pair(1)
        v3 = dot(halves(right, 1), leaf_inv(3))
        v2 = dot(halves(right, 0) - dot(v3, coupling2(1)), leaf_inv(2))
        VV[:, :WIDE] = v2
        VV[:, WIDE:] = v3
        t_send(1, own_columns(v2, v3))

    mark("t_share")
    net.wait("share", G.at[pl.ds(0, 3), pl.ds(0, 2), 0])
    mark("u_chain2")

    @pl.when(first_half)
    def _():
        for g in PAIR:
            for c in range(TALL):
                for i in range(BLK):
                    SS[(g * TALL + c) * BLK + i] = SX[i % 2, c, g, i // 2]
        shared = SS[...].reshape(2 * WIDE, LANES)
        t_send(0, TP[...] - dot(VV[...], shared))
        t_near(1)
        w2 = put_w(WL.at[1, :, 0], -dot(leaf_inv(2), shared[:WIDE]))
        put_w(WL.at[1, :, 1], -dot(leaf_inv(3), shared[WIDE:] + dot(coupling2(1), w2)))
        head, tail = two_columns(leaf_inv(2), leaf_inv(3), coupling2(1))
        put_w(WR.at[:, 0], head)
        put_w(WR.at[:, 1], tail)
        net.start(w_rows(WL), w_rows(WL), partner, "w", "w")
        net.start(w_rows(WR), w_rows(WR), partner, "w", "w")
        t_near(0)

    @pl.when(core == 0)
    def _():
        none = jnp.zeros((HALF, LANES), F32)
        tiles = [jnp.concatenate([none, YX[k, :HALF], none, YX[k, HALF:]], axis=0) for k in range(cols)]
        z1 = put_z(1, dot(mine(1) - halves(tiles, 1), turned(1)))
        put_z(0, dot(mine(0) - halves(tiles, 0) - dot(z1, coupling2(1)), turned(0)))
        net.wait("w", G.at[pl.ds(0, 3), 0, 0])

    mark("v_out")

    @pl.when(first_half)
    def _():
        net.wait("z", ZM)

    o_ref[upper, far] = jnp.zeros((LANES, WIDE), F32)
    for i in range(TALL):
        lines = slice(quarter * i, quarter * (i + 1))
        o_ref[lines, :LANES] = WL[i // 2, spot, i % 2, :, hh].reshape(quarter, LANES)
        o_ref[lines, LANES:WIDE] = WR[spot, i % 2, :, hh].reshape(quarter, LANES) if i >= 2 else jnp.zeros((quarter, LANES), F32)
    o_ref[lower, far] = jnp.concatenate([own_columns(ZM[2 * n], ZM[2 * n + 1]) for n in PAIR], axis=1)

    mark("v_near")

    @pl.when(first_half)
    def _():
        t_far(1)
        t_far(0)

    mark("v_tend")

    @pl.when(core == 0)
    def _():
        for side in PAIR:
            net.wait((side, "partner"), TG.at[side])

    def t_rows(i):
        return jnp.concatenate([jnp.concatenate([TG[side, b % 2, c, i, b // 2] for c in range(TALL) for b in range(BLK)], axis=0)
                                for side in PAIR], axis=1)

    mark("w_x21")
    o_ref[lower, near] = -sum(dot(ZM[i], t_rows(i)) for i in range(TALL))

    mark("x_end")
    for name in ("lead", "rest"):
        net.wait(name, G.at[pl.ds(0, 3), pl.ds(0, 3), 0], "send")
    net.wait("c1", G.at[pl.ds(0, 3), pl.ds(0, 2), 0], "send")
    net.wait("on", G.at[pl.ds(0, 3), pl.ds(0, 9), 0], "send")
    net.wait("share", G.at[pl.ds(0, 3), pl.ds(0, 2), 0], "send")
    net.wait("pair", U.at[0], "send")
    net.wait("c0", C0.at[0, pl.ds(0, 2)], "send")

    @pl.when(first_half)
    def _():
        net.wait("c0far", C0.at[0, pl.ds(0, 2)], "send")
        net.wait("t", G.at[pl.ds(0, 3), pl.ds(0, 8), 0], "send")
        net.wait("tpair", TG, "send")
        net.wait("w", G.at[pl.ds(0, 3), 0, 0], "send")

    @pl.when(core == 0)
    def _():
        net.wait("c0pair", C0.at[0, 0], "send")
        net.wait("z", ZM, "send")

    mark()
    counts = [len([key for key in net.names if key[0] == side]) for side in ("send", "recv")]
    assert counts == [send.shape[0], recv.shape[0]], counts


def solution(mesh):
    rows, cols = mesh.shape["row"], mesh.shape["col"]
    block_spec = P(("batch", "row"), "col")

    def device_body(local_l):
        vmem = functools.partial(pltpu.VMEM, dtype=F32)
        return pl.pallas_call(
            functools.partial(kernel, rows, cols),
            out_shape=jax.ShapeDtypeStruct(local_l.shape, F32),
            in_specs=[pl.BlockSpec(memory_space=pl.ANY)],
            out_specs=pl.BlockSpec(memory_space=pltpu.VMEM),
            scratch_shapes=[
                vmem(local_l.shape),
                vmem((2, GROUPS, 2, BLK, LANES)),
                vmem((cols, GROUPS, 2, TALL, 2, BLK, LANES)),
                vmem((CORES, cols, LANES, WIDE)),
                vmem((TALL, TALL * BLK, BLK, WIDE)),
                vmem((TALL, 2 * BLK, BLK, WIDE)),
                vmem((TALL, TALL * BLK, BLK, WIDE)),
                vmem((2, cols, 2, TALL, 2, BLK, LANES)),
                vmem((cols, 2, TALL, 2, BLK, LANES)),
                vmem((TALL, LANES, WIDE)),
                vmem((TALL, LANES, WIDE)),
                vmem((2, 2, TALL, TALL, TALL, BLK, LANES)),
                vmem((2, TALL, 2, TALL, BLK, LANES)),
                vmem((cols, LANES, LANES)),
                vmem((WIDE, 2 * WIDE)),
                vmem((2 * TALL * BLK, BLK, LANES)),
                vmem((WIDE, LANES)),
                pltpu.SemaphoreType.DMA((3,)),
                pltpu.SemaphoreType.DMA((13,)),
                pltpu.SemaphoreType.DMA((37,)),
            ],
            compiler_params=pltpu.CompilerParams(collective_id=0, has_side_effects=True),
        )(local_l)

    return jax.shard_map(device_body, mesh=mesh, in_specs=(block_spec,), out_specs=block_spec, check_vma=False)
```

```python
import functools

import jax
import jax.numpy as jnp
from jax import lax
from jax.experimental import pallas as pl
from jax.experimental.pallas import tpu as pltpu
from jax.sharding import PartitionSpec as P

BLK = 8
CORES = 2
LANES = 128
HALF = LANES // 2
WIDE = 2 * LANES
TALL = 4
GROUPS = 10
LEAD = (0, 1, 2)
REST = (3, 4, 5)
PAIR = range(2)
SIDES = (-1, 1)
STEPS = (1, -1, 2)
MESH = pl.DeviceIdType.MESH


class Marks:
    def __init__(self):
        self.scope = None

    def __call__(self, name=None):
        if self.scope is not None:
            self.scope.__exit__(None, None, None)
        self.scope = None if name is None else jax.named_scope(name)
        if name is not None:
            self.scope.__enter__()
F32 = jnp.float32


def dot(left, right):
    return jnp.dot(left, right, precision=lax.Precision.HIGHEST, preferred_element_type=F32)


def iota(shape, dim):
    return lax.broadcasted_iota(jnp.int32, shape, dim)


def halves(tiles, half):
    low = iota(tiles[0].shape, 1) < HALF
    out = []
    for first, second in ((tiles[0], tiles[1]), (tiles[2], tiles[3])):
        if half == 0:
            out.append(jnp.where(low, first, pltpu.roll(second, HALF, 1)))
        else:
            out.append(jnp.where(low, pltpu.roll(first, HALF, 1), second))
    return jnp.concatenate(out, axis=1)


class Net:
    def __init__(self, send, recv):
        self.send, self.recv, self.names = send, recv, {}

    def slot(self, side, name):
        held = [key for key in self.names if key[0] == side]
        return self.names.setdefault((side, name), len(held))

    def start(self, src, dst, device, send, recv):
        self.make(src, dst, device, send, recv).start()

    def make(self, src, dst, device, send, recv):
        return pltpu.make_async_remote_copy(
            src_ref=src, dst_ref=dst, send_sem=self.send.at[self.slot("send", send)], recv_sem=self.recv.at[self.slot("recv", recv)],
            device_id=device, device_id_type=MESH)

    def wait(self, name, like, side="recv"):
        sems = self.recv if side == "recv" else self.send
        pltpu.make_async_copy(like, like, sems.at[self.slot(side, name)]).wait()


def shift(val, lanes):
    return jnp.concatenate([pltpu.roll(val[:, LANES * i:LANES * (i + 1)], lanes % LANES, 1) for i in range(2)], axis=1)


def kernel(rows, cols, hbm_ref, o_ref, l_ref, U, G, C0, LF, PK, LI, WL, WR, ZM, ZS, TG, SX, YX, VV, SS, TP, load, send, recv):
    chips = rows // CORES
    row = lax.axis_index("row")
    y = lax.axis_index("col")
    x, core = row // CORES, row % CORES
    spot, hh = row % cols, row // cols
    net = Net(send, recv)
    first_half = core == 1

    def at(xx, cc, yy):
        return {"row": xx * CORES + cc, "col": yy}

    def xs(step):
        return lax.rem(x + step + chips, chips)

    def ys(step):
        return lax.rem(y + step + cols, cols)

    def along(axis, step, cc=core):
        return at(xs(step), cc, y) if axis == "x" else at(x, cc, ys(step))

    mark = Marks()
    mark("a_signal")
    upper, lower, near, far = pl.ds(0, LANES), pl.ds(LANES, LANES), pl.ds(0, WIDE), pl.ds(WIDE, WIDE)
    windows = [(upper, near), (lower, far), (lower, near)]
    loads = [pltpu.make_async_copy(hbm_ref.at[w], l_ref.at[w], load.at[i]) for i, w in enumerate(windows)]
    for made in loads:
        made.start()
    partner = at(x, 1 - core, y)
    barrier = pltpu.get_barrier_semaphore()
    peers = [partner] + [along(axis, d, cc) for axis in "xy" for d in range(1, chips) for cc in range(CORES)]
    for peer in peers:
        pl.semaphore_signal(barrier, inc=1, device_id=peer, device_id_type=MESH)

    mark("a_pack")
    quarter = LANES // TALL
    for part in range(2):
        loads[part].wait()
        piece = l_ref[part * LANES:(part + 1) * LANES, part * WIDE:(part + 1) * WIDE]
        low = iota((quarter, LANES), 1) < HALF
        band = [piece[quarter * i:quarter * (i + 1)] for i in range(TALL)]
        packed = [jnp.where(low, band[2 * m][:, LANES * m:LANES * (m + 1)], band[2 * m + 1][:, LANES * m:LANES * (m + 1)])
                  for m in PAIR]
        links = (band[1][:, :LANES], band[3][:, LANES:])
        links = [jnp.where(low[:2 * BLK], val[:2 * BLK], pltpu.roll(val[2 * BLK:], HALF, 1)) for val in links]
        tiles = []
        for m in (part, 1 - part):
            tiles += [packed[m].reshape(2, 2, BLK, LANES)[i] for i in PAIR] + [links[m].reshape(2, BLK, LANES)]
        for i in (2, 3):
            tiles += [band[i][:, :LANES].reshape(2, 2, BLK, LANES)[h] for h in PAIR]
        for g in range(GROUPS):
            U[part, g] = tiles[g]

        @pl.when(core == 1 - part)
        def _():
            for g in range(GROUPS):
                G[y, g, hh, spot] = tiles[g]

    loads[2].wait()
    C0[core, y] = l_ref[lower, near]
    mark("b_barrier")
    pl.semaphore_wait(barrier, len(peers))

    axis_first = "xyyyyx"

    def other(axis):
        return "y" if axis == "x" else "x"

    def source(g, f, s, k=None):
        xx, yy = (xs(f), ys(s)) if axis_first[g] == "x" else (xs(s), ys(f))
        return G.at[yy, g, xx // 2, pl.ds(2 * (xx % 2), 2) if k is None else 2 * (xx % 2) + k]

    def pass_on(g, f, s, k, step, name):
        piece = source(g, f, s, k)
        net.start(piece, piece, along(other(axis_first[g]), step), "on", name)

    def own(groups, name):
        lo, count = min(groups), len(groups)
        for step in STEPS:
            for axis in "xy":
                for part in range(2):
                    net.start(U.at[part, pl.ds(lo, count)], G.at[y, pl.ds(lo, count), hh, spot], along(axis, step, 1 - part),
                              name, (name, axis, -step if step < 2 else step))

    def forward(groups, name, steps):
        for step in steps:
            for axis in "xy":
                net.wait((name, axis, step), G.at[0, pl.ds(0, len(groups)), 0, pl.ds(0, 2)])
                for g in groups:
                    if axis_first[g] == axis:
                        for away in STEPS:
                            pass_on(g, step, 0, None, away, (g, "far"))

    def arrive(groups):
        for g in groups:
            net.wait((g, "far"), G.at[pl.ds(0, 3), g, :, pl.ds(0, 3)])

    mark("d_own")
    own(LEAD, "lead")
    net.start(U.at[core], G.at[y, :, hh, spot], partner, "pair", "pair")
    mark("e_near")
    forward(LEAD, "lead", SIDES)
    own(REST, "rest")
    mark("g_two")
    forward(LEAD, "lead", (2,))
    mark("h_more")
    for d in range(1, chips):
        for part, axis in enumerate("yx"):
            net.start(U.at[part, pl.ds(6, TALL)], G.at[y, pl.ds(6, TALL), hh, spot], along(axis, d, 1 - part), "c1", "c1")
    for s in SIDES:
        net.start(l_ref.at[lower, near], C0.at[core, y], along("y", -s, 1), "c0", ("c0", s))

    @pl.when(core == 0)
    def _():
        net.start(l_ref.at[lower, near], C0.at[core, y], partner, "c0pair", "c0pair")

    mark("i_near2")
    forward(REST, "rest", SIDES)
    mark("i_two2")
    forward(REST, "rest", (2,))
    mark("j_more")
    net.wait("pair", U.at[0])
    mark("k_leafin")
    arrive(LEAD)

    lane = iota((BLK, LANES), 1)
    sub = iota((BLK, LANES), 0)
    block_of = (lane // BLK) % BLK

    def tile_of(k, q, c, b):
        return G[k, q + b // TALL, b % 2, c, (b // 2) % 2]

    def gathered(k, q):
        return jnp.concatenate([tile_of(k, q, c, b) for c in range(TALL) for b in range(BLK)], axis=0)

    def start_leaves(m):
        zero = jnp.zeros((BLK, LANES), F32)
        diag = [[None] * TALL for _ in range(TALL)]
        inv = [[zero] * TALL for _ in range(TALL)]
        for c in range(TALL):
            inv[c][c] = jnp.where(sub == lane % BLK, 1.0, 0.0)
            for k in range(c + 1):
                total = zero
                for b in range(BLK):
                    total = jnp.where(block_of == b, tile_of(k, 3 * m, c, b), total)
                diag[c][k] = total
        for t in range(BLK * TALL):
            ct, jt = t // BLK, t % BLK
            index = (lane // BLK) * BLK + jt
            spread = [jnp.take_along_axis(diag[c][ct], index, axis=1) for c in range(ct, TALL)]
            pivot = 1.0 / spread[0][jt:jt + 1, :]
            below = jnp.where(sub > jt, spread[0], 0.0)
            for k in range(ct + 1):
                solved = inv[ct][k][jt:jt + 1, :] * pivot
                inv[ct][k] = jnp.where(sub == jt, solved, inv[ct][k] - below * solved)
                for c in range(ct + 1, TALL):
                    inv[c][k] = inv[c][k] - spread[c - ct] * solved
        full = [gathered(k, 3 * m) for k in range(cols)]
        for e in PAIR:
            LF[2 * m + e] = halves(full, e).reshape(TALL * BLK, BLK, WIDE)
            for c in range(TALL):
                PK[2 * m + e, c] = halves(inv[c], e)

    def double(m, nb):
        count, lanes = TALL * nb, BLK * nb
        size = BLK * count
        group = ((iota((BLK, WIDE), 1) % HALF) // BLK) // nb
        even = ((iota((size, WIDE), 1) % HALF) // BLK) // nb % 2 == 0

        def coupling(leaf):
            out = []
            for bb in range(nb):
                for c in range(TALL):
                    total = LF[leaf, c * BLK + nb + bb]
                    for s in range(3, BLK // nb, 2):
                        total = jnp.where(group == s - 1, LF[leaf, c * BLK + s * nb + bb], total)
                    out.append(total)
            return jnp.concatenate(out, axis=0)

        def spread(val, flip):
            tiles = val.reshape(count, BLK, WIDE)
            return jnp.concatenate([jnp.where(group == (b // nb) ^ flip, tiles[(b % nb) * TALL + c], 0.0)
                                    for c in range(TALL) for b in range(BLK)], axis=0)

        one, two = (PK[2 * m + e, 0:count].reshape(size, WIDE) for e in PAIR)
        temp = dot(jnp.where(even, coupling(2 * m), shift(coupling(2 * m + 1), lanes)),
                   spread(jnp.where(even, one, shift(two, lanes)), 0))
        corner = dot(jnp.where(even, shift(two, -lanes), one), spread(temp, 1))
        for e, (val, low) in enumerate(((one, corner), (two, shift(corner, -lanes)))):
            parts = (jnp.where(even, val, 0.0), jnp.where(even, -low, val))
            for half in PAIR:
                tiles = parts[half].reshape(count, BLK, WIDE)
                if nb < TALL:
                    PK[2 * m + e, half * count:(half + 1) * count] = tiles
                else:
                    for i in range(count):
                        LI[2 * m + e, (i % TALL) * BLK + half * TALL + i // TALL] = tiles[i]

    mark("l_base")
    start_leaves(0)
    mark("n_dbl1")
    double(0, 1)
    mark("n_c0")

    @pl.when(first_half)
    def _():
        for s in SIDES:
            net.wait(("c0", s), C0.at[:, 0])
            piece = C0.at[0 if s < 0 else 1, ys(s)]
            net.start(piece, piece, along("y", -s), "c0far", "c0far")

    mark("n_dbl2")
    double(0, 2)
    mark("n_dbl4")
    double(0, TALL)
    mark("o_arr2")

    def leaf_inv(i):
        return LI[i].reshape(WIDE, WIDE)

    def turned(i):
        return leaf_inv((i + 2) % TALL)

    def coupling2(m):
        stacked = [jnp.concatenate([G[k, 3 * m + 2, b % 2, c, b // 2] for c in range(TALL) for b in range(TALL)], axis=0)
                   for k in range(cols)]
        top, bottom = halves(stacked, 0), halves(stacked, 1)
        return jnp.concatenate([val[quarter * c:quarter * (c + 1)] for c in range(TALL) for val in (top, bottom)], axis=0)

    def mine(i):
        r, l = iota((WIDE, WIDE), 0), iota((WIDE, WIDE), 1)
        own = CORES * x + r // LANES
        return jnp.where(((r // quarter) % TALL == i) & (l // HALF == own % cols) & (r % BLK == l % BLK)
                         & ((l % HALF) // BLK == 2 * ((r // BLK) % TALL) + own // cols), 1.0, 0.0)

    def put_w(ref, val):
        ref[...] = val.reshape(TALL, TALL, 2, BLK, LANES)
        return val

    def put_z(i, val):
        ZM[i] = val[:LANES]
        ZS[i] = val[LANES:]
        net.start(ZS.at[i], ZM.at[i], partner, "z", "z")
        return val

    def t_piece(side, step, k=None):
        xx = xs(step)
        return TG.at[side, xx // 2, pl.ds(2 * (xx % 2), 2) if k is None else 2 * (xx % 2) + k]

    def t_start(side, step, k, device, name, kind="t"):
        net.start(t_piece(side, step, k), t_piece(side, step, k), device, kind, (side, name))

    def t_send(side, val):
        t_piece(side, 0)[...] = val.reshape(CORES, TALL, TALL, BLK, LANES)
        for i in PAIR:
            for s in SIDES:
                k = i if s < 0 else 1 - i
                t_start(side, 0, k, along("x", -s), (s, i))
        t_start(side, 0, None, partner, "partner", "tpair")

    def t_near(side):
        for i in PAIR:
            for s in SIDES:
                k = i if s < 0 else 1 - i
                net.wait((side, (s, i)), t_piece(side, s, k))
                if i == 0:
                    t_start(side, s, k, along("x", -s), "far")
                t_start(side, s, k, partner, "partner", "tpair")

    def t_far(side):
        net.wait((side, "far"), t_piece(side, 2))
        t_start(side, 2, None, partner, "partner", "tpair")

    def c0_pair(n):
        return [jnp.concatenate([C0[k, c, :, LANES * n:LANES * (n + 1)] for k in range(CORES)], axis=0) for c in range(cols)]

    def own_columns(first, second):
        low = iota((first.shape[0], LANES), 1) < HALF
        out = []
        for val in (first, second):
            tile = jnp.where(y // 2 == 0, val[:, :LANES], val[:, LANES:])
            moved = pltpu.roll(tile, HALF, 1)
            out.append(jnp.where(y % 2 == 0, tile, moved) if val is first else jnp.where(y % 2 == 0, moved, tile))
        return jnp.where(low, out[0], out[1])

    def w_rows(ref):
        own = CORES * x
        return ref.at[..., own % cols, :, :, own // cols, :, :]

    mark("p_chain1")
    low_half = iota((WIDE, LANES), 1) < HALF
    blank = jnp.zeros((WIDE, WIDE), F32)

    def two_columns(one, two, coupling):
        head = own_columns(one, blank)
        return head, jnp.where(low_half, -dot(two, dot(coupling, head)), own_columns(blank, two))

    @pl.when(first_half)
    def _():
        head, tail = two_columns(leaf_inv(0), leaf_inv(1), coupling2(0))
        put_w(WL.at[0, :, 0], head)
        put_w(WL.at[0, :, 1], tail)

    @pl.when(core == 0)
    def _():
        z3 = put_z(3, dot(mine(3), turned(3)))
        put_z(2, dot(mine(2) - dot(z3, coupling2(0)), turned(2)))

    mark("q_c1")
    net.wait("c1", G.at[pl.ds(0, 3), pl.ds(0, 2), 0])

    def x_piece(step):
        xx = xs(step)
        return SX.at[xx // 2, pl.ds(2 * (xx % 2), 2)]

    @pl.when(first_half)
    def _():
        def own_rows(k):
            return jnp.concatenate(
                [G[k, 6 + i // 2, x // 2, 2 * (x % 2) + kk, i % 2] for kk in range(CORES) for i in range(BLK)], axis=0)

        product = dot(jnp.concatenate([own_rows(k) for k in range(cols)], axis=1), WL[0].reshape(2 * WIDE, LANES))
        x_piece(0)[...] = product.reshape(CORES, 2, TALL, BLK, LANES)
        for d in range(1, chips):
            net.start(x_piece(0), x_piece(0), along("x", d), "share", "share")

    @pl.when(core == 0)
    def _():
        lhs = [jnp.concatenate([ZM[i, HALF:], ZS[i, HALF:]], axis=0) for i in (2, 3)]
        YX[y] = sum(dot(lhs[i], gathered(y, 6 + 2 * i)) for i in PAIR)
        for d in range(1, cols):
            net.start(YX.at[y], YX.at[y], along("y", d), "share", "share")

    mark("s_c0")

    @pl.when(first_half)
    def _():
        net.wait("c0pair", C0.at[0, 0])
        net.wait("c0far", C0.at[0, pl.ds(0, 2)])
        TP[...] = dot(jnp.concatenate(c0_pair(0), axis=1), WL[0].reshape(2 * WIDE, LANES))

    mark("s_arr")
    arrive(REST)
    mark("s_other")
    start_leaves(1)
    double(1, 1)
    mark("s_dbl")
    double(1, 2)
    double(1, TALL)
    mark("t_V")

    @pl.when(first_half)
    def _():
        right = c0_pair(1)
        v3 = dot(halves(right, 1), leaf_inv(3))
        v2 = dot(halves(right, 0) - dot(v3, coupling2(1)), leaf_inv(2))
        VV[:, :WIDE] = v2
        VV[:, WIDE:] = v3
        t_send(1, own_columns(v2, v3))

    mark("t_share")
    net.wait("share", G.at[pl.ds(0, 3), pl.ds(0, 2), 0])
    mark("u_chain2")

    @pl.when(first_half)
    def _():
        for g in PAIR:
            for c in range(TALL):
                for i in range(BLK):
                    SS[(g * TALL + c) * BLK + i] = SX[i % 2, c, g, i // 2]
        shared = SS[...].reshape(2 * WIDE, LANES)
        t_send(0, TP[...] - dot(VV[...], shared))
        t_near(1)
        w2 = put_w(WL.at[1, :, 0], -dot(leaf_inv(2), shared[:WIDE]))
        put_w(WL.at[1, :, 1], -dot(leaf_inv(3), shared[WIDE:] + dot(coupling2(1), w2)))
        head, tail = two_columns(leaf_inv(2), leaf_inv(3), coupling2(1))
        put_w(WR.at[:, 0], head)
        put_w(WR.at[:, 1], tail)
        net.start(w_rows(WL), w_rows(WL), partner, "w", "w")
        net.start(w_rows(WR), w_rows(WR), partner, "w", "w")
        t_near(0)

    @pl.when(core == 0)
    def _():
        none = jnp.zeros((HALF, LANES), F32)
        tiles = [jnp.concatenate([none, YX[k, :HALF], none, YX[k, HALF:]], axis=0) for k in range(cols)]
        z1 = put_z(1, dot(mine(1) - halves(tiles, 1), turned(1)))
        put_z(0, dot(mine(0) - halves(tiles, 0) - dot(z1, coupling2(1)), turned(0)))
        net.wait("w", G.at[pl.ds(0, 3), 0, 0])

    mark("v_out")

    @pl.when(first_half)
    def _():
        net.wait("z", ZM)

    o_ref[upper, far] = jnp.zeros((LANES, WIDE), F32)
    for i in range(TALL):
        lines = slice(quarter * i, quarter * (i + 1))
        o_ref[lines, :LANES] = WL[i // 2, spot, i % 2, :, hh].reshape(quarter, LANES)
        o_ref[lines, LANES:WIDE] = WR[spot, i % 2, :, hh].reshape(quarter, LANES) if i >= 2 else jnp.zeros((quarter, LANES), F32)
    o_ref[lower, far] = jnp.concatenate([own_columns(ZM[2 * n], ZM[2 * n + 1]) for n in PAIR], axis=1)

    mark("v_near")

    @pl.when(first_half)
    def _():
        t_far(1)
        t_far(0)

    mark("v_tend")

    @pl.when(core == 0)
    def _():
        for side in PAIR:
            net.wait((side, "partner"), TG.at[side])

    def t_rows(i):
        return jnp.concatenate([jnp.concatenate([TG[side, b % 2, c, i, b // 2] for c in range(TALL) for b in range(BLK)], axis=0)
                                for side in PAIR], axis=1)

    mark("w_x21")
    o_ref[lower, near] = -sum(dot(ZM[i], t_rows(i)) for i in range(TALL))

    mark("x_end")
    for name in ("lead", "rest"):
        net.wait(name, G.at[pl.ds(0, 3), pl.ds(0, 3), 0], "send")
    net.wait("c1", G.at[pl.ds(0, 3), pl.ds(0, 2), 0], "send")
    net.wait("on", G.at[pl.ds(0, 3), pl.ds(0, 9), 0], "send")
    net.wait("share", G.at[pl.ds(0, 3), pl.ds(0, 2), 0], "send")
    net.wait("pair", U.at[0], "send")
    net.wait("c0", C0.at[0, pl.ds(0, 2)], "send")

    @pl.when(first_half)
    def _():
        net.wait("c0far", C0.at[0, pl.ds(0, 2)], "send")
        net.wait("t", G.at[pl.ds(0, 3), pl.ds(0, 8), 0], "send")
        net.wait("tpair", TG, "send")
        net.wait("w", G.at[pl.ds(0, 3), 0, 0], "send")

    @pl.when(core == 0)
    def _():
        net.wait("c0pair", C0.at[0, 0], "send")
        net.wait("z", ZM, "send")

    mark()
    counts = [len([key for key in net.names if key[0] == side]) for side in ("send", "recv")]
    assert counts == [send.shape[0], recv.shape[0]], counts


def solution(mesh):
    rows, cols = mesh.shape["row"], mesh.shape["col"]
    block_spec = P(("batch", "row"), "col")

    def device_body(local_l):
        vmem = functools.partial(pltpu.VMEM, dtype=F32)
        return pl.pallas_call(
            functools.partial(kernel, rows, cols),
            out_shape=jax.ShapeDtypeStruct(local_l.shape, F32),
            in_specs=[pl.BlockSpec(memory_space=pl.ANY)],
            out_specs=pl.BlockSpec(memory_space=pltpu.VMEM),
            scratch_shapes=[
                vmem(local_l.shape),
                vmem((2, GROUPS, 2, BLK, LANES)),
                vmem((cols, GROUPS, 2, TALL, 2, BLK, LANES)),
                vmem((CORES, cols, LANES, WIDE)),
                vmem((TALL, TALL * BLK, BLK, WIDE)),
                vmem((TALL, 2 * BLK, BLK, WIDE)),
                vmem((TALL, TALL * BLK, BLK, WIDE)),
                vmem((2, cols, 2, TALL, 2, BLK, LANES)),
                vmem((cols, 2, TALL, 2, BLK, LANES)),
                vmem((TALL, LANES, WIDE)),
                vmem((TALL, LANES, WIDE)),
                vmem((2, 2, TALL, TALL, TALL, BLK, LANES)),
                vmem((2, TALL, 2, TALL, BLK, LANES)),
                vmem((cols, LANES, LANES)),
                vmem((WIDE, 2 * WIDE)),
                vmem((2 * TALL * BLK, BLK, LANES)),
                vmem((WIDE, LANES)),
                pltpu.SemaphoreType.DMA((3,)),
                pltpu.SemaphoreType.DMA((13,)),
                pltpu.SemaphoreType.DMA((37,)),
            ],
            compiler_params=pltpu.CompilerParams(collective_id=0, has_side_effects=True),
        )(local_l)

    return jax.shard_map(device_body, mesh=mesh, in_specs=(block_spec,), out_specs=block_spec, check_vma=False)
```

```python
import functools

import jax
import jax.numpy as jnp
from jax import lax
from jax.experimental import pallas as pl
from jax.experimental.pallas import tpu as pltpu
from jax.sharding import PartitionSpec as P

BLK = 8
CORES = 2
LANES = 128
HALF = LANES // 2
WIDE = 2 * LANES
TALL = 4
GROUPS = 5
LEAVES = range(2)
PAIR = range(2)
SIDES = (-1, 1)
MESH = pl.DeviceIdType.MESH


class Marks:
    def __init__(self):
        self.scope = None

    def __call__(self, name=None):
        if self.scope is not None:
            self.scope.__exit__(None, None, None)
        self.scope = None if name is None else jax.named_scope(name)
        if name is not None:
            self.scope.__enter__()
F32 = jnp.float32


def dot(left, right):
    return jnp.dot(left, right, precision=lax.Precision.HIGHEST, preferred_element_type=F32)


def iota(shape, dim):
    return lax.broadcasted_iota(jnp.int32, shape, dim)


def halves(tiles, half):
    low = iota(tiles[0].shape, 1) < HALF
    out = []
    for first, second in ((tiles[0], tiles[1]), (tiles[2], tiles[3])):
        if half == 0:
            out.append(jnp.where(low, first, pltpu.roll(second, HALF, 1)))
        else:
            out.append(jnp.where(low, pltpu.roll(first, HALF, 1), second))
    return jnp.concatenate(out, axis=1)


class Net:
    def __init__(self, send, recv):
        self.send, self.recv, self.names = send, recv, {}

    def slot(self, side, name):
        held = [key for key in self.names if key[0] == side]
        return self.names.setdefault((side, name), len(held))

    def start(self, src, dst, device, send, recv):
        self.make(src, dst, device, send, recv).start()

    def make(self, src, dst, device, send, recv):
        return pltpu.make_async_remote_copy(
            src_ref=src, dst_ref=dst, send_sem=self.send.at[self.slot("send", send)], recv_sem=self.recv.at[self.slot("recv", recv)],
            device_id=device, device_id_type=MESH)

    def wait(self, name, like, side="recv"):
        sems = self.recv if side == "recv" else self.send
        pltpu.make_async_copy(like, like, sems.at[self.slot(side, name)]).wait()


def shift(val, lanes):
    return jnp.concatenate([pltpu.roll(val[:, LANES * i:LANES * (i + 1)], lanes % LANES, 1) for i in range(2)], axis=1)


def kernel(rows, cols, hbm_ref, o_ref, l_ref, U, G, C0, LF, PK, LI, WL, WR, ZM, ZS, TG, SX, YX, VV, SS, TP, load, send, recv):
    chips = rows // CORES
    row = lax.axis_index("row")
    y = lax.axis_index("col")
    x, core = row // CORES, row % CORES
    spot, hh = row % cols, row // cols
    net = Net(send, recv)
    first_half = core == 1

    def at(xx, cc, yy):
        return {"row": xx * CORES + cc, "col": yy}

    def xs(step):
        return lax.rem(x + step + chips, chips)

    def ys(step):
        return lax.rem(y + step + cols, cols)

    def along(axis, step, cc=core):
        return at(xs(step), cc, y) if axis == "x" else at(x, cc, ys(step))

    mark = Marks()
    mark("a_signal")
    upper, lower, near, far = pl.ds(0, LANES), pl.ds(LANES, LANES), pl.ds(0, WIDE), pl.ds(WIDE, WIDE)
    windows = [(upper, near), (lower, far), (lower, near)]
    loads = [pltpu.make_async_copy(hbm_ref.at[w], l_ref.at[w], load.at[i]) for i, w in enumerate(windows)]
    for made in loads:
        made.start()
    partner = at(x, 1 - core, y)
    barrier = pltpu.get_barrier_semaphore()
    peers = [partner] + [along(axis, d, cc) for axis in "xy" for d in range(1, chips) for cc in range(CORES)]
    for peer in peers:
        pl.semaphore_signal(barrier, inc=1, device_id=peer, device_id_type=MESH)

    mark("a_pack")
    quarter = LANES // TALL
    for part in range(2):
        loads[part].wait()
        piece = l_ref[part * LANES:(part + 1) * LANES, part * WIDE:(part + 1) * WIDE]
        low = iota((quarter, LANES), 1) < HALF
        band = [piece[quarter * i:quarter * (i + 1)] for i in range(TALL)]
        packed = [jnp.where(low, band[2 * m][:, LANES * m:LANES * (m + 1)], band[2 * m + 1][:, LANES * m:LANES * (m + 1)])
                  for m in PAIR]
        packed.append(jnp.where(low, band[1][:, :LANES], pltpu.roll(band[3][:, LANES:], HALF, 1)))
        packed += [band[2][:, :LANES], band[3][:, :LANES]]
        tiles = [val.reshape(TALL, BLK, LANES) for val in packed]
        for g in range(GROUPS):
            U[part, g] = tiles[g]

        @pl.when(core == 1 - part)
        def _():
            for g in range(GROUPS):
                G[y, g, hh, spot] = tiles[g]

    loads[2].wait()
    C0[core, y] = l_ref[lower, near]
    mark("b_barrier")
    pl.semaphore_wait(barrier, len(peers))

    axis_first = ["x", "y", "y"]

    def other(axis):
        return "y" if axis == "x" else "x"

    def source(g, f, s, k=None):
        xx, yy = (xs(f), ys(s)) if axis_first[g] == "x" else (xs(s), ys(f))
        return G.at[yy, g, xx // 2, pl.ds(2 * (xx % 2), 2) if k is None else 2 * (xx % 2) + k]

    def pass_on(g, f, s, k, step, name):
        piece = source(g, f, s, k)
        net.start(piece, piece, along(other(axis_first[g]), step), g, name)

    def pass_leaf(g, f):
        for s in SIDES:
            pass_on(g, f, 0, None, -s, (g, "far") if f == 2 else (g, f, s))
        if f == 2:
            pass_on(g, f, 0, None, 2, (g, "far"))

    def half_on(g, f, s):
        pass_on(g, f, s, 0 if s < 0 else 1, -s, (g, "far"))

    mark("d_own")
    for axis in "xy":
        for step in SIDES:
            for part in range(2):
                net.start(U.at[part, pl.ds(0, 2)], G.at[y, pl.ds(0, 2), hh, spot], along(axis, step, 1 - part), "leaf", ("leaf", axis, -step))
    for g in LEAVES:
        for part in range(2):
            net.start(U.at[part, g], G.at[y, g, hh, spot], along(axis_first[g], 2, 1 - part), "leaf", (g, "two"))
    net.start(U.at[core], G.at[y, :, hh, spot], partner, "pair", "pair")

    def near_by(groups, name, count):
        for step in SIDES:
            for axis in "xy":
                net.wait((name, axis, step), G.at[0, pl.ds(0, count), 0, pl.ds(0, 2)])
                for g in groups:
                    if axis_first[g] == axis:
                        pass_leaf(g, step)
                    else:
                        half_on(g, 0, step)

    def two_away(groups):
        for g in groups:
            net.wait((g, "two"), G.at[0, 0, 0, pl.ds(0, 2)])
            pass_leaf(g, 2)

    def across(groups):
        for f in SIDES:
            for s in SIDES:
                for g in groups:
                    net.wait((g, f, s), source(g, f, s))
                    half_on(g, f, s)

    mark("e_near")
    near_by(LEAVES, "leaf", 2)
    for part in range(2):
        for axis in "xy":
            for step in SIDES:
                net.start(U.at[part, 2], G.at[y, 2, hh, spot], along(axis, step, 1 - part), "link", ("link", axis, -step))
        net.start(U.at[part, 2], G.at[y, 2, hh, spot], along(axis_first[2], 2, 1 - part), "link", (2, "two"))
    mark("g_two")
    two_away(LEAVES)
    mark("h_diag")
    across(LEAVES)
    net.wait("pair", U.at[0])
    mark("i_near2")
    near_by((2,), "link", 1)
    mark("j_second")
    for s in SIDES:
        net.start(l_ref.at[lower, near], C0.at[core, y], along("y", -s, 1), "c0", ("c0", s))

    @pl.when(core == 0)
    def _():
        net.start(l_ref.at[lower, near], C0.at[core, y], partner, "c0pair", "c0pair")

    for d in range(1, chips):
        for part, axis in enumerate("yx"):
            net.start(U.at[part, pl.ds(3, 2)], G.at[y, pl.ds(3, 2), hh, spot], along(axis, d, 1 - part), "rest", "c1")

    mark("k_leafin")
    for g in LEAVES:
        net.wait((g, "far"), G.at[pl.ds(0, 3), g, 0])

    two_away((2,))
    mark("l_base")
    lane = iota((BLK, LANES), 1)
    sub = iota((BLK, LANES), 0)
    block_of = (lane // BLK) % BLK
    diag = [[[None] * TALL for _ in range(TALL)] for _ in PAIR]
    inv = [[[None] * TALL for _ in range(TALL)] for _ in PAIR]
    for m in PAIR:
        for c in range(TALL):
            for k in range(c + 1):
                total = jnp.zeros((BLK, LANES), F32)
                for b in range(BLK):
                    total = jnp.where(block_of == b, G[k, m, b % 2, c, b // 2], total)
                diag[m][c][k] = total
                inv[m][c][k] = jnp.where(sub == lane % BLK, 1.0, 0.0) if c == k else jnp.zeros((BLK, LANES), F32)
    for t in range(BLK * TALL):
        ct, jt = t // BLK, t % BLK
        index = (lane // BLK) * BLK + jt
        for m in PAIR:
            spread = [jnp.take_along_axis(diag[m][c][ct], index, axis=1) for c in range(ct, TALL)]
            pivot = 1.0 / spread[0][jt:jt + 1, :]
            below = jnp.where(sub > jt, spread[0], 0.0)
            for k in range(ct + 1):
                solved = inv[m][ct][k][jt:jt + 1, :] * pivot
                inv[m][ct][k] = jnp.where(sub == jt, solved, inv[m][ct][k] - below * solved)
                for c in range(ct + 1, TALL):
                    inv[m][c][k] = inv[m][c][k] - spread[c - ct] * solved
    for m in PAIR:
        for c in range(TALL):
            tiles = [inv[m][c][k] if k <= c else jnp.zeros((BLK, LANES), F32) for k in range(TALL)]
            for e in PAIR:
                PK[2 * m + e, c] = halves(tiles, e)

    def gathered(k, g):
        return jnp.concatenate([G[k, g, b % 2, c, b // 2] for c in range(TALL) for b in range(BLK)], axis=0)

    mark("m_sep")
    for m in PAIR:
        tiles = [gathered(k, m) for k in range(cols)]
        for e in PAIR:
            LF[2 * m + e] = halves(tiles, e).reshape(TALL * BLK, BLK, WIDE)

    def double(m, nb):
        count, lanes = TALL * nb, BLK * nb
        size = BLK * count
        group = ((iota((BLK, WIDE), 1) % HALF) // BLK) // nb
        even = ((iota((size, WIDE), 1) % HALF) // BLK) // nb % 2 == 0

        def coupling(leaf):
            out = []
            for bb in range(nb):
                for c in range(TALL):
                    total = LF[leaf, c * BLK + nb + bb]
                    for s in range(3, BLK // nb, 2):
                        total = jnp.where(group == s - 1, LF[leaf, c * BLK + s * nb + bb], total)
                    out.append(total)
            return jnp.concatenate(out, axis=0)

        def spread(val, flip):
            tiles = val.reshape(count, BLK, WIDE)
            return jnp.concatenate([jnp.where(group == (b // nb) ^ flip, tiles[(b % nb) * TALL + c], 0.0)
                                    for c in range(TALL) for b in range(BLK)], axis=0)

        one, two = (PK[2 * m + e, 0:count].reshape(size, WIDE) for e in PAIR)
        temp = dot(jnp.where(even, coupling(2 * m), shift(coupling(2 * m + 1), lanes)),
                   spread(jnp.where(even, one, shift(two, lanes)), 0))
        corner = dot(jnp.where(even, shift(two, -lanes), one), spread(temp, 1))
        for e, (val, low) in enumerate(((one, corner), (two, shift(corner, -lanes)))):
            parts = (jnp.where(even, val, 0.0), jnp.where(even, -low, val))
            for half in PAIR:
                tiles = parts[half].reshape(count, BLK, WIDE)
                if nb < TALL:
                    PK[2 * m + e, half * count:(half + 1) * count] = tiles
                else:
                    for i in range(count):
                        LI[2 * m + e, (i % TALL) * BLK + half * TALL + i // TALL] = tiles[i]

    mark("n_dbl1")
    for m in PAIR:
        double(m, 1)
    mark("n_two2")
    across((2,))
    mark("n_c0")

    @pl.when(first_half)
    def _():
        for s in SIDES:
            net.wait(("c0", s), C0.at[:, 0])
            piece = C0.at[0 if s < 0 else 1, ys(s)]
            net.start(piece, piece, along("y", -s), "c0far", "c0far")

    mark("n_dbl2")
    for m in PAIR:
        double(m, 2)
    mark("n_dbl4")
    for m in PAIR:
        double(m, 4)
    mark("o_arr2")
    net.wait((2, "far"), G.at[pl.ds(0, 3), 2, 0])

    def leaf_inv(i):
        return LI[i].reshape(WIDE, WIDE)

    def coupling2(m):
        return halves([gathered(k, 2) for k in range(cols)], m)

    def mine(i):
        r, l = iota((WIDE, WIDE), 0), iota((WIDE, WIDE), 1)
        own = CORES * x + r // LANES
        return jnp.where(((r // quarter) % TALL == i) & (l // HALF == own % cols) & (r % BLK == l % BLK)
                         & ((l % HALF) // BLK == 2 * ((r // BLK) % TALL) + own // cols), 1.0, 0.0)

    def put_w(ref, val):
        ref[...] = val.reshape(TALL, TALL, 2, BLK, LANES)
        return val

    def put_z(i, val):
        ZM[i] = val[:LANES]
        ZS[i] = val[LANES:]
        net.start(ZS.at[i], ZM.at[i], partner, "z", "z")
        return val

    def t_piece(side, step, k=None):
        xx = xs(step)
        return TG.at[side, xx // 2, pl.ds(2 * (xx % 2), 2) if k is None else 2 * (xx % 2) + k]

    def t_start(side, step, k, device, name, kind="t"):
        net.start(t_piece(side, step, k), t_piece(side, step, k), device, kind, (side, name))

    def t_send(side, val):
        t_piece(side, 0)[...] = val.reshape(CORES, TALL, TALL, BLK, LANES)
        for i in PAIR:
            for s in SIDES:
                k = i if s < 0 else 1 - i
                t_start(side, 0, k, along("x", -s), (s, i))
        t_start(side, 0, None, partner, "partner", "tpair")

    def t_near(side):
        for i in PAIR:
            for s in SIDES:
                k = i if s < 0 else 1 - i
                net.wait((side, (s, i)), t_piece(side, s, k))
                if i == 0:
                    t_start(side, s, k, along("x", -s), "far")
                t_start(side, s, k, partner, "partner", "tpair")

    def t_far(side):
        net.wait((side, "far"), t_piece(side, 2))
        t_start(side, 2, None, partner, "partner", "tpair")

    def c0_pair(n):
        return [jnp.concatenate([C0[k, c, :, LANES * n:LANES * (n + 1)] for k in range(CORES)], axis=0) for c in range(cols)]

    def own_columns(first, second):
        low = iota((first.shape[0], LANES), 1) < HALF
        out = []
        for val in (first, second):
            tile = jnp.where(y // 2 == 0, val[:, :LANES], val[:, LANES:])
            moved = pltpu.roll(tile, HALF, 1)
            out.append(jnp.where(y % 2 == 0, tile, moved) if val is first else jnp.where(y % 2 == 0, moved, tile))
        return jnp.where(low, out[0], out[1])

    def w_rows(ref):
        own = CORES * x
        return ref.at[..., own % cols, :, :, own // cols, :, :]

    mark("p_chain1")
    low_half = iota((WIDE, LANES), 1) < HALF
    blank = jnp.zeros((WIDE, WIDE), F32)

    def two_columns(one, two, coupling):
        head = own_columns(one, blank)
        return head, jnp.where(low_half, -dot(two, dot(coupling, head)), own_columns(blank, two))

    @pl.when(first_half)
    def _():
        head, tail = two_columns(leaf_inv(0), leaf_inv(1), coupling2(0))
        put_w(WL.at[0, :, 0], head)
        put_w(WL.at[0, :, 1], tail)

    @pl.when(core == 0)
    def _():
        z3 = put_z(3, dot(mine(3), leaf_inv(3)))
        put_z(2, dot(mine(2) - dot(z3, coupling2(1)), leaf_inv(2)))

    mark("q_c1")
    net.wait("c1", G.at[pl.ds(0, 3), 0, 0])

    def x_piece(step):
        xx = xs(step)
        return SX.at[xx // 2, pl.ds(2 * (xx % 2), 2)]

    @pl.when(first_half)
    def _():
        def own_rows(k):
            return jnp.concatenate(
                [G[k, g, x // 2, 2 * (x % 2) + kk, a] for kk in range(CORES) for g in (3, 4) for a in range(TALL)], axis=0)

        product = dot(jnp.concatenate([own_rows(k) for k in range(cols)], axis=1), WL[0].reshape(2 * WIDE, LANES))
        x_piece(0)[...] = product.reshape(CORES, 2, TALL, BLK, LANES)
        for d in range(1, chips):
            net.start(x_piece(0), x_piece(0), along("x", d), "share", "share")

    @pl.when(core == 0)
    def _():
        lhs = [jnp.concatenate([ZM[i, HALF:], ZS[i, HALF:]], axis=0) for i in (2, 3)]
        YX[y] = sum(dot(lhs[i], gathered(y, 3 + i)) for i in PAIR)
        for d in range(1, cols):
            net.start(YX.at[y], YX.at[y], along("y", d), "share", "share")

    mark("q_c0")

    @pl.when(first_half)
    def _():
        net.wait("c0pair", C0.at[0, 0])
        net.wait("c0far", C0.at[0, pl.ds(0, 2)])
        TP[...] = dot(jnp.concatenate(c0_pair(0), axis=1), WL[0].reshape(2 * WIDE, LANES))

    mark("r_V")

    @pl.when(first_half)
    def _():
        right = c0_pair(1)
        v3 = dot(halves(right, 1), leaf_inv(3))
        v2 = dot(halves(right, 0) - dot(v3, coupling2(1)), leaf_inv(2))
        VV[:, :WIDE] = v2
        VV[:, WIDE:] = v3
        t_send(1, own_columns(v2, v3))

    mark("o_share")
    net.wait("share", G.at[pl.ds(0, 3), 0, 0])
    mark("p_chain2")

    @pl.when(first_half)
    def _():
        for g in PAIR:
            for c in range(TALL):
                for i in range(BLK):
                    SS[(g * TALL + c) * BLK + i] = SX[i % 2, c, g, i // 2]
        shared = SS[...].reshape(2 * WIDE, LANES)
        t_send(0, TP[...] - dot(VV[...], shared))
        t_near(1)
        w2 = put_w(WL.at[1, :, 0], -dot(leaf_inv(2), shared[:WIDE]))
        put_w(WL.at[1, :, 1], -dot(leaf_inv(3), shared[WIDE:] + dot(coupling2(1), w2)))
        head, tail = two_columns(leaf_inv(2), leaf_inv(3), coupling2(1))
        put_w(WR.at[:, 0], head)
        put_w(WR.at[:, 1], tail)
        net.start(w_rows(WL), w_rows(WL), partner, "w", "w")
        net.start(w_rows(WR), w_rows(WR), partner, "w", "w")
        t_near(0)

    @pl.when(core == 0)
    def _():
        none = jnp.zeros((HALF, LANES), F32)
        tiles = [jnp.concatenate([none, YX[k, :HALF], none, YX[k, HALF:]], axis=0) for k in range(cols)]
        z1 = put_z(1, dot(mine(1) - halves(tiles, 1), leaf_inv(1)))
        put_z(0, dot(mine(0) - halves(tiles, 0) - dot(z1, coupling2(0)), leaf_inv(0)))
        net.wait("w", G.at[0, pl.ds(0, 3), 0, pl.ds(0, 2)])

    mark("s_out")

    @pl.when(first_half)
    def _():
        net.wait("z", ZM)

    o_ref[upper, far] = jnp.zeros((LANES, WIDE), F32)
    for i in range(TALL):
        lines = slice(quarter * i, quarter * (i + 1))
        o_ref[lines, :LANES] = WL[i // 2, spot, i % 2, :, hh].reshape(quarter, LANES)
        o_ref[lines, LANES:WIDE] = WR[spot, i % 2, :, hh].reshape(quarter, LANES) if i >= 2 else jnp.zeros((quarter, LANES), F32)
    o_ref[lower, far] = jnp.concatenate([own_columns(ZM[2 * n], ZM[2 * n + 1]) for n in PAIR], axis=1)

    mark("t_near")

    @pl.when(first_half)
    def _():
        t_far(1)
        t_far(0)

    mark("t_end")

    @pl.when(core == 0)
    def _():
        for side in PAIR:
            net.wait((side, "partner"), TG.at[side])

    def t_rows(i):
        return jnp.concatenate([jnp.concatenate([TG[side, b % 2, c, i, b // 2] for c in range(TALL) for b in range(BLK)], axis=0)
                                for side in PAIR], axis=1)

    mark("u_x21")
    o_ref[lower, near] = -sum(dot(ZM[i], t_rows(i)) for i in range(TALL))

    mark("v_end")
    for name in ("leaf", 0, 1, 2):
        net.wait(name, G.at[0, :, 0], "send")
    net.wait("link", U, "send")
    net.wait("rest", G.at[pl.ds(0, 3), 0, 0], "send")
    net.wait("share", G.at[pl.ds(0, 3), 0, 0], "send")
    net.wait("pair", U.at[0], "send")
    net.wait("c0", C0.at[0, pl.ds(0, 2)], "send")

    @pl.when(first_half)
    def _():
        net.wait("c0far", C0.at[0, pl.ds(0, 2)], "send")
        net.wait("t", G.at[:, pl.ds(0, 3), 0], "send")
        net.wait("tpair", TG, "send")
        net.wait("w", G.at[0, pl.ds(0, 3), 0, pl.ds(0, 2)], "send")

    @pl.when(core == 0)
    def _():
        net.wait("c0pair", C0.at[0, 0], "send")
        net.wait("z", ZM, "send")

    mark()
    counts = [len([key for key in net.names if key[0] == side]) for side in ("send", "recv")]
    assert counts == [send.shape[0], recv.shape[0]], counts


def solution(mesh):
    rows, cols = mesh.shape["row"], mesh.shape["col"]
    block_spec = P(("batch", "row"), "col")

    def device_body(local_l):
        vmem = functools.partial(pltpu.VMEM, dtype=F32)
        return pl.pallas_call(
            functools.partial(kernel, rows, cols),
            out_shape=jax.ShapeDtypeStruct(local_l.shape, F32),
            in_specs=[pl.BlockSpec(memory_space=pl.ANY)],
            out_specs=pl.BlockSpec(memory_space=pltpu.VMEM),
            scratch_shapes=[
                vmem(local_l.shape),
                vmem((2, GROUPS, TALL, BLK, LANES)),
                vmem((cols, GROUPS, 2, TALL, TALL, BLK, LANES)),
                vmem((CORES, cols, LANES, WIDE)),
                vmem((TALL, TALL * BLK, BLK, WIDE)),
                vmem((TALL, 2 * BLK, BLK, WIDE)),
                vmem((TALL, TALL * BLK, BLK, WIDE)),
                vmem((2, cols, 2, TALL, 2, BLK, LANES)),
                vmem((cols, 2, TALL, 2, BLK, LANES)),
                vmem((TALL, LANES, WIDE)),
                vmem((TALL, LANES, WIDE)),
                vmem((2, 2, TALL, TALL, TALL, BLK, LANES)),
                vmem((2, TALL, 2, TALL, BLK, LANES)),
                vmem((cols, LANES, LANES)),
                vmem((WIDE, 2 * WIDE)),
                vmem((2 * TALL * BLK, BLK, LANES)),
                vmem((WIDE, LANES)),
                pltpu.SemaphoreType.DMA((3,)),
                pltpu.SemaphoreType.DMA((15,)),
                pltpu.SemaphoreType.DMA((45,)),
            ],
            compiler_params=pltpu.CompilerParams(collective_id=0, has_side_effects=True),
        )(local_l)

    return jax.shard_map(device_body, mesh=mesh, in_specs=(block_spec,), out_specs=block_spec, check_vma=False)
```

```python
import functools

import jax
import jax.numpy as jnp
from jax import lax
from jax.experimental import pallas as pl
from jax.experimental.pallas import tpu as pltpu
from jax.sharding import PartitionSpec as P

BLK = 8
CORES = 2
LANES = 128
HALF = LANES // 2
WIDE = 2 * LANES
TALL = 4
GROUPS = 5
LEAVES = range(2)
PAIR = range(2)
SIDES = (-1, 1)
MESH = pl.DeviceIdType.MESH


class Marks:
    def __init__(self):
        self.scope = None

    def __call__(self, name=None):
        if self.scope is not None:
            self.scope.__exit__(None, None, None)
        self.scope = None if name is None else jax.named_scope(name)
        if name is not None:
            self.scope.__enter__()
F32 = jnp.float32


def dot(left, right):
    return jnp.dot(left, right, precision=lax.Precision.HIGHEST, preferred_element_type=F32)


def iota(shape, dim):
    return lax.broadcasted_iota(jnp.int32, shape, dim)


def halves(tiles, half):
    low = iota(tiles[0].shape, 1) < HALF
    out = []
    for first, second in ((tiles[0], tiles[1]), (tiles[2], tiles[3])):
        if half == 0:
            out.append(jnp.where(low, first, pltpu.roll(second, HALF, 1)))
        else:
            out.append(jnp.where(low, pltpu.roll(first, HALF, 1), second))
    return jnp.concatenate(out, axis=1)


class Net:
    def __init__(self, send, recv):
        self.send, self.recv, self.names = send, recv, {}

    def slot(self, side, name):
        held = [key for key in self.names if key[0] == side]
        return self.names.setdefault((side, name), len(held))

    def start(self, src, dst, device, send, recv):
        self.make(src, dst, device, send, recv).start()

    def make(self, src, dst, device, send, recv):
        return pltpu.make_async_remote_copy(
            src_ref=src, dst_ref=dst, send_sem=self.send.at[self.slot("send", send)], recv_sem=self.recv.at[self.slot("recv", recv)],
            device_id=device, device_id_type=MESH)

    def wait(self, name, like, side="recv"):
        sems = self.recv if side == "recv" else self.send
        pltpu.make_async_copy(like, like, sems.at[self.slot(side, name)]).wait()


def shift(val, lanes):
    return jnp.concatenate([pltpu.roll(val[:, LANES * i:LANES * (i + 1)], lanes % LANES, 1) for i in range(2)], axis=1)


def kernel(rows, cols, hbm_ref, o_ref, l_ref, U, G, C0, LF, PK, LI, WL, WR, ZM, ZS, TG, SX, YX, VV, SS, TP, load, send, recv):
    chips = rows // CORES
    row = lax.axis_index("row")
    y = lax.axis_index("col")
    x, core = row // CORES, row % CORES
    spot, hh = row % cols, row // cols
    net = Net(send, recv)
    first_half = core == 1

    def at(xx, cc, yy):
        return {"row": xx * CORES + cc, "col": yy}

    def xs(step):
        return lax.rem(x + step + chips, chips)

    def ys(step):
        return lax.rem(y + step + cols, cols)

    def along(axis, step, cc=core):
        return at(xs(step), cc, y) if axis == "x" else at(x, cc, ys(step))

    mark = Marks()
    mark("a_signal")
    upper, lower, near, far = pl.ds(0, LANES), pl.ds(LANES, LANES), pl.ds(0, WIDE), pl.ds(WIDE, WIDE)
    windows = [(upper, near), (lower, far), (lower, near)]
    loads = [pltpu.make_async_copy(hbm_ref.at[w], l_ref.at[w], load.at[i]) for i, w in enumerate(windows)]
    for made in loads:
        made.start()
    partner = at(x, 1 - core, y)
    barrier = pltpu.get_barrier_semaphore()
    peers = [partner] + [along(axis, d, cc) for axis in "xy" for d in range(1, chips) for cc in range(CORES)]
    for peer in peers:
        pl.semaphore_signal(barrier, inc=1, device_id=peer, device_id_type=MESH)

    mark("a_pack")
    quarter = LANES // TALL
    for part in range(2):
        loads[part].wait()
        piece = l_ref[part * LANES:(part + 1) * LANES, part * WIDE:(part + 1) * WIDE]
        low = iota((quarter, LANES), 1) < HALF
        band = [piece[quarter * i:quarter * (i + 1)] for i in range(TALL)]
        packed = [jnp.where(low, band[2 * m][:, LANES * m:LANES * (m + 1)], band[2 * m + 1][:, LANES * m:LANES * (m + 1)])
                  for m in PAIR]
        packed.append(jnp.where(low, band[1][:, :LANES], pltpu.roll(band[3][:, LANES:], HALF, 1)))
        packed += [band[2][:, :LANES], band[3][:, :LANES]]
        tiles = [val.reshape(TALL, BLK, LANES) for val in packed]
        for g in range(GROUPS):
            U[part, g] = tiles[g]

        @pl.when(core == 1 - part)
        def _():
            for g in range(GROUPS):
                G[y, g, hh, spot] = tiles[g]

    loads[2].wait()
    C0[core, y] = l_ref[lower, near]
    mark("b_barrier")
    pl.semaphore_wait(barrier, len(peers))

    axis_first = ["x", "y", "y"]

    def other(axis):
        return "y" if axis == "x" else "x"

    def source(g, f, s, k=None):
        xx, yy = (xs(f), ys(s)) if axis_first[g] == "x" else (xs(s), ys(f))
        return G.at[yy, g, xx // 2, pl.ds(2 * (xx % 2), 2) if k is None else 2 * (xx % 2) + k]

    def pass_on(g, f, s, k, step, name):
        piece = source(g, f, s, k)
        net.start(piece, piece, along(other(axis_first[g]), step), g, name)

    def pass_leaf(g, f):
        for s in SIDES:
            pass_on(g, f, 0, None, -s, (g, "far") if f == 2 else (g, f, s))
        if f == 2:
            pass_on(g, f, 0, None, 2, (g, "far"))

    def half_on(g, f, s):
        pass_on(g, f, s, 0 if s < 0 else 1, -s, (g, "far"))

    mark("d_own")
    for axis in "xy":
        for step in SIDES:
            for part in range(2):
                net.start(U.at[part, pl.ds(0, 2)], G.at[y, pl.ds(0, 2), hh, spot], along(axis, step, 1 - part), "leaf", ("leaf", axis, -step))
    for g in LEAVES:
        for part in range(2):
            net.start(U.at[part, g], G.at[y, g, hh, spot], along(axis_first[g], 2, 1 - part), "leaf", (g, "two"))
    net.start(U.at[core], G.at[y, :, hh, spot], partner, "pair", "pair")
    for s in SIDES:
        net.start(l_ref.at[lower, near], C0.at[core, y], along("y", -s, 1), "c0", ("c0", s))

    @pl.when(core == 0)
    def _():
        net.start(l_ref.at[lower, near], C0.at[core, y], partner, "c0pair", "c0pair")


    def near_by(groups, name, count):
        for step in SIDES:
            for axis in "xy":
                net.wait((name, axis, step), G.at[0, pl.ds(0, count), 0, pl.ds(0, 2)])
                for g in groups:
                    if axis_first[g] == axis:
                        pass_leaf(g, step)
                    else:
                        half_on(g, 0, step)

    def two_away(groups):
        for g in groups:
            net.wait((g, "two"), G.at[0, 0, 0, pl.ds(0, 2)])
            pass_leaf(g, 2)

    def across(groups):
        for f in SIDES:
            for s in SIDES:
                for g in groups:
                    net.wait((g, f, s), source(g, f, s))
                    half_on(g, f, s)

    mark("e_near")
    near_by(LEAVES, "leaf", 2)
    for part in range(2):
        for axis in "xy":
            for step in SIDES:
                net.start(U.at[part, 2], G.at[y, 2, hh, spot], along(axis, step, 1 - part), "link", ("link", axis, -step))
        net.start(U.at[part, 2], G.at[y, 2, hh, spot], along(axis_first[2], 2, 1 - part), "link", (2, "two"))
    mark("g_two")
    two_away(LEAVES)
    mark("h_diag")
    across(LEAVES)
    net.wait("pair", U.at[0])
    mark("i_near2")
    near_by((2,), "link", 1)
    mark("j_second")
    for d in range(1, chips):
        for part, axis in enumerate("yx"):
            net.start(U.at[part, pl.ds(3, 2)], G.at[y, pl.ds(3, 2), hh, spot], along(axis, d, 1 - part), "rest", "c1")

    mark("j_c0")

    @pl.when(first_half)
    def _():
        for s in SIDES:
            net.wait(("c0", s), C0.at[:, 0])
            piece = C0.at[0 if s < 0 else 1, ys(s)]
            net.start(piece, piece, along("y", -s), "c0far", "c0far")

    mark("k_leafin")
    for g in LEAVES:
        net.wait((g, "far"), G.at[pl.ds(0, 3), g, 0])

    two_away((2,))
    mark("l_base")
    lane = iota((BLK, LANES), 1)
    sub = iota((BLK, LANES), 0)
    block_of = (lane // BLK) % BLK
    diag = [[[None] * TALL for _ in range(TALL)] for _ in PAIR]
    inv = [[[None] * TALL for _ in range(TALL)] for _ in PAIR]
    for m in PAIR:
        for c in range(TALL):
            for k in range(c + 1):
                total = jnp.zeros((BLK, LANES), F32)
                for b in range(BLK):
                    total = jnp.where(block_of == b, G[k, m, b % 2, c, b // 2], total)
                diag[m][c][k] = total
                inv[m][c][k] = jnp.where(sub == lane % BLK, 1.0, 0.0) if c == k else jnp.zeros((BLK, LANES), F32)
    for t in range(BLK * TALL):
        ct, jt = t // BLK, t % BLK
        index = (lane // BLK) * BLK + jt
        for m in PAIR:
            spread = [jnp.take_along_axis(diag[m][c][ct], index, axis=1) for c in range(ct, TALL)]
            pivot = 1.0 / spread[0][jt:jt + 1, :]
            below = jnp.where(sub > jt, spread[0], 0.0)
            for k in range(ct + 1):
                solved = inv[m][ct][k][jt:jt + 1, :] * pivot
                inv[m][ct][k] = jnp.where(sub == jt, solved, inv[m][ct][k] - below * solved)
                for c in range(ct + 1, TALL):
                    inv[m][c][k] = inv[m][c][k] - spread[c - ct] * solved
    for m in PAIR:
        for c in range(TALL):
            tiles = [inv[m][c][k] if k <= c else jnp.zeros((BLK, LANES), F32) for k in range(TALL)]
            for e in PAIR:
                PK[2 * m + e, c] = halves(tiles, e)

    def gathered(k, g):
        return jnp.concatenate([G[k, g, b % 2, c, b // 2] for c in range(TALL) for b in range(BLK)], axis=0)

    mark("m_sep")
    for m in PAIR:
        tiles = [gathered(k, m) for k in range(cols)]
        for e in PAIR:
            LF[2 * m + e] = halves(tiles, e).reshape(TALL * BLK, BLK, WIDE)

    def double(m, nb):
        count, lanes = TALL * nb, BLK * nb
        size = BLK * count
        group = ((iota((BLK, WIDE), 1) % HALF) // BLK) // nb
        even = ((iota((size, WIDE), 1) % HALF) // BLK) // nb % 2 == 0

        def coupling(leaf):
            out = []
            for bb in range(nb):
                for c in range(TALL):
                    total = LF[leaf, c * BLK + nb + bb]
                    for s in range(3, BLK // nb, 2):
                        total = jnp.where(group == s - 1, LF[leaf, c * BLK + s * nb + bb], total)
                    out.append(total)
            return jnp.concatenate(out, axis=0)

        def spread(val, flip):
            tiles = val.reshape(count, BLK, WIDE)
            return jnp.concatenate([jnp.where(group == (b // nb) ^ flip, tiles[(b % nb) * TALL + c], 0.0)
                                    for c in range(TALL) for b in range(BLK)], axis=0)

        one, two = (PK[2 * m + e, 0:count].reshape(size, WIDE) for e in PAIR)
        temp = dot(jnp.where(even, coupling(2 * m), shift(coupling(2 * m + 1), lanes)),
                   spread(jnp.where(even, one, shift(two, lanes)), 0))
        corner = dot(jnp.where(even, shift(two, -lanes), one), spread(temp, 1))
        for e, (val, low) in enumerate(((one, corner), (two, shift(corner, -lanes)))):
            parts = (jnp.where(even, val, 0.0), jnp.where(even, -low, val))
            for half in PAIR:
                tiles = parts[half].reshape(count, BLK, WIDE)
                if nb < TALL:
                    PK[2 * m + e, half * count:(half + 1) * count] = tiles
                else:
                    for i in range(count):
                        LI[2 * m + e, (i % TALL) * BLK + half * TALL + i // TALL] = tiles[i]

    mark("n_dbl1")
    for m in PAIR:
        double(m, 1)
    mark("n_two2")
    across((2,))
    mark("n_dbl2")
    for m in PAIR:
        double(m, 2)
    mark("n_dbl4")
    for m in PAIR:
        double(m, 4)
    mark("o_arr2")
    net.wait((2, "far"), G.at[pl.ds(0, 3), 2, 0])

    def leaf_inv(i):
        return LI[i].reshape(WIDE, WIDE)

    def coupling2(m):
        return halves([gathered(k, 2) for k in range(cols)], m)

    def mine(i):
        r, l = iota((WIDE, WIDE), 0), iota((WIDE, WIDE), 1)
        own = CORES * x + r // LANES
        return jnp.where(((r // quarter) % TALL == i) & (l // HALF == own % cols) & (r % BLK == l % BLK)
                         & ((l % HALF) // BLK == 2 * ((r // BLK) % TALL) + own // cols), 1.0, 0.0)

    def put_w(ref, val):
        ref[...] = val.reshape(TALL, TALL, 2, BLK, LANES)
        return val

    def put_z(i, val):
        ZM[i] = val[:LANES]
        ZS[i] = val[LANES:]
        net.start(ZS.at[i], ZM.at[i], partner, "z", "z")
        return val

    def t_piece(side, step, k=None):
        xx = xs(step)
        return TG.at[side, xx // 2, pl.ds(2 * (xx % 2), 2) if k is None else 2 * (xx % 2) + k]

    def t_start(side, step, k, device, name, kind="t"):
        net.start(t_piece(side, step, k), t_piece(side, step, k), device, kind, (side, name))

    def t_send(side, val):
        t_piece(side, 0)[...] = val.reshape(CORES, TALL, TALL, BLK, LANES)
        for i in PAIR:
            for s in SIDES:
                k = i if s < 0 else 1 - i
                t_start(side, 0, k, along("x", -s), (s, i))
        t_start(side, 0, None, partner, "partner", "tpair")

    def t_near(side):
        for i in PAIR:
            for s in SIDES:
                k = i if s < 0 else 1 - i
                net.wait((side, (s, i)), t_piece(side, s, k))
                if i == 0:
                    t_start(side, s, k, along("x", -s), "far")
                t_start(side, s, k, partner, "partner", "tpair")

    def t_far(side):
        net.wait((side, "far"), t_piece(side, 2))
        t_start(side, 2, None, partner, "partner", "tpair")

    def c0_pair(n):
        return [jnp.concatenate([C0[k, c, :, LANES * n:LANES * (n + 1)] for k in range(CORES)], axis=0) for c in range(cols)]

    def own_columns(first, second):
        low = iota((first.shape[0], LANES), 1) < HALF
        out = []
        for val in (first, second):
            tile = jnp.where(y // 2 == 0, val[:, :LANES], val[:, LANES:])
            moved = pltpu.roll(tile, HALF, 1)
            out.append(jnp.where(y % 2 == 0, tile, moved) if val is first else jnp.where(y % 2 == 0, moved, tile))
        return jnp.where(low, out[0], out[1])

    def w_rows(ref):
        own = CORES * x
        return ref.at[..., own % cols, :, :, own // cols, :, :]

    mark("p_chain1")
    low_half = iota((WIDE, LANES), 1) < HALF
    blank = jnp.zeros((WIDE, WIDE), F32)

    def two_columns(one, two, coupling):
        head = own_columns(one, blank)
        return head, jnp.where(low_half, -dot(two, dot(coupling, head)), own_columns(blank, two))

    @pl.when(first_half)
    def _():
        head, tail = two_columns(leaf_inv(0), leaf_inv(1), coupling2(0))
        put_w(WL.at[0, :, 0], head)
        put_w(WL.at[0, :, 1], tail)

    @pl.when(core == 0)
    def _():
        z3 = put_z(3, dot(mine(3), leaf_inv(3)))
        put_z(2, dot(mine(2) - dot(z3, coupling2(1)), leaf_inv(2)))

    mark("q_c1")
    net.wait("c1", G.at[pl.ds(0, 3), 0, 0])

    def x_piece(step):
        xx = xs(step)
        return SX.at[xx // 2, pl.ds(2 * (xx % 2), 2)]

    @pl.when(first_half)
    def _():
        def own_rows(k):
            return jnp.concatenate(
                [G[k, g, x // 2, 2 * (x % 2) + kk, a] for kk in range(CORES) for g in (3, 4) for a in range(TALL)], axis=0)

        product = dot(jnp.concatenate([own_rows(k) for k in range(cols)], axis=1), WL[0].reshape(2 * WIDE, LANES))
        x_piece(0)[...] = product.reshape(CORES, 2, TALL, BLK, LANES)
        for d in range(1, chips):
            net.start(x_piece(0), x_piece(0), along("x", d), "share", "share")

    @pl.when(core == 0)
    def _():
        lhs = [jnp.concatenate([ZM[i, HALF:], ZS[i, HALF:]], axis=0) for i in (2, 3)]
        YX[y] = sum(dot(lhs[i], gathered(y, 3 + i)) for i in PAIR)
        for d in range(1, cols):
            net.start(YX.at[y], YX.at[y], along("y", d), "share", "share")

    mark("q_c0")

    @pl.when(first_half)
    def _():
        net.wait("c0pair", C0.at[0, 0])
        net.wait("c0far", C0.at[0, pl.ds(0, 2)])
        TP[...] = dot(jnp.concatenate(c0_pair(0), axis=1), WL[0].reshape(2 * WIDE, LANES))

    mark("r_V")

    @pl.when(first_half)
    def _():
        right = c0_pair(1)
        v3 = dot(halves(right, 1), leaf_inv(3))
        v2 = dot(halves(right, 0) - dot(v3, coupling2(1)), leaf_inv(2))
        VV[:, :WIDE] = v2
        VV[:, WIDE:] = v3
        t_send(1, own_columns(v2, v3))

    mark("o_share")
    net.wait("share", G.at[pl.ds(0, 3), 0, 0])
    mark("p_chain2")

    @pl.when(first_half)
    def _():
        for g in PAIR:
            for c in range(TALL):
                for i in range(BLK):
                    SS[(g * TALL + c) * BLK + i] = SX[i % 2, c, g, i // 2]
        shared = SS[...].reshape(2 * WIDE, LANES)
        t_send(0, TP[...] - dot(VV[...], shared))
        t_near(1)
        w2 = put_w(WL.at[1, :, 0], -dot(leaf_inv(2), shared[:WIDE]))
        put_w(WL.at[1, :, 1], -dot(leaf_inv(3), shared[WIDE:] + dot(coupling2(1), w2)))
        head, tail = two_columns(leaf_inv(2), leaf_inv(3), coupling2(1))
        put_w(WR.at[:, 0], head)
        put_w(WR.at[:, 1], tail)
        net.start(w_rows(WL), w_rows(WL), partner, "w", "w")
        net.start(w_rows(WR), w_rows(WR), partner, "w", "w")
        t_near(0)

    @pl.when(core == 0)
    def _():
        none = jnp.zeros((HALF, LANES), F32)
        tiles = [jnp.concatenate([none, YX[k, :HALF], none, YX[k, HALF:]], axis=0) for k in range(cols)]
        z1 = put_z(1, dot(mine(1) - halves(tiles, 1), leaf_inv(1)))
        put_z(0, dot(mine(0) - halves(tiles, 0) - dot(z1, coupling2(0)), leaf_inv(0)))
        net.wait("w", G.at[0, pl.ds(0, 3), 0, pl.ds(0, 2)])

    mark("s_out")

    @pl.when(first_half)
    def _():
        net.wait("z", ZM)

    o_ref[upper, far] = jnp.zeros((LANES, WIDE), F32)
    for i in range(TALL):
        lines = slice(quarter * i, quarter * (i + 1))
        o_ref[lines, :LANES] = WL[i // 2, spot, i % 2, :, hh].reshape(quarter, LANES)
        o_ref[lines, LANES:WIDE] = WR[spot, i % 2, :, hh].reshape(quarter, LANES) if i >= 2 else jnp.zeros((quarter, LANES), F32)
    o_ref[lower, far] = jnp.concatenate([own_columns(ZM[2 * n], ZM[2 * n + 1]) for n in PAIR], axis=1)

    mark("t_near")

    @pl.when(first_half)
    def _():
        t_far(1)
        t_far(0)

    mark("t_end")

    @pl.when(core == 0)
    def _():
        for side in PAIR:
            net.wait((side, "partner"), TG.at[side])

    def t_rows(i):
        return jnp.concatenate([jnp.concatenate([TG[side, b % 2, c, i, b // 2] for c in range(TALL) for b in range(BLK)], axis=0)
                                for side in PAIR], axis=1)

    mark("u_x21")
    o_ref[lower, near] = -sum(dot(ZM[i], t_rows(i)) for i in range(TALL))

    mark("v_end")
    for name in ("leaf", 0, 1, 2):
        net.wait(name, G.at[0, :, 0], "send")
    net.wait("link", U, "send")
    net.wait("rest", G.at[pl.ds(0, 3), 0, 0], "send")
    net.wait("share", G.at[pl.ds(0, 3), 0, 0], "send")
    net.wait("pair", U.at[0], "send")
    net.wait("c0", C0.at[0, pl.ds(0, 2)], "send")

    @pl.when(first_half)
    def _():
        net.wait("c0far", C0.at[0, pl.ds(0, 2)], "send")
        net.wait("t", G.at[:, pl.ds(0, 3), 0], "send")
        net.wait("tpair", TG, "send")
        net.wait("w", G.at[0, pl.ds(0, 3), 0, pl.ds(0, 2)], "send")

    @pl.when(core == 0)
    def _():
        net.wait("c0pair", C0.at[0, 0], "send")
        net.wait("z", ZM, "send")

    mark()
    counts = [len([key for key in net.names if key[0] == side]) for side in ("send", "recv")]
    assert counts == [send.shape[0], recv.shape[0]], counts


def solution(mesh):
    rows, cols = mesh.shape["row"], mesh.shape["col"]
    block_spec = P(("batch", "row"), "col")

    def device_body(local_l):
        vmem = functools.partial(pltpu.VMEM, dtype=F32)
        return pl.pallas_call(
            functools.partial(kernel, rows, cols),
            out_shape=jax.ShapeDtypeStruct(local_l.shape, F32),
            in_specs=[pl.BlockSpec(memory_space=pl.ANY)],
            out_specs=pl.BlockSpec(memory_space=pltpu.VMEM),
            scratch_shapes=[
                vmem(local_l.shape),
                vmem((2, GROUPS, TALL, BLK, LANES)),
                vmem((cols, GROUPS, 2, TALL, TALL, BLK, LANES)),
                vmem((CORES, cols, LANES, WIDE)),
                vmem((TALL, TALL * BLK, BLK, WIDE)),
                vmem((TALL, 2 * BLK, BLK, WIDE)),
                vmem((TALL, TALL * BLK, BLK, WIDE)),
                vmem((2, cols, 2, TALL, 2, BLK, LANES)),
                vmem((cols, 2, TALL, 2, BLK, LANES)),
                vmem((TALL, LANES, WIDE)),
                vmem((TALL, LANES, WIDE)),
                vmem((2, 2, TALL, TALL, TALL, BLK, LANES)),
                vmem((2, TALL, 2, TALL, BLK, LANES)),
                vmem((cols, LANES, LANES)),
                vmem((WIDE, 2 * WIDE)),
                vmem((2 * TALL * BLK, BLK, LANES)),
                vmem((WIDE, LANES)),
                pltpu.SemaphoreType.DMA((3,)),
                pltpu.SemaphoreType.DMA((15,)),
                pltpu.SemaphoreType.DMA((45,)),
            ],
            compiler_params=pltpu.CompilerParams(collective_id=0, has_side_effects=True),
        )(local_l)

    return jax.shard_map(device_body, mesh=mesh, in_specs=(block_spec,), out_specs=block_spec, check_vma=False)
```

```python
import functools

import jax
import jax.numpy as jnp
from jax import lax
from jax.experimental import pallas as pl
from jax.experimental.pallas import tpu as pltpu
from jax.sharding import PartitionSpec as P

BLK = 8
CORES = 2
LANES = 128
HALF = LANES // 2
WIDE = 2 * LANES
TALL = 4
GROUPS = 5
LEAVES = range(2)
PAIR = range(2)
SIDES = (-1, 1)
MESH = pl.DeviceIdType.MESH


class Marks:
    def __init__(self):
        self.scope = None

    def __call__(self, name=None):
        if self.scope is not None:
            self.scope.__exit__(None, None, None)
        self.scope = None if name is None else jax.named_scope(name)
        if name is not None:
            self.scope.__enter__()
F32 = jnp.float32


def dot(left, right):
    return jnp.dot(left, right, precision=lax.Precision.HIGHEST, preferred_element_type=F32)


def iota(shape, dim):
    return lax.broadcasted_iota(jnp.int32, shape, dim)


def halves(tiles, half):
    low = iota(tiles[0].shape, 1) < HALF
    out = []
    for first, second in ((tiles[0], tiles[1]), (tiles[2], tiles[3])):
        if half == 0:
            out.append(jnp.where(low, first, pltpu.roll(second, HALF, 1)))
        else:
            out.append(jnp.where(low, pltpu.roll(first, HALF, 1), second))
    return jnp.concatenate(out, axis=1)


class Net:
    def __init__(self, send, recv):
        self.send, self.recv, self.names = send, recv, {}

    def slot(self, side, name):
        held = [key for key in self.names if key[0] == side]
        return self.names.setdefault((side, name), len(held))

    def start(self, src, dst, device, send, recv):
        self.make(src, dst, device, send, recv).start()

    def make(self, src, dst, device, send, recv):
        return pltpu.make_async_remote_copy(
            src_ref=src, dst_ref=dst, send_sem=self.send.at[self.slot("send", send)], recv_sem=self.recv.at[self.slot("recv", recv)],
            device_id=device, device_id_type=MESH)

    def wait(self, name, like, side="recv"):
        sems = self.recv if side == "recv" else self.send
        pltpu.make_async_copy(like, like, sems.at[self.slot(side, name)]).wait()


def shift(val, lanes):
    return jnp.concatenate([pltpu.roll(val[:, LANES * i:LANES * (i + 1)], lanes % LANES, 1) for i in range(2)], axis=1)


def kernel(rows, cols, hbm_ref, o_ref, l_ref, U, G, C0, LF, PK, LI, WL, WR, ZM, ZS, TG, SX, YX, VV, SS, TP, load, send, recv):
    chips = rows // CORES
    row = lax.axis_index("row")
    y = lax.axis_index("col")
    x, core = row // CORES, row % CORES
    spot, hh = row % cols, row // cols
    net = Net(send, recv)
    first_half = core == 1

    def at(xx, cc, yy):
        return {"row": xx * CORES + cc, "col": yy}

    def xs(step):
        return lax.rem(x + step + chips, chips)

    def ys(step):
        return lax.rem(y + step + cols, cols)

    def along(axis, step, cc=core):
        return at(xs(step), cc, y) if axis == "x" else at(x, cc, ys(step))

    mark = Marks()
    mark("a_signal")
    upper, lower, near, far = pl.ds(0, LANES), pl.ds(LANES, LANES), pl.ds(0, WIDE), pl.ds(WIDE, WIDE)
    windows = [(upper, near), (lower, far), (lower, near)]
    loads = [pltpu.make_async_copy(hbm_ref.at[w], l_ref.at[w], load.at[i]) for i, w in enumerate(windows)]
    for made in loads:
        made.start()
    partner = at(x, 1 - core, y)
    barrier = pltpu.get_barrier_semaphore()
    peers = [partner] + [along(axis, d, cc) for axis in "xy" for d in range(1, chips) for cc in range(CORES)]
    for peer in peers:
        pl.semaphore_signal(barrier, inc=1, device_id=peer, device_id_type=MESH)

    mark("a_pack")
    quarter = LANES // TALL
    for part in range(2):
        loads[part].wait()
        piece = l_ref[part * LANES:(part + 1) * LANES, part * WIDE:(part + 1) * WIDE]
        low = iota((quarter, LANES), 1) < HALF
        band = [piece[quarter * i:quarter * (i + 1)] for i in range(TALL)]
        packed = [jnp.where(low, band[2 * m][:, LANES * m:LANES * (m + 1)], band[2 * m + 1][:, LANES * m:LANES * (m + 1)])
                  for m in PAIR]
        packed.append(jnp.where(low, band[1][:, :LANES], pltpu.roll(band[3][:, LANES:], HALF, 1)))
        packed += [band[2][:, :LANES], band[3][:, :LANES]]
        if part:
            packed[:2] = packed[1::-1]
        tiles = [val.reshape(TALL, BLK, LANES) for val in packed]
        for g in range(GROUPS):
            U[part, g] = tiles[g]

        @pl.when(core == 1 - part)
        def _():
            for g in range(GROUPS):
                G[y, g, hh, spot] = tiles[g]

    loads[2].wait()
    C0[core, y] = l_ref[lower, near]
    mark("b_barrier")
    pl.semaphore_wait(barrier, len(peers))

    axis_first = ["x", "y", "y"]

    def other(axis):
        return "y" if axis == "x" else "x"

    def source(g, f, s, k=None):
        xx, yy = (xs(f), ys(s)) if axis_first[g] == "x" else (xs(s), ys(f))
        return G.at[yy, g, xx // 2, pl.ds(2 * (xx % 2), 2) if k is None else 2 * (xx % 2) + k]

    def pass_on(g, f, s, k, step, name):
        piece = source(g, f, s, k)
        net.start(piece, piece, along(other(axis_first[g]), step), g, name)

    def pass_leaf(g, f):
        for s in SIDES:
            pass_on(g, f, 0, None, -s, (g, "far") if f == 2 else (g, f, s))
        if f == 2:
            pass_on(g, f, 0, None, 2, (g, "far"))

    def half_on(g, f, s):
        pass_on(g, f, s, 0 if s < 0 else 1, -s, (g, "far"))

    mark("d_own")
    for axis in "xy":
        for step in SIDES:
            for part in range(2):
                net.start(U.at[part, pl.ds(0, 2)], G.at[y, pl.ds(0, 2), hh, spot], along(axis, step, 1 - part), "leaf", ("leaf", axis, -step))
    for g in LEAVES:
        for part in range(2):
            net.start(U.at[part, g], G.at[y, g, hh, spot], along(axis_first[g], 2, 1 - part), "leaf", (g, "two"))
    net.start(U.at[core], G.at[y, :, hh, spot], partner, "pair", "pair")
    for s in SIDES:
        net.start(l_ref.at[lower, near], C0.at[core, y], along("y", -s, 1), "c0", ("c0", s))

    @pl.when(core == 0)
    def _():
        net.start(l_ref.at[lower, near], C0.at[core, y], partner, "c0pair", "c0pair")


    def near_by(groups, name, count):
        for step in SIDES:
            for axis in "xy":
                net.wait((name, axis, step), G.at[0, pl.ds(0, count), 0, pl.ds(0, 2)])
                for g in groups:
                    if axis_first[g] == axis:
                        pass_leaf(g, step)
                    else:
                        half_on(g, 0, step)

    def two_away(groups):
        for g in groups:
            net.wait((g, "two"), G.at[0, 0, 0, pl.ds(0, 2)])
            pass_leaf(g, 2)

    def across(groups):
        for f in SIDES:
            for s in SIDES:
                for g in groups:
                    net.wait((g, f, s), source(g, f, s))
                    half_on(g, f, s)

    mark("e_near")
    near_by(LEAVES, "leaf", 2)
    for part in range(2):
        for axis in "xy":
            for step in SIDES:
                net.start(U.at[part, 2], G.at[y, 2, hh, spot], along(axis, step, 1 - part), "link", ("link", axis, -step))
        net.start(U.at[part, 2], G.at[y, 2, hh, spot], along(axis_first[2], 2, 1 - part), "link", (2, "two"))
    mark("g_two")
    two_away(LEAVES)
    mark("h_diag")
    across(LEAVES)
    net.wait("pair", U.at[0])
    mark("i_near2")
    near_by((2,), "link", 1)
    mark("j_second")
    for d in range(1, chips):
        for part, axis in enumerate("yx"):
            net.start(U.at[part, pl.ds(3, 2)], G.at[y, pl.ds(3, 2), hh, spot], along(axis, d, 1 - part), "rest", "c1")

    mark("j_c0")

    @pl.when(first_half)
    def _():
        for s in SIDES:
            net.wait(("c0", s), C0.at[:, 0])
            piece = C0.at[0 if s < 0 else 1, ys(s)]
            net.start(piece, piece, along("y", -s), "c0far", "c0far")

    mark("k_leafin")
    for g in LEAVES:
        net.wait((g, "far"), G.at[pl.ds(0, 3), g, 0])

    two_away((2,))
    mark("l_base")
    lane = iota((BLK, LANES), 1)
    sub = iota((BLK, LANES), 0)
    block_of = (lane // BLK) % BLK
    diag = [[[None] * TALL for _ in range(TALL)] for _ in PAIR]
    inv = [[[None] * TALL for _ in range(TALL)] for _ in PAIR]
    for m in PAIR:
        for c in range(TALL):
            for k in range(c + 1):
                total = jnp.zeros((BLK, LANES), F32)
                for b in range(BLK):
                    total = jnp.where(block_of == b, G[k, m, b % 2, c, b // 2], total)
                diag[m][c][k] = total
                inv[m][c][k] = jnp.where(sub == lane % BLK, 1.0, 0.0) if c == k else jnp.zeros((BLK, LANES), F32)
    for t in range(BLK * TALL):
        ct, jt = t // BLK, t % BLK
        index = (lane // BLK) * BLK + jt
        for m in PAIR:
            spread = [jnp.take_along_axis(diag[m][c][ct], index, axis=1) for c in range(ct, TALL)]
            pivot = 1.0 / spread[0][jt:jt + 1, :]
            below = jnp.where(sub > jt, spread[0], 0.0)
            for k in range(ct + 1):
                solved = inv[m][ct][k][jt:jt + 1, :] * pivot
                inv[m][ct][k] = jnp.where(sub == jt, solved, inv[m][ct][k] - below * solved)
                for c in range(ct + 1, TALL):
                    inv[m][c][k] = inv[m][c][k] - spread[c - ct] * solved
    for m in PAIR:
        for c in range(TALL):
            tiles = [inv[m][c][k] if k <= c else jnp.zeros((BLK, LANES), F32) for k in range(TALL)]
            for e in PAIR:
                PK[2 * m + e, c] = halves(tiles, e)

    def gathered(k, g):
        return jnp.concatenate([G[k, g, b % 2, c, b // 2] for c in range(TALL) for b in range(BLK)], axis=0)

    mark("m_sep")
    for m in PAIR:
        tiles = [gathered(k, m) for k in range(cols)]
        for e in PAIR:
            LF[2 * m + e] = halves(tiles, e).reshape(TALL * BLK, BLK, WIDE)

    def double(m, nb):
        count, lanes = TALL * nb, BLK * nb
        size = BLK * count
        group = ((iota((BLK, WIDE), 1) % HALF) // BLK) // nb
        even = ((iota((size, WIDE), 1) % HALF) // BLK) // nb % 2 == 0

        def coupling(leaf):
            out = []
            for bb in range(nb):
                for c in range(TALL):
                    total = LF[leaf, c * BLK + nb + bb]
                    for s in range(3, BLK // nb, 2):
                        total = jnp.where(group == s - 1, LF[leaf, c * BLK + s * nb + bb], total)
                    out.append(total)
            return jnp.concatenate(out, axis=0)

        def spread(val, flip):
            tiles = val.reshape(count, BLK, WIDE)
            return jnp.concatenate([jnp.where(group == (b // nb) ^ flip, tiles[(b % nb) * TALL + c], 0.0)
                                    for c in range(TALL) for b in range(BLK)], axis=0)

        one, two = (PK[2 * m + e, 0:count].reshape(size, WIDE) for e in PAIR)
        temp = dot(jnp.where(even, coupling(2 * m), shift(coupling(2 * m + 1), lanes)),
                   spread(jnp.where(even, one, shift(two, lanes)), 0))
        corner = dot(jnp.where(even, shift(two, -lanes), one), spread(temp, 1))
        for e, (val, low) in enumerate(((one, corner), (two, shift(corner, -lanes)))):
            parts = (jnp.where(even, val, 0.0), jnp.where(even, -low, val))
            for half in PAIR:
                tiles = parts[half].reshape(count, BLK, WIDE)
                if nb < TALL:
                    PK[2 * m + e, half * count:(half + 1) * count] = tiles
                else:
                    for i in range(count):
                        LI[2 * m + e, (i % TALL) * BLK + half * TALL + i // TALL] = tiles[i]

    mark("n_dbl1")
    double(0, 1)
    mark("n_two2")
    across((2,))
    mark("n_dbl2")
    double(0, 2)
    double(0, TALL)
    mark("o_arr2")
    net.wait((2, "far"), G.at[pl.ds(0, 3), 2, 0])

    def leaf_inv(i):
        return LI[i].reshape(WIDE, WIDE)

    def turned(i):
        return leaf_inv((i + 2) % TALL)

    def coupling2(m):
        return halves([gathered(k, 2) for k in range(cols)], m)

    def mine(i):
        r, l = iota((WIDE, WIDE), 0), iota((WIDE, WIDE), 1)
        own = CORES * x + r // LANES
        return jnp.where(((r // quarter) % TALL == i) & (l // HALF == own % cols) & (r % BLK == l % BLK)
                         & ((l % HALF) // BLK == 2 * ((r // BLK) % TALL) + own // cols), 1.0, 0.0)

    def put_w(ref, val):
        ref[...] = val.reshape(TALL, TALL, 2, BLK, LANES)
        return val

    def put_z(i, val):
        ZM[i] = val[:LANES]
        ZS[i] = val[LANES:]
        net.start(ZS.at[i], ZM.at[i], partner, "z", "z")
        return val

    def t_piece(side, step, k=None):
        xx = xs(step)
        return TG.at[side, xx // 2, pl.ds(2 * (xx % 2), 2) if k is None else 2 * (xx % 2) + k]

    def t_start(side, step, k, device, name, kind="t"):
        net.start(t_piece(side, step, k), t_piece(side, step, k), device, kind, (side, name))

    def t_send(side, val):
        t_piece(side, 0)[...] = val.reshape(CORES, TALL, TALL, BLK, LANES)
        for i in PAIR:
            for s in SIDES:
                k = i if s < 0 else 1 - i
                t_start(side, 0, k, along("x", -s), (s, i))
        t_start(side, 0, None, partner, "partner", "tpair")

    def t_near(side):
        for i in PAIR:
            for s in SIDES:
                k = i if s < 0 else 1 - i
                net.wait((side, (s, i)), t_piece(side, s, k))
                if i == 0:
                    t_start(side, s, k, along("x", -s), "far")
                t_start(side, s, k, partner, "partner", "tpair")

    def t_far(side):
        net.wait((side, "far"), t_piece(side, 2))
        t_start(side, 2, None, partner, "partner", "tpair")

    def c0_pair(n):
        return [jnp.concatenate([C0[k, c, :, LANES * n:LANES * (n + 1)] for k in range(CORES)], axis=0) for c in range(cols)]

    def own_columns(first, second):
        low = iota((first.shape[0], LANES), 1) < HALF
        out = []
        for val in (first, second):
            tile = jnp.where(y // 2 == 0, val[:, :LANES], val[:, LANES:])
            moved = pltpu.roll(tile, HALF, 1)
            out.append(jnp.where(y % 2 == 0, tile, moved) if val is first else jnp.where(y % 2 == 0, moved, tile))
        return jnp.where(low, out[0], out[1])

    def w_rows(ref):
        own = CORES * x
        return ref.at[..., own % cols, :, :, own // cols, :, :]

    mark("p_chain1")
    low_half = iota((WIDE, LANES), 1) < HALF
    blank = jnp.zeros((WIDE, WIDE), F32)

    def two_columns(one, two, coupling):
        head = own_columns(one, blank)
        return head, jnp.where(low_half, -dot(two, dot(coupling, head)), own_columns(blank, two))

    @pl.when(first_half)
    def _():
        head, tail = two_columns(leaf_inv(0), leaf_inv(1), coupling2(0))
        put_w(WL.at[0, :, 0], head)
        put_w(WL.at[0, :, 1], tail)

    @pl.when(core == 0)
    def _():
        z3 = put_z(3, dot(mine(3), turned(3)))
        put_z(2, dot(mine(2) - dot(z3, coupling2(1)), turned(2)))

    mark("q_c1")
    net.wait("c1", G.at[pl.ds(0, 3), 0, 0])

    def x_piece(step):
        xx = xs(step)
        return SX.at[xx // 2, pl.ds(2 * (xx % 2), 2)]

    @pl.when(first_half)
    def _():
        def own_rows(k):
            return jnp.concatenate(
                [G[k, g, x // 2, 2 * (x % 2) + kk, a] for kk in range(CORES) for g in (3, 4) for a in range(TALL)], axis=0)

        product = dot(jnp.concatenate([own_rows(k) for k in range(cols)], axis=1), WL[0].reshape(2 * WIDE, LANES))
        x_piece(0)[...] = product.reshape(CORES, 2, TALL, BLK, LANES)
        for d in range(1, chips):
            net.start(x_piece(0), x_piece(0), along("x", d), "share", "share")

    @pl.when(core == 0)
    def _():
        lhs = [jnp.concatenate([ZM[i, HALF:], ZS[i, HALF:]], axis=0) for i in (2, 3)]
        YX[y] = sum(dot(lhs[i], gathered(y, 3 + i)) for i in PAIR)
        for d in range(1, cols):
            net.start(YX.at[y], YX.at[y], along("y", d), "share", "share")

    mark("q_other")
    for nb in (1, 2, TALL):
        double(1, nb)
    mark("q_c0")

    @pl.when(first_half)
    def _():
        net.wait("c0pair", C0.at[0, 0])
        net.wait("c0far", C0.at[0, pl.ds(0, 2)])
        TP[...] = dot(jnp.concatenate(c0_pair(0), axis=1), WL[0].reshape(2 * WIDE, LANES))

    mark("r_V")

    @pl.when(first_half)
    def _():
        right = c0_pair(1)
        v3 = dot(halves(right, 1), leaf_inv(3))
        v2 = dot(halves(right, 0) - dot(v3, coupling2(1)), leaf_inv(2))
        VV[:, :WIDE] = v2
        VV[:, WIDE:] = v3
        t_send(1, own_columns(v2, v3))

    mark("o_share")
    net.wait("share", G.at[pl.ds(0, 3), 0, 0])
    mark("p_chain2")

    @pl.when(first_half)
    def _():
        for g in PAIR:
            for c in range(TALL):
                for i in range(BLK):
                    SS[(g * TALL + c) * BLK + i] = SX[i % 2, c, g, i // 2]
        shared = SS[...].reshape(2 * WIDE, LANES)
        t_send(0, TP[...] - dot(VV[...], shared))
        t_near(1)
        w2 = put_w(WL.at[1, :, 0], -dot(leaf_inv(2), shared[:WIDE]))
        put_w(WL.at[1, :, 1], -dot(leaf_inv(3), shared[WIDE:] + dot(coupling2(1), w2)))
        head, tail = two_columns(leaf_inv(2), leaf_inv(3), coupling2(1))
        put_w(WR.at[:, 0], head)
        put_w(WR.at[:, 1], tail)
        net.start(w_rows(WL), w_rows(WL), partner, "w", "w")
        net.start(w_rows(WR), w_rows(WR), partner, "w", "w")
        t_near(0)

    @pl.when(core == 0)
    def _():
        none = jnp.zeros((HALF, LANES), F32)
        tiles = [jnp.concatenate([none, YX[k, :HALF], none, YX[k, HALF:]], axis=0) for k in range(cols)]
        z1 = put_z(1, dot(mine(1) - halves(tiles, 1), turned(1)))
        put_z(0, dot(mine(0) - halves(tiles, 0) - dot(z1, coupling2(0)), turned(0)))
        net.wait("w", G.at[0, pl.ds(0, 3), 0, pl.ds(0, 2)])

    mark("s_out")

    @pl.when(first_half)
    def _():
        net.wait("z", ZM)

    o_ref[upper, far] = jnp.zeros((LANES, WIDE), F32)
    for i in range(TALL):
        lines = slice(quarter * i, quarter * (i + 1))
        o_ref[lines, :LANES] = WL[i // 2, spot, i % 2, :, hh].reshape(quarter, LANES)
        o_ref[lines, LANES:WIDE] = WR[spot, i % 2, :, hh].reshape(quarter, LANES) if i >= 2 else jnp.zeros((quarter, LANES), F32)
    o_ref[lower, far] = jnp.concatenate([own_columns(ZM[2 * n], ZM[2 * n + 1]) for n in PAIR], axis=1)

    def x21(side):
        total = 0.0
        for i in range(TALL):
            part = jnp.concatenate([TG[side, b % 2, c, i, b // 2] for c in range(TALL) for b in range(BLK)], axis=0)
            total = total - dot(ZM[i], part)
        o_ref[lower, LANES * side:LANES * (side + 1)] = total

    for side in (1, 0):
        mark(f"t_in{side}")

        @pl.when(first_half)
        def _():
            t_far(side)

        @pl.when(core == 0)
        def _():
            net.wait((side, "partner"), TG.at[side])

        mark(f"u_x21{side}")
        x21(side)

    mark("v_end")
    for name in ("leaf", 0, 1, 2):
        net.wait(name, G.at[0, :, 0], "send")
    net.wait("link", U, "send")
    net.wait("rest", G.at[pl.ds(0, 3), 0, 0], "send")
    net.wait("share", G.at[pl.ds(0, 3), 0, 0], "send")
    net.wait("pair", U.at[0], "send")
    net.wait("c0", C0.at[0, pl.ds(0, 2)], "send")

    @pl.when(first_half)
    def _():
        net.wait("c0far", C0.at[0, pl.ds(0, 2)], "send")
        net.wait("t", G.at[:, pl.ds(0, 3), 0], "send")
        net.wait("tpair", TG, "send")
        net.wait("w", G.at[0, pl.ds(0, 3), 0, pl.ds(0, 2)], "send")

    @pl.when(core == 0)
    def _():
        net.wait("c0pair", C0.at[0, 0], "send")
        net.wait("z", ZM, "send")

    mark()
    counts = [len([key for key in net.names if key[0] == side]) for side in ("send", "recv")]
    assert counts == [send.shape[0], recv.shape[0]], counts


def solution(mesh):
    rows, cols = mesh.shape["row"], mesh.shape["col"]
    block_spec = P(("batch", "row"), "col")

    def device_body(local_l):
        vmem = functools.partial(pltpu.VMEM, dtype=F32)
        return pl.pallas_call(
            functools.partial(kernel, rows, cols),
            out_shape=pltpu.VMEM(local_l.shape, F32),
            in_specs=[pl.BlockSpec(memory_space=pl.ANY)],
            out_specs=pl.BlockSpec(memory_space=pltpu.VMEM),
            scratch_shapes=[
                vmem(local_l.shape),
                vmem((2, GROUPS, TALL, BLK, LANES)),
                vmem((cols, GROUPS, 2, TALL, TALL, BLK, LANES)),
                vmem((CORES, cols, LANES, WIDE)),
                vmem((TALL, TALL * BLK, BLK, WIDE)),
                vmem((TALL, 2 * BLK, BLK, WIDE)),
                vmem((TALL, TALL * BLK, BLK, WIDE)),
                vmem((2, cols, 2, TALL, 2, BLK, LANES)),
                vmem((cols, 2, TALL, 2, BLK, LANES)),
                vmem((TALL, LANES, WIDE)),
                vmem((TALL, LANES, WIDE)),
                vmem((2, 2, TALL, TALL, TALL, BLK, LANES)),
                vmem((2, TALL, 2, TALL, BLK, LANES)),
                vmem((cols, LANES, LANES)),
                vmem((WIDE, 2 * WIDE)),
                vmem((2 * TALL * BLK, BLK, LANES)),
                vmem((WIDE, LANES)),
                pltpu.SemaphoreType.DMA((3,)),
                pltpu.SemaphoreType.DMA((15,)),
                pltpu.SemaphoreType.DMA((45,)),
            ],
            compiler_params=pltpu.CompilerParams(collective_id=0, has_side_effects=True),
        )(local_l)

    return jax.shard_map(device_body, mesh=mesh, in_specs=(block_spec,), out_specs=block_spec, check_vma=False)
```

```python
import functools

import jax
import jax.numpy as jnp
from jax import lax
from jax.experimental import pallas as pl
from jax.experimental.pallas import tpu as pltpu
from jax.sharding import PartitionSpec as P

BLK = 8
CORES = 2
LANES = 128
HALF = LANES // 2
WIDE = 2 * LANES
TALL = 4
GROUPS = 5
LEAVES = range(2)
PAIR = range(2)
SIDES = (-1, 1)
MESH = pl.DeviceIdType.MESH


class Marks:
    def __init__(self):
        self.scope = None

    def __call__(self, name=None):
        if self.scope is not None:
            self.scope.__exit__(None, None, None)
        self.scope = None if name is None else jax.named_scope(name)
        if name is not None:
            self.scope.__enter__()
F32 = jnp.float32


def dot(left, right):
    return jnp.dot(left, right, precision=lax.Precision.HIGHEST, preferred_element_type=F32)


def iota(shape, dim):
    return lax.broadcasted_iota(jnp.int32, shape, dim)


def halves(tiles, half):
    low = iota(tiles[0].shape, 1) < HALF
    out = []
    for first, second in ((tiles[0], tiles[1]), (tiles[2], tiles[3])):
        if half == 0:
            out.append(jnp.where(low, first, pltpu.roll(second, HALF, 1)))
        else:
            out.append(jnp.where(low, pltpu.roll(first, HALF, 1), second))
    return jnp.concatenate(out, axis=1)


class Net:
    def __init__(self, send, recv):
        self.send, self.recv, self.names = send, recv, {}

    def slot(self, side, name):
        held = [key for key in self.names if key[0] == side]
        return self.names.setdefault((side, name), len(held))

    def start(self, src, dst, device, send, recv):
        self.make(src, dst, device, send, recv).start()

    def make(self, src, dst, device, send, recv):
        return pltpu.make_async_remote_copy(
            src_ref=src, dst_ref=dst, send_sem=self.send.at[self.slot("send", send)], recv_sem=self.recv.at[self.slot("recv", recv)],
            device_id=device, device_id_type=MESH)

    def wait(self, name, like, side="recv"):
        sems = self.recv if side == "recv" else self.send
        pltpu.make_async_copy(like, like, sems.at[self.slot(side, name)]).wait()


def shift(val, lanes):
    return jnp.concatenate([pltpu.roll(val[:, LANES * i:LANES * (i + 1)], lanes % LANES, 1) for i in range(2)], axis=1)


def kernel(rows, cols, hbm_ref, o_ref, l_ref, U, G, C0, LF, PK, LI, WL, WR, ZM, ZS, TG, SX, YX, VV, SS, TP, load, send, recv):
    chips = rows // CORES
    row = lax.axis_index("row")
    y = lax.axis_index("col")
    x, core = row // CORES, row % CORES
    spot, hh = row % cols, row // cols
    net = Net(send, recv)
    first_half = core == 1

    def at(xx, cc, yy):
        return {"row": xx * CORES + cc, "col": yy}

    def xs(step):
        return lax.rem(x + step + chips, chips)

    def ys(step):
        return lax.rem(y + step + cols, cols)

    def along(axis, step, cc=core):
        return at(xs(step), cc, y) if axis == "x" else at(x, cc, ys(step))

    mark = Marks()
    mark("a_signal")
    upper, lower, near, far = pl.ds(0, LANES), pl.ds(LANES, LANES), pl.ds(0, WIDE), pl.ds(WIDE, WIDE)
    windows = [(upper, near), (lower, far), (lower, near)]
    loads = [pltpu.make_async_copy(hbm_ref.at[w], l_ref.at[w], load.at[i]) for i, w in enumerate(windows)]
    for made in loads:
        made.start()
    partner = at(x, 1 - core, y)
    barrier = pltpu.get_barrier_semaphore()
    peers = [partner] + [along(axis, d, cc) for axis in "xy" for d in range(1, chips) for cc in range(CORES)]
    for peer in peers:
        pl.semaphore_signal(barrier, inc=1, device_id=peer, device_id_type=MESH)

    mark("a_pack")
    quarter = LANES // TALL
    for part in range(2):
        loads[part].wait()
        piece = l_ref[part * LANES:(part + 1) * LANES, part * WIDE:(part + 1) * WIDE]
        low = iota((quarter, LANES), 1) < HALF
        band = [piece[quarter * i:quarter * (i + 1)] for i in range(TALL)]
        packed = [jnp.where(low, band[2 * m][:, LANES * m:LANES * (m + 1)], band[2 * m + 1][:, LANES * m:LANES * (m + 1)])
                  for m in PAIR]
        packed.append(jnp.where(low, band[1][:, :LANES], pltpu.roll(band[3][:, LANES:], HALF, 1)))
        packed += [band[2][:, :LANES], band[3][:, :LANES]]
        tiles = [val.reshape(TALL, BLK, LANES) for val in packed]
        for g in range(GROUPS):
            U[part, g] = tiles[g]

        @pl.when(core == 1 - part)
        def _():
            for g in range(GROUPS):
                G[y, g, hh, spot] = tiles[g]

    loads[2].wait()
    C0[core, y] = l_ref[lower, near]
    mark("b_barrier")
    pl.semaphore_wait(barrier, len(peers))

    axis_first = ["x", "y", "y"]

    def other(axis):
        return "y" if axis == "x" else "x"

    def source(g, f, s, k=None):
        xx, yy = (xs(f), ys(s)) if axis_first[g] == "x" else (xs(s), ys(f))
        return G.at[yy, g, xx // 2, pl.ds(2 * (xx % 2), 2) if k is None else 2 * (xx % 2) + k]

    def pass_on(g, f, s, k, step, name):
        piece = source(g, f, s, k)
        net.start(piece, piece, along(other(axis_first[g]), step), g, name)

    def pass_leaf(g, f):
        for s in SIDES:
            pass_on(g, f, 0, None, -s, (g, "far") if f == 2 else (g, f, s))
        if f == 2:
            pass_on(g, f, 0, None, 2, (g, "far"))

    def half_on(g, f, s):
        pass_on(g, f, s, 0 if s < 0 else 1, -s, (g, "far"))

    mark("d_own")
    for axis in "xy":
        for step in SIDES:
            for part in range(2):
                net.start(U.at[part, pl.ds(0, 2)], G.at[y, pl.ds(0, 2), hh, spot], along(axis, step, 1 - part), "leaf", ("leaf", axis, -step))
    for g in LEAVES:
        for part in range(2):
            net.start(U.at[part, g], G.at[y, g, hh, spot], along(axis_first[g], 2, 1 - part), "leaf", (g, "two"))
    net.start(U.at[core], G.at[y, :, hh, spot], partner, "pair", "pair")

    def near_by(groups, name, count):
        for step in SIDES:
            for axis in "xy":
                net.wait((name, axis, step), G.at[0, pl.ds(0, count), 0, pl.ds(0, 2)])
                for g in groups:
                    if axis_first[g] == axis:
                        pass_leaf(g, step)
                    else:
                        half_on(g, 0, step)

    def two_away(groups):
        for g in groups:
            net.wait((g, "two"), G.at[0, 0, 0, pl.ds(0, 2)])
            pass_leaf(g, 2)

    def across(groups):
        for f in SIDES:
            for s in SIDES:
                for g in groups:
                    net.wait((g, f, s), source(g, f, s))
                    half_on(g, f, s)

    mark("e_near")
    near_by(LEAVES, "leaf", 2)
    for part in range(2):
        for axis in "xy":
            for step in SIDES:
                net.start(U.at[part, 2], G.at[y, 2, hh, spot], along(axis, step, 1 - part), "link", ("link", axis, -step))
        net.start(U.at[part, 2], G.at[y, 2, hh, spot], along(axis_first[2], 2, 1 - part), "link", (2, "two"))
    for s in SIDES:
        net.start(l_ref.at[lower, near], C0.at[core, y], along("y", -s, 1), "c0", ("c0", s))

    @pl.when(core == 0)
    def _():
        net.start(l_ref.at[lower, near], C0.at[core, y], partner, "c0pair", "c0pair")

    mark("g_two")
    two_away(LEAVES)
    mark("h_diag")
    across(LEAVES)
    net.wait("pair", U.at[0])
    mark("i_near2")
    near_by((2,), "link", 1)
    mark("j_second")
    for d in range(1, chips):
        for part, axis in enumerate("yx"):
            net.start(U.at[part, pl.ds(3, 2)], G.at[y, pl.ds(3, 2), hh, spot], along(axis, d, 1 - part), "rest", "c1")

    mark("j_c0")

    @pl.when(first_half)
    def _():
        for s in SIDES:
            net.wait(("c0", s), C0.at[:, 0])
            piece = C0.at[0 if s < 0 else 1, ys(s)]
            net.start(piece, piece, along("y", -s), "c0far", "c0far")

    mark("k_leafin")
    for g in LEAVES:
        net.wait((g, "far"), G.at[pl.ds(0, 3), g, 0])

    two_away((2,))
    mark("l_base")
    lane = iota((BLK, LANES), 1)
    sub = iota((BLK, LANES), 0)
    block_of = (lane // BLK) % BLK
    diag = [[[None] * TALL for _ in range(TALL)] for _ in PAIR]
    inv = [[[None] * TALL for _ in range(TALL)] for _ in PAIR]
    for m in PAIR:
        for c in range(TALL):
            for k in range(c + 1):
                total = jnp.zeros((BLK, LANES), F32)
                for b in range(BLK):
                    total = jnp.where(block_of == b, G[k, m, b % 2, c, b // 2], total)
                diag[m][c][k] = total
                inv[m][c][k] = jnp.where(sub == lane % BLK, 1.0, 0.0) if c == k else jnp.zeros((BLK, LANES), F32)
    for t in range(BLK * TALL):
        ct, jt = t // BLK, t % BLK
        index = (lane // BLK) * BLK + jt
        for m in PAIR:
            spread = [jnp.take_along_axis(diag[m][c][ct], index, axis=1) for c in range(ct, TALL)]
            pivot = 1.0 / spread[0][jt:jt + 1, :]
            below = jnp.where(sub > jt, spread[0], 0.0)
            for k in range(ct + 1):
                solved = inv[m][ct][k][jt:jt + 1, :] * pivot
                inv[m][ct][k] = jnp.where(sub == jt, solved, inv[m][ct][k] - below * solved)
                for c in range(ct + 1, TALL):
                    inv[m][c][k] = inv[m][c][k] - spread[c - ct] * solved
    for m in PAIR:
        for c in range(TALL):
            tiles = [inv[m][c][k] if k <= c else jnp.zeros((BLK, LANES), F32) for k in range(TALL)]
            for e in PAIR:
                PK[2 * m + e, c] = halves(tiles, e)

    def gathered(k, g):
        return jnp.concatenate([G[k, g, b % 2, c, b // 2] for c in range(TALL) for b in range(BLK)], axis=0)

    mark("m_sep")
    for m in PAIR:
        tiles = [gathered(k, m) for k in range(cols)]
        for e in PAIR:
            LF[2 * m + e] = halves(tiles, e).reshape(TALL * BLK, BLK, WIDE)

    def double(m, nb):
        count, lanes = TALL * nb, BLK * nb
        size = BLK * count
        group = ((iota((BLK, WIDE), 1) % HALF) // BLK) // nb
        even = ((iota((size, WIDE), 1) % HALF) // BLK) // nb % 2 == 0

        def coupling(leaf):
            out = []
            for bb in range(nb):
                for c in range(TALL):
                    total = LF[leaf, c * BLK + nb + bb]
                    for s in range(3, BLK // nb, 2):
                        total = jnp.where(group == s - 1, LF[leaf, c * BLK + s * nb + bb], total)
                    out.append(total)
            return jnp.concatenate(out, axis=0)

        def spread(val, flip):
            tiles = val.reshape(count, BLK, WIDE)
            return jnp.concatenate([jnp.where(group == (b // nb) ^ flip, tiles[(b % nb) * TALL + c], 0.0)
                                    for c in range(TALL) for b in range(BLK)], axis=0)

        one, two = (PK[2 * m + e, 0:count].reshape(size, WIDE) for e in PAIR)
        temp = dot(jnp.where(even, coupling(2 * m), shift(coupling(2 * m + 1), lanes)),
                   spread(jnp.where(even, one, shift(two, lanes)), 0))
        corner = dot(jnp.where(even, shift(two, -lanes), one), spread(temp, 1))
        for e, (val, low) in enumerate(((one, corner), (two, shift(corner, -lanes)))):
            parts = (jnp.where(even, val, 0.0), jnp.where(even, -low, val))
            for half in PAIR:
                tiles = parts[half].reshape(count, BLK, WIDE)
                if nb < TALL:
                    PK[2 * m + e, half * count:(half + 1) * count] = tiles
                else:
                    for i in range(count):
                        LI[2 * m + e, (i % TALL) * BLK + half * TALL + i // TALL] = tiles[i]

    mark("n_dbl1")
    for m in PAIR:
        double(m, 1)
    mark("n_two2")
    across((2,))
    mark("n_dbl2")
    for m in PAIR:
        double(m, 2)
    mark("n_dbl4")
    for m in PAIR:
        double(m, 4)
    mark("o_arr2")
    net.wait((2, "far"), G.at[pl.ds(0, 3), 2, 0])

    def leaf_inv(i):
        return LI[i].reshape(WIDE, WIDE)

    def coupling2(m):
        return halves([gathered(k, 2) for k in range(cols)], m)

    def mine(i):
        r, l = iota((WIDE, WIDE), 0), iota((WIDE, WIDE), 1)
        own = CORES * x + r // LANES
        return jnp.where(((r // quarter) % TALL == i) & (l // HALF == own % cols) & (r % BLK == l % BLK)
                         & ((l % HALF) // BLK == 2 * ((r // BLK) % TALL) + own // cols), 1.0, 0.0)

    def put_w(ref, val):
        ref[...] = val.reshape(TALL, TALL, 2, BLK, LANES)
        return val

    def put_z(i, val):
        ZM[i] = val[:LANES]
        ZS[i] = val[LANES:]
        net.start(ZS.at[i], ZM.at[i], partner, "z", "z")
        return val

    def t_piece(side, step, k=None):
        xx = xs(step)
        return TG.at[side, xx // 2, pl.ds(2 * (xx % 2), 2) if k is None else 2 * (xx % 2) + k]

    def t_start(side, step, k, device, name, kind="t"):
        net.start(t_piece(side, step, k), t_piece(side, step, k), device, kind, (side, name))

    def t_send(side, val):
        t_piece(side, 0)[...] = val.reshape(CORES, TALL, TALL, BLK, LANES)
        for i in PAIR:
            for s in SIDES:
                k = i if s < 0 else 1 - i
                t_start(side, 0, k, along("x", -s), (s, i))
        t_start(side, 0, None, partner, "partner", "tpair")

    def t_near(side):
        for i in PAIR:
            for s in SIDES:
                k = i if s < 0 else 1 - i
                net.wait((side, (s, i)), t_piece(side, s, k))
                if i == 0:
                    t_start(side, s, k, along("x", -s), "far")
                t_start(side, s, k, partner, "partner", "tpair")

    def t_far(side):
        net.wait((side, "far"), t_piece(side, 2))
        t_start(side, 2, None, partner, "partner", "tpair")

    def c0_pair(n):
        return [jnp.concatenate([C0[k, c, :, LANES * n:LANES * (n + 1)] for k in range(CORES)], axis=0) for c in range(cols)]

    def own_columns(first, second):
        low = iota((first.shape[0], LANES), 1) < HALF
        out = []
        for val in (first, second):
            tile = jnp.where(y // 2 == 0, val[:, :LANES], val[:, LANES:])
            moved = pltpu.roll(tile, HALF, 1)
            out.append(jnp.where(y % 2 == 0, tile, moved) if val is first else jnp.where(y % 2 == 0, moved, tile))
        return jnp.where(low, out[0], out[1])

    def w_rows(ref):
        own = CORES * x
        return ref.at[..., own % cols, :, :, own // cols, :, :]

    mark("p_chain1")
    low_half = iota((WIDE, LANES), 1) < HALF
    blank = jnp.zeros((WIDE, WIDE), F32)

    def two_columns(one, two, coupling):
        head = own_columns(one, blank)
        return head, jnp.where(low_half, -dot(two, dot(coupling, head)), own_columns(blank, two))

    @pl.when(first_half)
    def _():
        head, tail = two_columns(leaf_inv(0), leaf_inv(1), coupling2(0))
        put_w(WL.at[0, :, 0], head)
        put_w(WL.at[0, :, 1], tail)

    @pl.when(core == 0)
    def _():
        z3 = put_z(3, dot(mine(3), leaf_inv(3)))
        put_z(2, dot(mine(2) - dot(z3, coupling2(1)), leaf_inv(2)))

    mark("q_c1")
    net.wait("c1", G.at[pl.ds(0, 3), 0, 0])

    def x_piece(step):
        xx = xs(step)
        return SX.at[xx // 2, pl.ds(2 * (xx % 2), 2)]

    @pl.when(first_half)
    def _():
        def own_rows(k):
            return jnp.concatenate(
                [G[k, g, x // 2, 2 * (x % 2) + kk, a] for kk in range(CORES) for g in (3, 4) for a in range(TALL)], axis=0)

        product = dot(jnp.concatenate([own_rows(k) for k in range(cols)], axis=1), WL[0].reshape(2 * WIDE, LANES))
        x_piece(0)[...] = product.reshape(CORES, 2, TALL, BLK, LANES)
        for d in range(1, chips):
            net.start(x_piece(0), x_piece(0), along("x", d), "share", "share")

    @pl.when(core == 0)
    def _():
        lhs = [jnp.concatenate([ZM[i, HALF:], ZS[i, HALF:]], axis=0) for i in (2, 3)]
        YX[y] = sum(dot(lhs[i], gathered(y, 3 + i)) for i in PAIR)
        for d in range(1, cols):
            net.start(YX.at[y], YX.at[y], along("y", d), "share", "share")

    mark("q_c0")

    @pl.when(first_half)
    def _():
        net.wait("c0pair", C0.at[0, 0])
        net.wait("c0far", C0.at[0, pl.ds(0, 2)])
        TP[...] = dot(jnp.concatenate(c0_pair(0), axis=1), WL[0].reshape(2 * WIDE, LANES))

    mark("r_V")

    @pl.when(first_half)
    def _():
        right = c0_pair(1)
        v3 = dot(halves(right, 1), leaf_inv(3))
        v2 = dot(halves(right, 0) - dot(v3, coupling2(1)), leaf_inv(2))
        VV[:, :WIDE] = v2
        VV[:, WIDE:] = v3
        t_send(1, own_columns(v2, v3))

    mark("o_share")
    net.wait("share", G.at[pl.ds(0, 3), 0, 0])
    mark("p_chain2")

    @pl.when(first_half)
    def _():
        for g in PAIR:
            for c in range(TALL):
                for i in range(BLK):
                    SS[(g * TALL + c) * BLK + i] = SX[i % 2, c, g, i // 2]
        shared = SS[...].reshape(2 * WIDE, LANES)
        t_send(0, TP[...] - dot(VV[...], shared))
        t_near(1)
        w2 = put_w(WL.at[1, :, 0], -dot(leaf_inv(2), shared[:WIDE]))
        put_w(WL.at[1, :, 1], -dot(leaf_inv(3), shared[WIDE:] + dot(coupling2(1), w2)))
        head, tail = two_columns(leaf_inv(2), leaf_inv(3), coupling2(1))
        put_w(WR.at[:, 0], head)
        put_w(WR.at[:, 1], tail)
        net.start(w_rows(WL), w_rows(WL), partner, "w", "w")
        net.start(w_rows(WR), w_rows(WR), partner, "w", "w")
        t_near(0)

    @pl.when(core == 0)
    def _():
        none = jnp.zeros((HALF, LANES), F32)
        tiles = [jnp.concatenate([none, YX[k, :HALF], none, YX[k, HALF:]], axis=0) for k in range(cols)]
        z1 = put_z(1, dot(mine(1) - halves(tiles, 1), leaf_inv(1)))
        put_z(0, dot(mine(0) - halves(tiles, 0) - dot(z1, coupling2(0)), leaf_inv(0)))
        net.wait("w", G.at[0, pl.ds(0, 3), 0, pl.ds(0, 2)])

    mark("s_out")

    @pl.when(first_half)
    def _():
        net.wait("z", ZM)

    o_ref[upper, far] = jnp.zeros((LANES, WIDE), F32)
    for i in range(TALL):
        lines = slice(quarter * i, quarter * (i + 1))
        o_ref[lines, :LANES] = WL[i // 2, spot, i % 2, :, hh].reshape(quarter, LANES)
        o_ref[lines, LANES:WIDE] = WR[spot, i % 2, :, hh].reshape(quarter, LANES) if i >= 2 else jnp.zeros((quarter, LANES), F32)
    o_ref[lower, far] = jnp.concatenate([own_columns(ZM[2 * n], ZM[2 * n + 1]) for n in PAIR], axis=1)

    def x21(side):
        total = 0.0
        for i in range(TALL):
            part = jnp.concatenate([TG[side, b % 2, c, i, b // 2] for c in range(TALL) for b in range(BLK)], axis=0)
            total = total - dot(ZM[i], part)
        o_ref[lower, LANES * side:LANES * (side + 1)] = total

    for side in (1, 0):
        mark(f"t_in{side}")

        @pl.when(first_half)
        def _():
            t_far(side)

        @pl.when(core == 0)
        def _():
            net.wait((side, "partner"), TG.at[side])

        mark(f"u_x21{side}")
        x21(side)

    mark("v_end")
    for name in ("leaf", 0, 1, 2):
        net.wait(name, G.at[0, :, 0], "send")
    net.wait("link", U, "send")
    net.wait("rest", G.at[pl.ds(0, 3), 0, 0], "send")
    net.wait("share", G.at[pl.ds(0, 3), 0, 0], "send")
    net.wait("pair", U.at[0], "send")
    net.wait("c0", C0.at[0, pl.ds(0, 2)], "send")

    @pl.when(first_half)
    def _():
        net.wait("c0far", C0.at[0, pl.ds(0, 2)], "send")
        net.wait("t", G.at[:, pl.ds(0, 3), 0], "send")
        net.wait("tpair", TG, "send")
        net.wait("w", G.at[0, pl.ds(0, 3), 0, pl.ds(0, 2)], "send")

    @pl.when(core == 0)
    def _():
        net.wait("c0pair", C0.at[0, 0], "send")
        net.wait("z", ZM, "send")

    mark()
    counts = [len([key for key in net.names if key[0] == side]) for side in ("send", "recv")]
    assert counts == [send.shape[0], recv.shape[0]], counts


def solution(mesh):
    rows, cols = mesh.shape["row"], mesh.shape["col"]
    block_spec = P(("batch", "row"), "col")

    def device_body(local_l):
        vmem = functools.partial(pltpu.VMEM, dtype=F32)
        return pl.pallas_call(
            functools.partial(kernel, rows, cols),
            out_shape=pltpu.VMEM(local_l.shape, F32),
            in_specs=[pl.BlockSpec(memory_space=pl.ANY)],
            out_specs=pl.BlockSpec(memory_space=pltpu.VMEM),
            scratch_shapes=[
                vmem(local_l.shape),
                vmem((2, GROUPS, TALL, BLK, LANES)),
                vmem((cols, GROUPS, 2, TALL, TALL, BLK, LANES)),
                vmem((CORES, cols, LANES, WIDE)),
                vmem((TALL, TALL * BLK, BLK, WIDE)),
                vmem((TALL, 2 * BLK, BLK, WIDE)),
                vmem((TALL, TALL * BLK, BLK, WIDE)),
                vmem((2, cols, 2, TALL, 2, BLK, LANES)),
                vmem((cols, 2, TALL, 2, BLK, LANES)),
                vmem((TALL, LANES, WIDE)),
                vmem((TALL, LANES, WIDE)),
                vmem((2, 2, TALL, TALL, TALL, BLK, LANES)),
                vmem((2, TALL, 2, TALL, BLK, LANES)),
                vmem((cols, LANES, LANES)),
                vmem((WIDE, 2 * WIDE)),
                vmem((2 * TALL * BLK, BLK, LANES)),
                vmem((WIDE, LANES)),
                pltpu.SemaphoreType.DMA((3,)),
                pltpu.SemaphoreType.DMA((15,)),
                pltpu.SemaphoreType.DMA((45,)),
            ],
            compiler_params=pltpu.CompilerParams(collective_id=0, has_side_effects=True),
        )(local_l)

    return jax.shard_map(device_body, mesh=mesh, in_specs=(block_spec,), out_specs=block_spec, check_vma=False)
```

```python
import functools

import jax
import jax.numpy as jnp
from jax import lax
from jax.experimental import pallas as pl
from jax.experimental.pallas import tpu as pltpu
from jax.sharding import PartitionSpec as P

BLK = 8
CORES = 2
LANES = 128
HALF = LANES // 2
WIDE = 2 * LANES
TALL = 4
GROUPS = 5
LEAVES = range(2)
PAIR = range(2)
SIDES = (-1, 1)
MESH = pl.DeviceIdType.MESH


class Marks:
    def __init__(self):
        self.scope = None

    def __call__(self, name=None):
        if self.scope is not None:
            self.scope.__exit__(None, None, None)
        self.scope = None if name is None else jax.named_scope(name)
        if name is not None:
            self.scope.__enter__()
F32 = jnp.float32


def dot(left, right):
    return jnp.dot(left, right, precision=lax.Precision.HIGHEST, preferred_element_type=F32)


def iota(shape, dim):
    return lax.broadcasted_iota(jnp.int32, shape, dim)


def halves(tiles, half):
    low = iota(tiles[0].shape, 1) < HALF
    out = []
    for first, second in ((tiles[0], tiles[1]), (tiles[2], tiles[3])):
        if half == 0:
            out.append(jnp.where(low, first, pltpu.roll(second, HALF, 1)))
        else:
            out.append(jnp.where(low, pltpu.roll(first, HALF, 1), second))
    return jnp.concatenate(out, axis=1)


class Net:
    def __init__(self, send, recv):
        self.send, self.recv, self.names = send, recv, {}

    def slot(self, side, name):
        held = [key for key in self.names if key[0] == side]
        return self.names.setdefault((side, name), len(held))

    def start(self, src, dst, device, send, recv):
        self.make(src, dst, device, send, recv).start()

    def make(self, src, dst, device, send, recv):
        return pltpu.make_async_remote_copy(
            src_ref=src, dst_ref=dst, send_sem=self.send.at[self.slot("send", send)], recv_sem=self.recv.at[self.slot("recv", recv)],
            device_id=device, device_id_type=MESH)

    def wait(self, name, like, side="recv"):
        sems = self.recv if side == "recv" else self.send
        pltpu.make_async_copy(like, like, sems.at[self.slot(side, name)]).wait()


def shift(val, lanes):
    return jnp.concatenate([pltpu.roll(val[:, LANES * i:LANES * (i + 1)], lanes % LANES, 1) for i in range(2)], axis=1)


def kernel(rows, cols, hbm_ref, o_ref, l_ref, U, G, C0, LF, PK, LI, WL, WR, ZM, ZS, TG, SX, YX, VV, SS, TP, load, send, recv):
    chips = rows // CORES
    row = lax.axis_index("row")
    y = lax.axis_index("col")
    x, core = row // CORES, row % CORES
    spot, hh = row % cols, row // cols
    net = Net(send, recv)
    first_half = core == 1

    def at(xx, cc, yy):
        return {"row": xx * CORES + cc, "col": yy}

    def xs(step):
        return lax.rem(x + step + chips, chips)

    def ys(step):
        return lax.rem(y + step + cols, cols)

    def along(axis, step, cc=core):
        return at(xs(step), cc, y) if axis == "x" else at(x, cc, ys(step))

    mark = Marks()
    mark("a_signal")
    upper, lower, near, far = pl.ds(0, LANES), pl.ds(LANES, LANES), pl.ds(0, WIDE), pl.ds(WIDE, WIDE)
    windows = [(upper, near), (lower, far), (lower, near)]
    loads = [pltpu.make_async_copy(hbm_ref.at[w], l_ref.at[w], load.at[i]) for i, w in enumerate(windows)]
    for made in loads:
        made.start()
    partner = at(x, 1 - core, y)
    barrier = pltpu.get_barrier_semaphore()
    peers = [partner] + [along(axis, d, cc) for axis in "xy" for d in range(1, chips) for cc in range(CORES)]
    for peer in peers:
        pl.semaphore_signal(barrier, inc=1, device_id=peer, device_id_type=MESH)

    mark("a_pack")
    quarter = LANES // TALL
    for part in range(2):
        loads[part].wait()
        piece = l_ref[part * LANES:(part + 1) * LANES, part * WIDE:(part + 1) * WIDE]
        low = iota((quarter, LANES), 1) < HALF
        band = [piece[quarter * i:quarter * (i + 1)] for i in range(TALL)]
        packed = [jnp.where(low, band[2 * m][:, LANES * m:LANES * (m + 1)], band[2 * m + 1][:, LANES * m:LANES * (m + 1)])
                  for m in PAIR]
        packed.append(jnp.where(low, band[1][:, :LANES], pltpu.roll(band[3][:, LANES:], HALF, 1)))
        packed += [band[2][:, :LANES], band[3][:, :LANES]]
        tiles = [val.reshape(TALL, BLK, LANES) for val in packed]
        for g in range(GROUPS):
            U[part, g] = tiles[g]

        @pl.when(core == 1 - part)
        def _():
            for g in range(GROUPS):
                G[y, g, hh, spot] = tiles[g]

    loads[2].wait()
    C0[core, y] = l_ref[lower, near]
    mark("b_barrier")
    pl.semaphore_wait(barrier, len(peers))

    axis_first = ["x", "y", "y"]

    def other(axis):
        return "y" if axis == "x" else "x"

    def source(g, f, s, k=None):
        xx, yy = (xs(f), ys(s)) if axis_first[g] == "x" else (xs(s), ys(f))
        return G.at[yy, g, xx // 2, pl.ds(2 * (xx % 2), 2) if k is None else 2 * (xx % 2) + k]

    def pass_on(g, f, s, k, step, name):
        piece = source(g, f, s, k)
        net.start(piece, piece, along(other(axis_first[g]), step), g, name)

    def pass_leaf(g, f):
        for s in SIDES:
            pass_on(g, f, 0, None, -s, (g, "far") if f == 2 else (g, f, s))
        if f == 2:
            pass_on(g, f, 0, None, 2, (g, "far"))

    def half_on(g, f, s):
        pass_on(g, f, s, 0 if s < 0 else 1, -s, (g, "far"))

    mark("d_own")
    for axis in "xy":
        for step in SIDES:
            for part in range(2):
                net.start(U.at[part, pl.ds(0, 2)], G.at[y, pl.ds(0, 2), hh, spot], along(axis, step, 1 - part), "leaf", ("leaf", axis, -step))
    for g in LEAVES:
        for part in range(2):
            net.start(U.at[part, g], G.at[y, g, hh, spot], along(axis_first[g], 2, 1 - part), "leaf", (g, "two"))
    net.start(U.at[core], G.at[y, :, hh, spot], partner, "pair", "pair")

    def near_by(groups, name, count):
        for step in SIDES:
            for axis in "xy":
                net.wait((name, axis, step), G.at[0, pl.ds(0, count), 0, pl.ds(0, 2)])
                for g in groups:
                    if axis_first[g] == axis:
                        pass_leaf(g, step)
                    else:
                        half_on(g, 0, step)

    def two_away(groups):
        for g in groups:
            net.wait((g, "two"), G.at[0, 0, 0, pl.ds(0, 2)])
            pass_leaf(g, 2)

    def across(groups):
        for f in SIDES:
            for s in SIDES:
                for g in groups:
                    net.wait((g, f, s), source(g, f, s))
                    half_on(g, f, s)

    mark("e_near")
    near_by(LEAVES, "leaf", 2)
    for part in range(2):
        for axis in "xy":
            for step in SIDES:
                net.start(U.at[part, 2], G.at[y, 2, hh, spot], along(axis, step, 1 - part), "link", ("link", axis, -step))
        net.start(U.at[part, 2], G.at[y, 2, hh, spot], along(axis_first[2], 2, 1 - part), "link", (2, "two"))
    for s in SIDES:
        net.start(l_ref.at[lower, near], C0.at[core, y], along("y", -s, 1), "c0", ("c0", s))

    @pl.when(core == 0)
    def _():
        net.start(l_ref.at[lower, near], C0.at[core, y], partner, "c0pair", "c0pair")

    mark("g_two")
    two_away(LEAVES)
    mark("h_diag")
    across(LEAVES)
    net.wait("pair", U.at[0])
    mark("i_near2")
    near_by((2,), "link", 1)
    mark("j_second")
    for d in range(1, chips):
        for part, axis in enumerate("yx"):
            net.start(U.at[part, pl.ds(3, 2)], G.at[y, pl.ds(3, 2), hh, spot], along(axis, d, 1 - part), "rest", "c1")

    mark("k_leafin")
    for g in LEAVES:
        net.wait((g, "far"), G.at[pl.ds(0, 3), g, 0])

    two_away((2,))
    mark("l_base")
    lane = iota((BLK, LANES), 1)
    sub = iota((BLK, LANES), 0)
    block_of = (lane // BLK) % BLK
    diag = [[[None] * TALL for _ in range(TALL)] for _ in PAIR]
    inv = [[[None] * TALL for _ in range(TALL)] for _ in PAIR]
    for m in PAIR:
        for c in range(TALL):
            for k in range(c + 1):
                total = jnp.zeros((BLK, LANES), F32)
                for b in range(BLK):
                    total = jnp.where(block_of == b, G[k, m, b % 2, c, b // 2], total)
                diag[m][c][k] = total
                inv[m][c][k] = jnp.where(sub == lane % BLK, 1.0, 0.0) if c == k else jnp.zeros((BLK, LANES), F32)
    for t in range(BLK * TALL):
        ct, jt = t // BLK, t % BLK
        index = (lane // BLK) * BLK + jt
        for m in PAIR:
            spread = [jnp.take_along_axis(diag[m][c][ct], index, axis=1) for c in range(ct, TALL)]
            pivot = 1.0 / spread[0][jt:jt + 1, :]
            below = jnp.where(sub > jt, spread[0], 0.0)
            for k in range(ct + 1):
                solved = inv[m][ct][k][jt:jt + 1, :] * pivot
                inv[m][ct][k] = jnp.where(sub == jt, solved, inv[m][ct][k] - below * solved)
                for c in range(ct + 1, TALL):
                    inv[m][c][k] = inv[m][c][k] - spread[c - ct] * solved
    for m in PAIR:
        for c in range(TALL):
            tiles = [inv[m][c][k] if k <= c else jnp.zeros((BLK, LANES), F32) for k in range(TALL)]
            for e in PAIR:
                PK[2 * m + e, c] = halves(tiles, e)

    def gathered(k, g):
        return jnp.concatenate([G[k, g, b % 2, c, b // 2] for c in range(TALL) for b in range(BLK)], axis=0)

    mark("m_sep")
    for m in PAIR:
        tiles = [gathered(k, m) for k in range(cols)]
        for e in PAIR:
            LF[2 * m + e] = halves(tiles, e).reshape(TALL * BLK, BLK, WIDE)

    def double(m, nb):
        count, lanes = TALL * nb, BLK * nb
        size = BLK * count
        group = ((iota((BLK, WIDE), 1) % HALF) // BLK) // nb
        even = ((iota((size, WIDE), 1) % HALF) // BLK) // nb % 2 == 0

        def coupling(leaf):
            out = []
            for bb in range(nb):
                for c in range(TALL):
                    total = LF[leaf, c * BLK + nb + bb]
                    for s in range(3, BLK // nb, 2):
                        total = jnp.where(group == s - 1, LF[leaf, c * BLK + s * nb + bb], total)
                    out.append(total)
            return jnp.concatenate(out, axis=0)

        def spread(val, flip):
            tiles = val.reshape(count, BLK, WIDE)
            return jnp.concatenate([jnp.where(group == (b // nb) ^ flip, tiles[(b % nb) * TALL + c], 0.0)
                                    for c in range(TALL) for b in range(BLK)], axis=0)

        one, two = (PK[2 * m + e, 0:count].reshape(size, WIDE) for e in PAIR)
        temp = dot(jnp.where(even, coupling(2 * m), shift(coupling(2 * m + 1), lanes)),
                   spread(jnp.where(even, one, shift(two, lanes)), 0))
        corner = dot(jnp.where(even, shift(two, -lanes), one), spread(temp, 1))
        for e, (val, low) in enumerate(((one, corner), (two, shift(corner, -lanes)))):
            parts = (jnp.where(even, val, 0.0), jnp.where(even, -low, val))
            for half in PAIR:
                tiles = parts[half].reshape(count, BLK, WIDE)
                if nb < TALL:
                    PK[2 * m + e, half * count:(half + 1) * count] = tiles
                else:
                    for i in range(count):
                        LI[2 * m + e, (i % TALL) * BLK + half * TALL + i // TALL] = tiles[i]

    mark("n_dbl1")
    for m in PAIR:
        double(m, 1)
    mark("n_two2")
    across((2,))
    mark("j_c0")

    @pl.when(first_half)
    def _():
        for s in SIDES:
            net.wait(("c0", s), C0.at[:, 0])
            piece = C0.at[0 if s < 0 else 1, ys(s)]
            net.start(piece, piece, along("y", -s), "c0far", "c0far")

    mark("n_dbl2")
    for m in PAIR:
        double(m, 2)
    mark("n_dbl4")
    for m in PAIR:
        double(m, 4)
    mark("o_arr2")
    net.wait((2, "far"), G.at[pl.ds(0, 3), 2, 0])

    def leaf_inv(i):
        return LI[i].reshape(WIDE, WIDE)

    def coupling2(m):
        return halves([gathered(k, 2) for k in range(cols)], m)

    def mine(i):
        r, l = iota((WIDE, WIDE), 0), iota((WIDE, WIDE), 1)
        own = CORES * x + r // LANES
        return jnp.where(((r // quarter) % TALL == i) & (l // HALF == own % cols) & (r % BLK == l % BLK)
                         & ((l % HALF) // BLK == 2 * ((r // BLK) % TALL) + own // cols), 1.0, 0.0)

    def put_w(ref, val):
        ref[...] = val.reshape(TALL, TALL, 2, BLK, LANES)
        return val

    def put_z(i, val):
        ZM[i] = val[:LANES]
        ZS[i] = val[LANES:]
        net.start(ZS.at[i], ZM.at[i], partner, "z", "z")
        return val

    def t_piece(side, step, k=None):
        xx = xs(step)
        return TG.at[side, xx // 2, pl.ds(2 * (xx % 2), 2) if k is None else 2 * (xx % 2) + k]

    def t_start(side, step, k, device, name, kind="t"):
        net.start(t_piece(side, step, k), t_piece(side, step, k), device, kind, (side, name))

    def t_send(side, val):
        t_piece(side, 0)[...] = val.reshape(CORES, TALL, TALL, BLK, LANES)
        for i in PAIR:
            for s in SIDES:
                k = i if s < 0 else 1 - i
                t_start(side, 0, k, along("x", -s), (s, i))
        t_start(side, 0, None, partner, "partner", "tpair")

    def t_near(side):
        for i in PAIR:
            for s in SIDES:
                k = i if s < 0 else 1 - i
                net.wait((side, (s, i)), t_piece(side, s, k))
                if i == 0:
                    t_start(side, s, k, along("x", -s), "far")
                t_start(side, s, k, partner, "partner", "tpair")

    def t_far(side):
        net.wait((side, "far"), t_piece(side, 2))
        t_start(side, 2, None, partner, "partner", "tpair")

    def c0_pair(n):
        return [jnp.concatenate([C0[k, c, :, LANES * n:LANES * (n + 1)] for k in range(CORES)], axis=0) for c in range(cols)]

    def own_columns(first, second):
        low = iota((first.shape[0], LANES), 1) < HALF
        out = []
        for val in (first, second):
            tile = jnp.where(y // 2 == 0, val[:, :LANES], val[:, LANES:])
            moved = pltpu.roll(tile, HALF, 1)
            out.append(jnp.where(y % 2 == 0, tile, moved) if val is first else jnp.where(y % 2 == 0, moved, tile))
        return jnp.where(low, out[0], out[1])

    def w_rows(ref):
        own = CORES * x
        return ref.at[..., own % cols, :, :, own // cols, :, :]

    mark("p_chain1")
    low_half = iota((WIDE, LANES), 1) < HALF
    blank = jnp.zeros((WIDE, WIDE), F32)

    def two_columns(one, two, coupling):
        head = own_columns(one, blank)
        return head, jnp.where(low_half, -dot(two, dot(coupling, head)), own_columns(blank, two))

    @pl.when(first_half)
    def _():
        head, tail = two_columns(leaf_inv(0), leaf_inv(1), coupling2(0))
        put_w(WL.at[0, :, 0], head)
        put_w(WL.at[0, :, 1], tail)

    @pl.when(core == 0)
    def _():
        z3 = put_z(3, dot(mine(3), leaf_inv(3)))
        put_z(2, dot(mine(2) - dot(z3, coupling2(1)), leaf_inv(2)))

    mark("q_c1")
    net.wait("c1", G.at[pl.ds(0, 3), 0, 0])

    def x_piece(step):
        xx = xs(step)
        return SX.at[xx // 2, pl.ds(2 * (xx % 2), 2)]

    @pl.when(first_half)
    def _():
        def own_rows(k):
            return jnp.concatenate(
                [G[k, g, x // 2, 2 * (x % 2) + kk, a] for kk in range(CORES) for g in (3, 4) for a in range(TALL)], axis=0)

        product = dot(jnp.concatenate([own_rows(k) for k in range(cols)], axis=1), WL[0].reshape(2 * WIDE, LANES))
        x_piece(0)[...] = product.reshape(CORES, 2, TALL, BLK, LANES)
        for d in range(1, chips):
            net.start(x_piece(0), x_piece(0), along("x", d), "share", "share")

    @pl.when(core == 0)
    def _():
        lhs = [jnp.concatenate([ZM[i, HALF:], ZS[i, HALF:]], axis=0) for i in (2, 3)]
        YX[y] = sum(dot(lhs[i], gathered(y, 3 + i)) for i in PAIR)
        for d in range(1, cols):
            net.start(YX.at[y], YX.at[y], along("y", d), "share", "share")

    mark("q_c0")

    @pl.when(first_half)
    def _():
        net.wait("c0pair", C0.at[0, 0])
        net.wait("c0far", C0.at[0, pl.ds(0, 2)])
        TP[...] = dot(jnp.concatenate(c0_pair(0), axis=1), WL[0].reshape(2 * WIDE, LANES))

    mark("r_V")

    @pl.when(first_half)
    def _():
        right = c0_pair(1)
        v3 = dot(halves(right, 1), leaf_inv(3))
        v2 = dot(halves(right, 0) - dot(v3, coupling2(1)), leaf_inv(2))
        VV[:, :WIDE] = v2
        VV[:, WIDE:] = v3
        t_send(1, own_columns(v2, v3))

    mark("o_share")
    net.wait("share", G.at[pl.ds(0, 3), 0, 0])
    mark("p_chain2")

    @pl.when(first_half)
    def _():
        for g in PAIR:
            for c in range(TALL):
                for i in range(BLK):
                    SS[(g * TALL + c) * BLK + i] = SX[i % 2, c, g, i // 2]
        shared = SS[...].reshape(2 * WIDE, LANES)
        t_send(0, TP[...] - dot(VV[...], shared))
        t_near(1)
        w2 = put_w(WL.at[1, :, 0], -dot(leaf_inv(2), shared[:WIDE]))
        put_w(WL.at[1, :, 1], -dot(leaf_inv(3), shared[WIDE:] + dot(coupling2(1), w2)))
        head, tail = two_columns(leaf_inv(2), leaf_inv(3), coupling2(1))
        put_w(WR.at[:, 0], head)
        put_w(WR.at[:, 1], tail)
        net.start(w_rows(WL), w_rows(WL), partner, "w", "w")
        net.start(w_rows(WR), w_rows(WR), partner, "w", "w")
        t_near(0)

    @pl.when(core == 0)
    def _():
        none = jnp.zeros((HALF, LANES), F32)
        tiles = [jnp.concatenate([none, YX[k, :HALF], none, YX[k, HALF:]], axis=0) for k in range(cols)]
        z1 = put_z(1, dot(mine(1) - halves(tiles, 1), leaf_inv(1)))
        put_z(0, dot(mine(0) - halves(tiles, 0) - dot(z1, coupling2(0)), leaf_inv(0)))
        net.wait("w", G.at[0, pl.ds(0, 3), 0, pl.ds(0, 2)])

    mark("s_out")

    @pl.when(first_half)
    def _():
        net.wait("z", ZM)

    o_ref[upper, far] = jnp.zeros((LANES, WIDE), F32)
    for i in range(TALL):
        lines = slice(quarter * i, quarter * (i + 1))
        o_ref[lines, :LANES] = WL[i // 2, spot, i % 2, :, hh].reshape(quarter, LANES)
        o_ref[lines, LANES:WIDE] = WR[spot, i % 2, :, hh].reshape(quarter, LANES) if i >= 2 else jnp.zeros((quarter, LANES), F32)
    o_ref[lower, far] = jnp.concatenate([own_columns(ZM[2 * n], ZM[2 * n + 1]) for n in PAIR], axis=1)

    def x21(side):
        total = 0.0
        for i in range(TALL):
            part = jnp.concatenate([TG[side, b % 2, c, i, b // 2] for c in range(TALL) for b in range(BLK)], axis=0)
            total = total - dot(ZM[i], part)
        o_ref[lower, LANES * side:LANES * (side + 1)] = total

    for side in (1, 0):
        mark(f"t_in{side}")

        @pl.when(first_half)
        def _():
            t_far(side)

        @pl.when(core == 0)
        def _():
            net.wait((side, "partner"), TG.at[side])

        mark(f"u_x21{side}")
        x21(side)

    mark("v_end")
    for name in ("leaf", 0, 1, 2):
        net.wait(name, G.at[0, :, 0], "send")
    net.wait("link", U, "send")
    net.wait("rest", G.at[pl.ds(0, 3), 0, 0], "send")
    net.wait("share", G.at[pl.ds(0, 3), 0, 0], "send")
    net.wait("pair", U.at[0], "send")
    net.wait("c0", C0.at[0, pl.ds(0, 2)], "send")

    @pl.when(first_half)
    def _():
        net.wait("c0far", C0.at[0, pl.ds(0, 2)], "send")
        net.wait("t", G.at[:, pl.ds(0, 3), 0], "send")
        net.wait("tpair", TG, "send")
        net.wait("w", G.at[0, pl.ds(0, 3), 0, pl.ds(0, 2)], "send")

    @pl.when(core == 0)
    def _():
        net.wait("c0pair", C0.at[0, 0], "send")
        net.wait("z", ZM, "send")

    mark()
    counts = [len([key for key in net.names if key[0] == side]) for side in ("send", "recv")]
    assert counts == [send.shape[0], recv.shape[0]], counts


def solution(mesh):
    rows, cols = mesh.shape["row"], mesh.shape["col"]
    block_spec = P(("batch", "row"), "col")

    def device_body(local_l):
        vmem = functools.partial(pltpu.VMEM, dtype=F32)
        return pl.pallas_call(
            functools.partial(kernel, rows, cols),
            out_shape=pltpu.VMEM(local_l.shape, F32),
            in_specs=[pl.BlockSpec(memory_space=pl.ANY)],
            out_specs=pl.BlockSpec(memory_space=pltpu.VMEM),
            scratch_shapes=[
                vmem(local_l.shape),
                vmem((2, GROUPS, TALL, BLK, LANES)),
                vmem((cols, GROUPS, 2, TALL, TALL, BLK, LANES)),
                vmem((CORES, cols, LANES, WIDE)),
                vmem((TALL, TALL * BLK, BLK, WIDE)),
                vmem((TALL, 2 * BLK, BLK, WIDE)),
                vmem((TALL, TALL * BLK, BLK, WIDE)),
                vmem((2, cols, 2, TALL, 2, BLK, LANES)),
                vmem((cols, 2, TALL, 2, BLK, LANES)),
                vmem((TALL, LANES, WIDE)),
                vmem((TALL, LANES, WIDE)),
                vmem((2, 2, TALL, TALL, TALL, BLK, LANES)),
                vmem((2, TALL, 2, TALL, BLK, LANES)),
                vmem((cols, LANES, LANES)),
                vmem((WIDE, 2 * WIDE)),
                vmem((2 * TALL * BLK, BLK, LANES)),
                vmem((WIDE, LANES)),
                pltpu.SemaphoreType.DMA((3,)),
                pltpu.SemaphoreType.DMA((15,)),
                pltpu.SemaphoreType.DMA((45,)),
            ],
            compiler_params=pltpu.CompilerParams(collective_id=0, has_side_effects=True),
        )(local_l)

    return jax.shard_map(device_body, mesh=mesh, in_specs=(block_spec,), out_specs=block_spec, check_vma=False)
```

```python
import functools

import jax
import jax.numpy as jnp
from jax import lax
from jax.experimental import pallas as pl
from jax.experimental.pallas import tpu as pltpu
from jax.sharding import PartitionSpec as P

BLK = 8
CORES = 2
LANES = 128
HALF = LANES // 2
WIDE = 2 * LANES
TALL = 4
GROUPS = 5
LEAVES = range(2)
PAIR = range(2)
SIDES = (-1, 1)
MESH = pl.DeviceIdType.MESH
F32 = jnp.float32


def dot(left, right):
    return jnp.dot(left, right, precision=lax.Precision.HIGHEST, preferred_element_type=F32)


def iota(shape, dim):
    return lax.broadcasted_iota(jnp.int32, shape, dim)


def halves(tiles, half):
    low = iota(tiles[0].shape, 1) < HALF
    out = []
    for first, second in ((tiles[0], tiles[1]), (tiles[2], tiles[3])):
        if half == 0:
            out.append(jnp.where(low, first, pltpu.roll(second, HALF, 1)))
        else:
            out.append(jnp.where(low, pltpu.roll(first, HALF, 1), second))
    return jnp.concatenate(out, axis=1)


class Net:
    def __init__(self, send, recv):
        self.send, self.recv, self.names = send, recv, {}

    def slot(self, side, name):
        held = [key for key in self.names if key[0] == side]
        return self.names.setdefault((side, name), len(held))

    def start(self, src, dst, device, send, recv):
        self.make(src, dst, device, send, recv).start()

    def make(self, src, dst, device, send, recv):
        return pltpu.make_async_remote_copy(
            src_ref=src, dst_ref=dst, send_sem=self.send.at[self.slot("send", send)], recv_sem=self.recv.at[self.slot("recv", recv)],
            device_id=device, device_id_type=MESH)

    def wait(self, name, like, side="recv"):
        sems = self.recv if side == "recv" else self.send
        pltpu.make_async_copy(like, like, sems.at[self.slot(side, name)]).wait()


def shift(val, lanes):
    return jnp.concatenate([pltpu.roll(val[:, LANES * i:LANES * (i + 1)], lanes % LANES, 1) for i in range(2)], axis=1)


def kernel(rows, cols, hbm_ref, o_ref, l_ref, U, G, C0, LF, PK, LI, WL, WR, ZM, ZS, TG, SX, YX, VV, SS, TP, load, send, recv):
    chips = rows // CORES
    row = lax.axis_index("row")
    y = lax.axis_index("col")
    x, core = row // CORES, row % CORES
    spot, hh = row % cols, row // cols
    net = Net(send, recv)
    first_half = core == 1

    def at(xx, cc, yy):
        return {"row": xx * CORES + cc, "col": yy}

    def xs(step):
        return lax.rem(x + step + chips, chips)

    def ys(step):
        return lax.rem(y + step + cols, cols)

    def along(axis, step, cc=core):
        return at(xs(step), cc, y) if axis == "x" else at(x, cc, ys(step))

    upper, lower, near, far = pl.ds(0, LANES), pl.ds(LANES, LANES), pl.ds(0, WIDE), pl.ds(WIDE, WIDE)
    windows = [(upper, near), (lower, far), (lower, near)]
    loads = [pltpu.make_async_copy(hbm_ref.at[w], l_ref.at[w], load.at[i]) for i, w in enumerate(windows)]
    for made in loads:
        made.start()
    partner = at(x, 1 - core, y)
    barrier = pltpu.get_barrier_semaphore()
    peers = [partner] + [along(axis, d, cc) for axis in "xy" for d in range(1, chips) for cc in range(CORES)]
    for peer in peers:
        pl.semaphore_signal(barrier, inc=1, device_id=peer, device_id_type=MESH)

    quarter = LANES // TALL
    for part in range(2):
        loads[part].wait()
        piece = l_ref[part * LANES:(part + 1) * LANES, part * WIDE:(part + 1) * WIDE]
        low = iota((quarter, LANES), 1) < HALF
        band = [piece[quarter * i:quarter * (i + 1)] for i in range(TALL)]
        packed = [jnp.where(low, band[2 * m][:, LANES * m:LANES * (m + 1)], band[2 * m + 1][:, LANES * m:LANES * (m + 1)])
                  for m in PAIR]
        packed.append(jnp.where(low, band[1][:, :LANES], pltpu.roll(band[3][:, LANES:], HALF, 1)))
        packed += [band[2][:, :LANES], band[3][:, :LANES]]
        tiles = [val.reshape(TALL, BLK, LANES) for val in packed]
        for g in range(GROUPS):
            U[part, g] = tiles[g]

        @pl.when(core == 1 - part)
        def _():
            for g in range(GROUPS):
                G[y, g, hh, spot] = tiles[g]

    loads[2].wait()
    C0[core, y] = l_ref[lower, near]
    pl.semaphore_wait(barrier, len(peers))

    axis_first = ["x", "y", "y"]

    def other(axis):
        return "y" if axis == "x" else "x"

    def source(g, f, s, k=None):
        xx, yy = (xs(f), ys(s)) if axis_first[g] == "x" else (xs(s), ys(f))
        return G.at[yy, g, xx // 2, pl.ds(2 * (xx % 2), 2) if k is None else 2 * (xx % 2) + k]

    def pass_on(g, f, s, k, step, name):
        piece = source(g, f, s, k)
        net.start(piece, piece, along(other(axis_first[g]), step), g, name)

    def pass_leaf(g, f):
        for s in SIDES:
            pass_on(g, f, 0, None, -s, (g, "far") if f == 2 else (g, f, s))
        if f == 2:
            pass_on(g, f, 0, None, 2, (g, "far"))

    def half_on(g, f, s):
        pass_on(g, f, s, 0 if s < 0 else 1, -s, (g, "far"))

    for axis in "xy":
        for step in SIDES:
            for part in range(2):
                net.start(U.at[part, pl.ds(0, 2)], G.at[y, pl.ds(0, 2), hh, spot], along(axis, step, 1 - part), "leaf", ("leaf", axis, -step))
    for g in LEAVES:
        for part in range(2):
            net.start(U.at[part, g], G.at[y, g, hh, spot], along(axis_first[g], 2, 1 - part), "leaf", (g, "two"))
    net.start(U.at[core], G.at[y, :, hh, spot], partner, "pair", "pair")
    for s in SIDES:
        net.start(l_ref.at[lower, near], C0.at[core, y], along("y", -s, 1), "c0", ("c0", s))

    @pl.when(core == 0)
    def _():
        net.start(l_ref.at[lower, near], C0.at[core, y], partner, "c0pair", "c0pair")


    def near_by(groups, name, count):
        for step in SIDES:
            for axis in "xy":
                net.wait((name, axis, step), G.at[0, pl.ds(0, count), 0, pl.ds(0, 2)])
                for g in groups:
                    if axis_first[g] == axis:
                        pass_leaf(g, step)
                    else:
                        half_on(g, 0, step)

    def two_away(groups):
        for g in groups:
            net.wait((g, "two"), G.at[0, 0, 0, pl.ds(0, 2)])
            pass_leaf(g, 2)

    def across(groups):
        for f in SIDES:
            for s in SIDES:
                for g in groups:
                    net.wait((g, f, s), source(g, f, s))
                    half_on(g, f, s)

    near_by(LEAVES, "leaf", 2)
    for part in range(2):
        for axis in "xy":
            for step in SIDES:
                net.start(U.at[part, 2], G.at[y, 2, hh, spot], along(axis, step, 1 - part), "link", ("link", axis, -step))
        net.start(U.at[part, 2], G.at[y, 2, hh, spot], along(axis_first[2], 2, 1 - part), "link", (2, "two"))
    two_away(LEAVES)
    across(LEAVES)
    net.wait("pair", U.at[0])
    near_by((2,), "link", 1)
    for d in range(1, chips):
        for part, axis in enumerate("yx"):
            net.start(U.at[part, pl.ds(3, 2)], G.at[y, pl.ds(3, 2), hh, spot], along(axis, d, 1 - part), "rest", "c1")


    @pl.when(first_half)
    def _():
        for s in SIDES:
            net.wait(("c0", s), C0.at[:, 0])
            piece = C0.at[0 if s < 0 else 1, ys(s)]
            net.start(piece, piece, along("y", -s), "c0far", "c0far")

    for g in LEAVES:
        net.wait((g, "far"), G.at[pl.ds(0, 3), g, 0])

    two_away((2,))
    lane = iota((BLK, LANES), 1)
    sub = iota((BLK, LANES), 0)
    block_of = (lane // BLK) % BLK
    diag = [[[None] * TALL for _ in range(TALL)] for _ in PAIR]
    inv = [[[None] * TALL for _ in range(TALL)] for _ in PAIR]
    for m in PAIR:
        for c in range(TALL):
            for k in range(c + 1):
                total = jnp.zeros((BLK, LANES), F32)
                for b in range(BLK):
                    total = jnp.where(block_of == b, G[k, m, b % 2, c, b // 2], total)
                diag[m][c][k] = total
                inv[m][c][k] = jnp.where(sub == lane % BLK, 1.0, 0.0) if c == k else jnp.zeros((BLK, LANES), F32)
    for t in range(BLK * TALL):
        ct, jt = t // BLK, t % BLK
        index = (lane // BLK) * BLK + jt
        for m in PAIR:
            spread = [jnp.take_along_axis(diag[m][c][ct], index, axis=1) for c in range(ct, TALL)]
            pivot = 1.0 / spread[0][jt:jt + 1, :]
            below = jnp.where(sub > jt, spread[0], 0.0)
            for k in range(ct + 1):
                solved = inv[m][ct][k][jt:jt + 1, :] * pivot
                inv[m][ct][k] = jnp.where(sub == jt, solved, inv[m][ct][k] - below * solved)
                for c in range(ct + 1, TALL):
                    inv[m][c][k] = inv[m][c][k] - spread[c - ct] * solved
    for m in PAIR:
        for c in range(TALL):
            tiles = [inv[m][c][k] if k <= c else jnp.zeros((BLK, LANES), F32) for k in range(TALL)]
            for e in PAIR:
                PK[2 * m + e, c] = halves(tiles, e)

    def gathered(k, g):
        return jnp.concatenate([G[k, g, b % 2, c, b // 2] for c in range(TALL) for b in range(BLK)], axis=0)

    for m in PAIR:
        tiles = [gathered(k, m) for k in range(cols)]
        for e in PAIR:
            LF[2 * m + e] = halves(tiles, e).reshape(TALL * BLK, BLK, WIDE)

    def double(m, nb):
        count, lanes = TALL * nb, BLK * nb
        size = BLK * count
        group = ((iota((BLK, WIDE), 1) % HALF) // BLK) // nb
        even = ((iota((size, WIDE), 1) % HALF) // BLK) // nb % 2 == 0

        def coupling(leaf):
            out = []
            for bb in range(nb):
                for c in range(TALL):
                    total = LF[leaf, c * BLK + nb + bb]
                    for s in range(3, BLK // nb, 2):
                        total = jnp.where(group == s - 1, LF[leaf, c * BLK + s * nb + bb], total)
                    out.append(total)
            return jnp.concatenate(out, axis=0)

        def spread(val, flip):
            tiles = val.reshape(count, BLK, WIDE)
            return jnp.concatenate([jnp.where(group == (b // nb) ^ flip, tiles[(b % nb) * TALL + c], 0.0)
                                    for c in range(TALL) for b in range(BLK)], axis=0)

        one, two = (PK[2 * m + e, 0:count].reshape(size, WIDE) for e in PAIR)
        temp = dot(jnp.where(even, coupling(2 * m), shift(coupling(2 * m + 1), lanes)),
                   spread(jnp.where(even, one, shift(two, lanes)), 0))
        corner = dot(jnp.where(even, shift(two, -lanes), one), spread(temp, 1))
        for e, (val, low) in enumerate(((one, corner), (two, shift(corner, -lanes)))):
            parts = (jnp.where(even, val, 0.0), jnp.where(even, -low, val))
            for half in PAIR:
                tiles = parts[half].reshape(count, BLK, WIDE)
                if nb < TALL:
                    PK[2 * m + e, half * count:(half + 1) * count] = tiles
                else:
                    for i in range(count):
                        LI[2 * m + e, (i % TALL) * BLK + half * TALL + i // TALL] = tiles[i]

    for m in PAIR:
        double(m, 1)
    across((2,))
    for m in PAIR:
        double(m, 2)
    for m in PAIR:
        double(m, 4)
    net.wait((2, "far"), G.at[pl.ds(0, 3), 2, 0])

    def leaf_inv(i):
        return LI[i].reshape(WIDE, WIDE)

    def coupling2(m):
        return halves([gathered(k, 2) for k in range(cols)], m)

    def mine(i):
        r, l = iota((WIDE, WIDE), 0), iota((WIDE, WIDE), 1)
        own = CORES * x + r // LANES
        return jnp.where(((r // quarter) % TALL == i) & (l // HALF == own % cols) & (r % BLK == l % BLK)
                         & ((l % HALF) // BLK == 2 * ((r // BLK) % TALL) + own // cols), 1.0, 0.0)

    def put_w(ref, val):
        ref[...] = val.reshape(TALL, TALL, 2, BLK, LANES)
        return val

    def put_z(i, val):
        ZM[i] = val[:LANES]
        ZS[i] = val[LANES:]
        net.start(ZS.at[i], ZM.at[i], partner, "z", "z")
        return val

    def t_piece(side, step, k=None):
        xx = xs(step)
        return TG.at[side, xx // 2, pl.ds(2 * (xx % 2), 2) if k is None else 2 * (xx % 2) + k]

    def t_start(side, step, k, device, name, kind="t"):
        net.start(t_piece(side, step, k), t_piece(side, step, k), device, kind, (side, name))

    def t_send(side, val):
        t_piece(side, 0)[...] = val.reshape(CORES, TALL, TALL, BLK, LANES)
        for i in PAIR:
            for s in SIDES:
                k = i if s < 0 else 1 - i
                t_start(side, 0, k, along("x", -s), (s, i))
        t_start(side, 0, None, partner, "partner", "tpair")

    def t_near(side):
        for i in PAIR:
            for s in SIDES:
                k = i if s < 0 else 1 - i
                net.wait((side, (s, i)), t_piece(side, s, k))
                if i == 0:
                    t_start(side, s, k, along("x", -s), "far")
                t_start(side, s, k, partner, "partner", "tpair")

    def t_far(side):
        net.wait((side, "far"), t_piece(side, 2))
        t_start(side, 2, None, partner, "partner", "tpair")

    def c0_pair(n):
        return [jnp.concatenate([C0[k, c, :, LANES * n:LANES * (n + 1)] for k in range(CORES)], axis=0) for c in range(cols)]

    def own_columns(first, second):
        low = iota((first.shape[0], LANES), 1) < HALF
        out = []
        for val in (first, second):
            tile = jnp.where(y // 2 == 0, val[:, :LANES], val[:, LANES:])
            moved = pltpu.roll(tile, HALF, 1)
            out.append(jnp.where(y % 2 == 0, tile, moved) if val is first else jnp.where(y % 2 == 0, moved, tile))
        return jnp.where(low, out[0], out[1])

    def w_rows(ref):
        own = CORES * x
        return ref.at[..., own % cols, :, :, own // cols, :, :]

    low_half = iota((WIDE, LANES), 1) < HALF
    blank = jnp.zeros((WIDE, WIDE), F32)

    def two_columns(one, two, coupling):
        head = own_columns(one, blank)
        return head, jnp.where(low_half, -dot(two, dot(coupling, head)), own_columns(blank, two))

    @pl.when(first_half)
    def _():
        head, tail = two_columns(leaf_inv(0), leaf_inv(1), coupling2(0))
        put_w(WL.at[0, :, 0], head)
        put_w(WL.at[0, :, 1], tail)

    @pl.when(core == 0)
    def _():
        z3 = put_z(3, dot(mine(3), leaf_inv(3)))
        put_z(2, dot(mine(2) - dot(z3, coupling2(1)), leaf_inv(2)))

    net.wait("c1", G.at[pl.ds(0, 3), 0, 0])

    def x_piece(step):
        xx = xs(step)
        return SX.at[xx // 2, pl.ds(2 * (xx % 2), 2)]

    @pl.when(first_half)
    def _():
        def own_rows(k):
            return jnp.concatenate(
                [G[k, g, x // 2, 2 * (x % 2) + kk, a] for kk in range(CORES) for g in (3, 4) for a in range(TALL)], axis=0)

        product = dot(jnp.concatenate([own_rows(k) for k in range(cols)], axis=1), WL[0].reshape(2 * WIDE, LANES))
        x_piece(0)[...] = product.reshape(CORES, 2, TALL, BLK, LANES)
        for d in range(1, chips):
            net.start(x_piece(0), x_piece(0), along("x", d), "share", "share")

    @pl.when(core == 0)
    def _():
        lhs = [jnp.concatenate([ZM[i, HALF:], ZS[i, HALF:]], axis=0) for i in (2, 3)]
        YX[y] = sum(dot(lhs[i], gathered(y, 3 + i)) for i in PAIR)
        for d in range(1, cols):
            net.start(YX.at[y], YX.at[y], along("y", d), "share", "share")


    @pl.when(first_half)
    def _():
        net.wait("c0pair", C0.at[0, 0])
        net.wait("c0far", C0.at[0, pl.ds(0, 2)])
        TP[...] = dot(jnp.concatenate(c0_pair(0), axis=1), WL[0].reshape(2 * WIDE, LANES))


    @pl.when(first_half)
    def _():
        right = c0_pair(1)
        v3 = dot(halves(right, 1), leaf_inv(3))
        v2 = dot(halves(right, 0) - dot(v3, coupling2(1)), leaf_inv(2))
        VV[:, :WIDE] = v2
        VV[:, WIDE:] = v3
        t_send(1, own_columns(v2, v3))

    net.wait("share", G.at[pl.ds(0, 3), 0, 0])

    @pl.when(first_half)
    def _():
        for g in PAIR:
            for c in range(TALL):
                for i in range(BLK):
                    SS[(g * TALL + c) * BLK + i] = SX[i % 2, c, g, i // 2]
        shared = SS[...].reshape(2 * WIDE, LANES)
        t_send(0, TP[...] - dot(VV[...], shared))
        t_near(1)
        w2 = put_w(WL.at[1, :, 0], -dot(leaf_inv(2), shared[:WIDE]))
        put_w(WL.at[1, :, 1], -dot(leaf_inv(3), shared[WIDE:] + dot(coupling2(1), w2)))
        head, tail = two_columns(leaf_inv(2), leaf_inv(3), coupling2(1))
        put_w(WR.at[:, 0], head)
        put_w(WR.at[:, 1], tail)
        net.start(w_rows(WL), w_rows(WL), partner, "w", "w")
        net.start(w_rows(WR), w_rows(WR), partner, "w", "w")
        t_near(0)

    @pl.when(core == 0)
    def _():
        none = jnp.zeros((HALF, LANES), F32)
        tiles = [jnp.concatenate([none, YX[k, :HALF], none, YX[k, HALF:]], axis=0) for k in range(cols)]
        z1 = put_z(1, dot(mine(1) - halves(tiles, 1), leaf_inv(1)))
        put_z(0, dot(mine(0) - halves(tiles, 0) - dot(z1, coupling2(0)), leaf_inv(0)))
        net.wait("w", G.at[0, pl.ds(0, 3), 0, pl.ds(0, 2)])


    @pl.when(first_half)
    def _():
        net.wait("z", ZM)

    o_ref[upper, far] = jnp.zeros((LANES, WIDE), F32)
    for i in range(TALL):
        lines = slice(quarter * i, quarter * (i + 1))
        o_ref[lines, :LANES] = WL[i // 2, spot, i % 2, :, hh].reshape(quarter, LANES)
        o_ref[lines, LANES:WIDE] = WR[spot, i % 2, :, hh].reshape(quarter, LANES) if i >= 2 else jnp.zeros((quarter, LANES), F32)
    o_ref[lower, far] = jnp.concatenate([own_columns(ZM[2 * n], ZM[2 * n + 1]) for n in PAIR], axis=1)

    def x21(side):
        total = 0.0
        for i in range(TALL):
            part = jnp.concatenate([TG[side, b % 2, c, i, b // 2] for c in range(TALL) for b in range(BLK)], axis=0)
            total = total - dot(ZM[i], part)
        o_ref[lower, LANES * side:LANES * (side + 1)] = total

    for side in (1, 0):

        @pl.when(first_half)
        def _():
            t_far(side)

        @pl.when(core == 0)
        def _():
            net.wait((side, "partner"), TG.at[side])

        x21(side)

    for name in ("leaf", 0, 1, 2):
        net.wait(name, G.at[0, :, 0], "send")
    net.wait("link", U, "send")
    net.wait("rest", G.at[pl.ds(0, 3), 0, 0], "send")
    net.wait("share", G.at[pl.ds(0, 3), 0, 0], "send")
    net.wait("pair", U.at[0], "send")
    net.wait("c0", C0.at[0, pl.ds(0, 2)], "send")

    @pl.when(first_half)
    def _():
        net.wait("c0far", C0.at[0, pl.ds(0, 2)], "send")
        net.wait("t", G.at[:, pl.ds(0, 3), 0], "send")
        net.wait("tpair", TG, "send")
        net.wait("w", G.at[0, pl.ds(0, 3), 0, pl.ds(0, 2)], "send")

    @pl.when(core == 0)
    def _():
        net.wait("c0pair", C0.at[0, 0], "send")
        net.wait("z", ZM, "send")

    counts = [len([key for key in net.names if key[0] == side]) for side in ("send", "recv")]
    assert counts == [send.shape[0], recv.shape[0]], counts


def solution(mesh):
    rows, cols = mesh.shape["row"], mesh.shape["col"]
    block_spec = P(("batch", "row"), "col")

    def device_body(local_l):
        vmem = functools.partial(pltpu.VMEM, dtype=F32)
        return pl.pallas_call(
            functools.partial(kernel, rows, cols),
            out_shape=pltpu.VMEM(local_l.shape, F32),
            in_specs=[pl.BlockSpec(memory_space=pl.ANY)],
            out_specs=pl.BlockSpec(memory_space=pltpu.VMEM),
            scratch_shapes=[
                vmem(local_l.shape),
                vmem((2, GROUPS, TALL, BLK, LANES)),
                vmem((cols, GROUPS, 2, TALL, TALL, BLK, LANES)),
                vmem((CORES, cols, LANES, WIDE)),
                vmem((TALL, TALL * BLK, BLK, WIDE)),
                vmem((TALL, 2 * BLK, BLK, WIDE)),
                vmem((TALL, TALL * BLK, BLK, WIDE)),
                vmem((2, cols, 2, TALL, 2, BLK, LANES)),
                vmem((cols, 2, TALL, 2, BLK, LANES)),
                vmem((TALL, LANES, WIDE)),
                vmem((TALL, LANES, WIDE)),
                vmem((2, 2, TALL, TALL, TALL, BLK, LANES)),
                vmem((2, TALL, 2, TALL, BLK, LANES)),
                vmem((cols, LANES, LANES)),
                vmem((WIDE, 2 * WIDE)),
                vmem((2 * TALL * BLK, BLK, LANES)),
                vmem((WIDE, LANES)),
                pltpu.SemaphoreType.DMA((3,)),
                pltpu.SemaphoreType.DMA((15,)),
                pltpu.SemaphoreType.DMA((45,)),
            ],
            compiler_params=pltpu.CompilerParams(collective_id=0, has_side_effects=True),
        )(local_l)

    return jax.shard_map(device_body, mesh=mesh, in_specs=(block_spec,), out_specs=block_spec, check_vma=False)
```

```python
import functools

import jax
import jax.numpy as jnp
from jax import lax
from jax.experimental import pallas as pl
from jax.experimental.pallas import tpu as pltpu
from jax.sharding import PartitionSpec as P

BLK = 8
CORES = 2
LANES = 128
HALF = LANES // 2
WIDE = 2 * LANES
TALL = 4
GROUPS = 5
LEAVES = range(2)
PAIR = range(2)
SIDES = (-1, 1)
MESH = pl.DeviceIdType.MESH
F32 = jnp.float32


def dot(left, right):
    return jnp.dot(left, right, precision=lax.Precision.HIGHEST, preferred_element_type=F32)


def iota(shape, dim):
    return lax.broadcasted_iota(jnp.int32, shape, dim)


def halves(tiles, half):
    low = iota(tiles[0].shape, 1) < HALF
    out = []
    for first, second in ((tiles[0], tiles[1]), (tiles[2], tiles[3])):
        if half == 0:
            out.append(jnp.where(low, first, pltpu.roll(second, HALF, 1)))
        else:
            out.append(jnp.where(low, pltpu.roll(first, HALF, 1), second))
    return jnp.concatenate(out, axis=1)


class Net:
    def __init__(self, send, recv):
        self.send, self.recv, self.names = send, recv, {}

    def slot(self, side, name):
        held = [key for key in self.names if key[0] == side]
        return self.names.setdefault((side, name), len(held))

    def start(self, src, dst, device, send, recv):
        self.make(src, dst, device, send, recv).start()

    def make(self, src, dst, device, send, recv):
        return pltpu.make_async_remote_copy(
            src_ref=src, dst_ref=dst, send_sem=self.send.at[self.slot("send", send)], recv_sem=self.recv.at[self.slot("recv", recv)],
            device_id=device, device_id_type=MESH)

    def wait(self, name, like, side="recv"):
        sems = self.recv if side == "recv" else self.send
        pltpu.make_async_copy(like, like, sems.at[self.slot(side, name)]).wait()


def shift(val, lanes):
    return jnp.concatenate([pltpu.roll(val[:, LANES * i:LANES * (i + 1)], lanes % LANES, 1) for i in range(2)], axis=1)


def kernel(rows, cols, hbm_ref, o_ref, l_ref, U, G, C0, LF, PK, LI, WL, WR, ZM, ZS, TG, SX, YX, VV, SS, TP, load, send, recv):
    chips = rows // CORES
    row = lax.axis_index("row")
    y = lax.axis_index("col")
    x, core = row // CORES, row % CORES
    spot, hh = row % cols, row // cols
    net = Net(send, recv)
    first_half = core == 1

    def at(xx, cc, yy):
        return {"row": xx * CORES + cc, "col": yy}

    def xs(step):
        return lax.rem(x + step + chips, chips)

    def ys(step):
        return lax.rem(y + step + cols, cols)

    def along(axis, step, cc=core):
        return at(xs(step), cc, y) if axis == "x" else at(x, cc, ys(step))

    upper, lower, near, far = pl.ds(0, LANES), pl.ds(LANES, LANES), pl.ds(0, WIDE), pl.ds(WIDE, WIDE)
    windows = [(upper, near), (lower, far), (lower, near)]
    loads = [pltpu.make_async_copy(hbm_ref.at[w], l_ref.at[w], load.at[i]) for i, w in enumerate(windows)]
    for made in loads:
        made.start()
    partner = at(x, 1 - core, y)
    barrier = pltpu.get_barrier_semaphore()
    peers = [partner] + [along(axis, d, cc) for axis in "xy" for d in range(1, chips) for cc in range(CORES)]
    for peer in peers:
        pl.semaphore_signal(barrier, inc=1, device_id=peer, device_id_type=MESH)

    quarter = LANES // TALL
    for part in range(2):
        loads[part].wait()
        piece = l_ref[part * LANES:(part + 1) * LANES, part * WIDE:(part + 1) * WIDE]
        low = iota((quarter, LANES), 1) < HALF
        band = [piece[quarter * i:quarter * (i + 1)] for i in range(TALL)]
        packed = [jnp.where(low, band[2 * m][:, LANES * m:LANES * (m + 1)], band[2 * m + 1][:, LANES * m:LANES * (m + 1)])
                  for m in PAIR]
        packed.append(jnp.where(low, band[1][:, :LANES], pltpu.roll(band[3][:, LANES:], HALF, 1)))
        packed += [band[2][:, :LANES], band[3][:, :LANES]]
        tiles = [val.reshape(TALL, BLK, LANES) for val in packed]
        for g in range(GROUPS):
            U[part, g] = tiles[g]

        @pl.when(core == 1 - part)
        def _():
            for g in range(GROUPS):
                G[y, g, hh, spot] = tiles[g]

    loads[2].wait()
    C0[core, y] = l_ref[lower, near]
    pl.semaphore_wait(barrier, len(peers))

    axis_first = ["y", "y", "x"]

    def other(axis):
        return "y" if axis == "x" else "x"

    def source(g, f, s, k=None):
        xx, yy = (xs(f), ys(s)) if axis_first[g] == "x" else (xs(s), ys(f))
        return G.at[yy, g, xx // 2, pl.ds(2 * (xx % 2), 2) if k is None else 2 * (xx % 2) + k]

    def pass_on(g, f, s, k, step, name):
        piece = source(g, f, s, k)
        net.start(piece, piece, along(other(axis_first[g]), step), g, name)

    def pass_leaf(g, f):
        for s in SIDES:
            pass_on(g, f, 0, None, -s, (g, "far") if f == 2 else (g, f, s))
        if f == 2:
            pass_on(g, f, 0, None, 2, (g, "far"))

    def half_on(g, f, s):
        pass_on(g, f, s, 0 if s < 0 else 1, -s, (g, "far"))

    for axis in "xy":
        for step in SIDES:
            for part in range(2):
                net.start(U.at[part, pl.ds(0, 2)], G.at[y, pl.ds(0, 2), hh, spot], along(axis, step, 1 - part), "leaf", ("leaf", axis, -step))
    for g in LEAVES:
        for part in range(2):
            net.start(U.at[part, g], G.at[y, g, hh, spot], along(axis_first[g], 2, 1 - part), "leaf", (g, "two"))
    net.start(U.at[core], G.at[y, :, hh, spot], partner, "pair", "pair")
    for s in SIDES:
        net.start(l_ref.at[lower, near], C0.at[core, y], along("y", -s, 1), "c0", ("c0", s))

    @pl.when(core == 0)
    def _():
        net.start(l_ref.at[lower, near], C0.at[core, y], partner, "c0pair", "c0pair")


    def near_by(groups, name, count):
        for step in SIDES:
            for axis in "xy":
                net.wait((name, axis, step), G.at[0, pl.ds(0, count), 0, pl.ds(0, 2)])
                for g in groups:
                    if axis_first[g] == axis:
                        pass_leaf(g, step)
                    else:
                        half_on(g, 0, step)

    def two_away(groups):
        for g in groups:
            net.wait((g, "two"), G.at[0, 0, 0, pl.ds(0, 2)])
            pass_leaf(g, 2)

    def across(groups):
        for f in SIDES:
            for s in SIDES:
                for g in groups:
                    net.wait((g, f, s), source(g, f, s))
                    half_on(g, f, s)

    near_by(LEAVES, "leaf", 2)
    for part in range(2):
        for axis in "xy":
            for step in SIDES:
                net.start(U.at[part, 2], G.at[y, 2, hh, spot], along(axis, step, 1 - part), "link", ("link", axis, -step))
        net.start(U.at[part, 2], G.at[y, 2, hh, spot], along(axis_first[2], 2, 1 - part), "link", (2, "two"))
    two_away(LEAVES)
    across(LEAVES)
    net.wait("pair", U.at[0])
    near_by((2,), "link", 1)
    for d in range(1, chips):
        for part, axis in enumerate("yx"):
            net.start(U.at[part, pl.ds(3, 2)], G.at[y, pl.ds(3, 2), hh, spot], along(axis, d, 1 - part), "rest", "c1")


    @pl.when(first_half)
    def _():
        for s in SIDES:
            net.wait(("c0", s), C0.at[:, 0])
            piece = C0.at[0 if s < 0 else 1, ys(s)]
            net.start(piece, piece, along("y", -s), "c0far", "c0far")

    for g in LEAVES:
        net.wait((g, "far"), G.at[pl.ds(0, 3), g, 0])

    two_away((2,))
    lane = iota((BLK, LANES), 1)
    sub = iota((BLK, LANES), 0)
    block_of = (lane // BLK) % BLK
    diag = [[[None] * TALL for _ in range(TALL)] for _ in PAIR]
    inv = [[[None] * TALL for _ in range(TALL)] for _ in PAIR]
    for m in PAIR:
        for c in range(TALL):
            for k in range(c + 1):
                total = jnp.zeros((BLK, LANES), F32)
                for b in range(BLK):
                    total = jnp.where(block_of == b, G[k, m, b % 2, c, b // 2], total)
                diag[m][c][k] = total
                inv[m][c][k] = jnp.where(sub == lane % BLK, 1.0, 0.0) if c == k else jnp.zeros((BLK, LANES), F32)
    for t in range(BLK * TALL):
        ct, jt = t // BLK, t % BLK
        index = (lane // BLK) * BLK + jt
        for m in PAIR:
            spread = [jnp.take_along_axis(diag[m][c][ct], index, axis=1) for c in range(ct, TALL)]
            pivot = 1.0 / spread[0][jt:jt + 1, :]
            below = jnp.where(sub > jt, spread[0], 0.0)
            for k in range(ct + 1):
                solved = inv[m][ct][k][jt:jt + 1, :] * pivot
                inv[m][ct][k] = jnp.where(sub == jt, solved, inv[m][ct][k] - below * solved)
                for c in range(ct + 1, TALL):
                    inv[m][c][k] = inv[m][c][k] - spread[c - ct] * solved
    for m in PAIR:
        for c in range(TALL):
            tiles = [inv[m][c][k] if k <= c else jnp.zeros((BLK, LANES), F32) for k in range(TALL)]
            for e in PAIR:
                PK[2 * m + e, c] = halves(tiles, e)

    def gathered(k, g):
        return jnp.concatenate([G[k, g, b % 2, c, b // 2] for c in range(TALL) for b in range(BLK)], axis=0)

    for m in PAIR:
        tiles = [gathered(k, m) for k in range(cols)]
        for e in PAIR:
            LF[2 * m + e] = halves(tiles, e).reshape(TALL * BLK, BLK, WIDE)

    def double(m, nb):
        count, lanes = TALL * nb, BLK * nb
        size = BLK * count
        group = ((iota((BLK, WIDE), 1) % HALF) // BLK) // nb
        even = ((iota((size, WIDE), 1) % HALF) // BLK) // nb % 2 == 0

        def coupling(leaf):
            out = []
            for bb in range(nb):
                for c in range(TALL):
                    total = LF[leaf, c * BLK + nb + bb]
                    for s in range(3, BLK // nb, 2):
                        total = jnp.where(group == s - 1, LF[leaf, c * BLK + s * nb + bb], total)
                    out.append(total)
            return jnp.concatenate(out, axis=0)

        def spread(val, flip):
            tiles = val.reshape(count, BLK, WIDE)
            return jnp.concatenate([jnp.where(group == (b // nb) ^ flip, tiles[(b % nb) * TALL + c], 0.0)
                                    for c in range(TALL) for b in range(BLK)], axis=0)

        one, two = (PK[2 * m + e, 0:count].reshape(size, WIDE) for e in PAIR)
        temp = dot(jnp.where(even, coupling(2 * m), shift(coupling(2 * m + 1), lanes)),
                   spread(jnp.where(even, one, shift(two, lanes)), 0))
        corner = dot(jnp.where(even, shift(two, -lanes), one), spread(temp, 1))
        for e, (val, low) in enumerate(((one, corner), (two, shift(corner, -lanes)))):
            parts = (jnp.where(even, val, 0.0), jnp.where(even, -low, val))
            for half in PAIR:
                tiles = parts[half].reshape(count, BLK, WIDE)
                if nb < TALL:
                    PK[2 * m + e, half * count:(half + 1) * count] = tiles
                else:
                    for i in range(count):
                        LI[2 * m + e, (i % TALL) * BLK + half * TALL + i // TALL] = tiles[i]

    for m in PAIR:
        double(m, 1)
    across((2,))
    for m in PAIR:
        double(m, 2)
    for m in PAIR:
        double(m, 4)
    net.wait((2, "far"), G.at[pl.ds(0, 3), 2, 0])

    def leaf_inv(i):
        return LI[i].reshape(WIDE, WIDE)

    def coupling2(m):
        return halves([gathered(k, 2) for k in range(cols)], m)

    def mine(i):
        r, l = iota((WIDE, WIDE), 0), iota((WIDE, WIDE), 1)
        own = CORES * x + r // LANES
        return jnp.where(((r // quarter) % TALL == i) & (l // HALF == own % cols) & (r % BLK == l % BLK)
                         & ((l % HALF) // BLK == 2 * ((r // BLK) % TALL) + own // cols), 1.0, 0.0)

    def put_w(ref, val):
        ref[...] = val.reshape(TALL, TALL, 2, BLK, LANES)
        return val

    def put_z(i, val):
        ZM[i] = val[:LANES]
        ZS[i] = val[LANES:]
        net.start(ZS.at[i], ZM.at[i], partner, "z", "z")
        return val

    def t_piece(side, step, k=None):
        xx = xs(step)
        return TG.at[side, xx // 2, pl.ds(2 * (xx % 2), 2) if k is None else 2 * (xx % 2) + k]

    def t_start(side, step, k, device, name, kind="t"):
        net.start(t_piece(side, step, k), t_piece(side, step, k), device, kind, (side, name))

    def t_send(side, val):
        t_piece(side, 0)[...] = val.reshape(CORES, TALL, TALL, BLK, LANES)
        for i in PAIR:
            for s in SIDES:
                k = i if s < 0 else 1 - i
                t_start(side, 0, k, along("x", -s), (s, i))
        t_start(side, 0, None, partner, "partner", "tpair")

    def t_near(side):
        for i in PAIR:
            for s in SIDES:
                k = i if s < 0 else 1 - i
                net.wait((side, (s, i)), t_piece(side, s, k))
                if i == 0:
                    t_start(side, s, k, along("x", -s), "far")
                t_start(side, s, k, partner, "partner", "tpair")

    def t_far(side):
        net.wait((side, "far"), t_piece(side, 2))
        t_start(side, 2, None, partner, "partner", "tpair")

    def c0_pair(n):
        return [jnp.concatenate([C0[k, c, :, LANES * n:LANES * (n + 1)] for k in range(CORES)], axis=0) for c in range(cols)]

    def own_columns(first, second):
        low = iota((first.shape[0], LANES), 1) < HALF
        out = []
        for val in (first, second):
            tile = jnp.where(y // 2 == 0, val[:, :LANES], val[:, LANES:])
            moved = pltpu.roll(tile, HALF, 1)
            out.append(jnp.where(y % 2 == 0, tile, moved) if val is first else jnp.where(y % 2 == 0, moved, tile))
        return jnp.where(low, out[0], out[1])

    def w_rows(ref):
        own = CORES * x
        return ref.at[..., own % cols, :, :, own // cols, :, :]

    low_half = iota((WIDE, LANES), 1) < HALF
    blank = jnp.zeros((WIDE, WIDE), F32)

    def two_columns(one, two, coupling):
        head = own_columns(one, blank)
        return head, jnp.where(low_half, -dot(two, dot(coupling, head)), own_columns(blank, two))

    @pl.when(first_half)
    def _():
        head, tail = two_columns(leaf_inv(0), leaf_inv(1), coupling2(0))
        put_w(WL.at[0, :, 0], head)
        put_w(WL.at[0, :, 1], tail)

    @pl.when(core == 0)
    def _():
        z3 = put_z(3, dot(mine(3), leaf_inv(3)))
        put_z(2, dot(mine(2) - dot(z3, coupling2(1)), leaf_inv(2)))

    net.wait("c1", G.at[pl.ds(0, 3), 0, 0])

    def x_piece(step):
        xx = xs(step)
        return SX.at[xx // 2, pl.ds(2 * (xx % 2), 2)]

    @pl.when(first_half)
    def _():
        def own_rows(k):
            return jnp.concatenate(
                [G[k, g, x // 2, 2 * (x % 2) + kk, a] for kk in range(CORES) for g in (3, 4) for a in range(TALL)], axis=0)

        product = dot(jnp.concatenate([own_rows(k) for k in range(cols)], axis=1), WL[0].reshape(2 * WIDE, LANES))
        x_piece(0)[...] = product.reshape(CORES, 2, TALL, BLK, LANES)
        for d in range(1, chips):
            net.start(x_piece(0), x_piece(0), along("x", d), "share", "share")

    @pl.when(core == 0)
    def _():
        lhs = [jnp.concatenate([ZM[i, HALF:], ZS[i, HALF:]], axis=0) for i in (2, 3)]
        YX[y] = sum(dot(lhs[i], gathered(y, 3 + i)) for i in PAIR)
        for d in range(1, cols):
            net.start(YX.at[y], YX.at[y], along("y", d), "share", "share")


    @pl.when(first_half)
    def _():
        net.wait("c0pair", C0.at[0, 0])
        net.wait("c0far", C0.at[0, pl.ds(0, 2)])
        TP[...] = dot(jnp.concatenate(c0_pair(0), axis=1), WL[0].reshape(2 * WIDE, LANES))


    @pl.when(first_half)
    def _():
        right = c0_pair(1)
        v3 = dot(halves(right, 1), leaf_inv(3))
        v2 = dot(halves(right, 0) - dot(v3, coupling2(1)), leaf_inv(2))
        VV[:, :WIDE] = v2
        VV[:, WIDE:] = v3
        t_send(1, own_columns(v2, v3))

    net.wait("share", G.at[pl.ds(0, 3), 0, 0])

    @pl.when(first_half)
    def _():
        for g in PAIR:
            for c in range(TALL):
                for i in range(BLK):
                    SS[(g * TALL + c) * BLK + i] = SX[i % 2, c, g, i // 2]
        shared = SS[...].reshape(2 * WIDE, LANES)
        t_send(0, TP[...] - dot(VV[...], shared))
        t_near(1)
        w2 = put_w(WL.at[1, :, 0], -dot(leaf_inv(2), shared[:WIDE]))
        put_w(WL.at[1, :, 1], -dot(leaf_inv(3), shared[WIDE:] + dot(coupling2(1), w2)))
        head, tail = two_columns(leaf_inv(2), leaf_inv(3), coupling2(1))
        put_w(WR.at[:, 0], head)
        put_w(WR.at[:, 1], tail)
        net.start(w_rows(WL), w_rows(WL), partner, "w", "w")
        net.start(w_rows(WR), w_rows(WR), partner, "w", "w")
        t_near(0)

    @pl.when(core == 0)
    def _():
        none = jnp.zeros((HALF, LANES), F32)
        tiles = [jnp.concatenate([none, YX[k, :HALF], none, YX[k, HALF:]], axis=0) for k in range(cols)]
        z1 = put_z(1, dot(mine(1) - halves(tiles, 1), leaf_inv(1)))
        put_z(0, dot(mine(0) - halves(tiles, 0) - dot(z1, coupling2(0)), leaf_inv(0)))
        net.wait("w", G.at[0, pl.ds(0, 3), 0, pl.ds(0, 2)])


    @pl.when(first_half)
    def _():
        net.wait("z", ZM)

    o_ref[upper, far] = jnp.zeros((LANES, WIDE), F32)
    for i in range(TALL):
        lines = slice(quarter * i, quarter * (i + 1))
        o_ref[lines, :LANES] = WL[i // 2, spot, i % 2, :, hh].reshape(quarter, LANES)
        o_ref[lines, LANES:WIDE] = WR[spot, i % 2, :, hh].reshape(quarter, LANES) if i >= 2 else jnp.zeros((quarter, LANES), F32)
    o_ref[lower, far] = jnp.concatenate([own_columns(ZM[2 * n], ZM[2 * n + 1]) for n in PAIR], axis=1)

    def x21(side):
        total = 0.0
        for i in range(TALL):
            part = jnp.concatenate([TG[side, b % 2, c, i, b // 2] for c in range(TALL) for b in range(BLK)], axis=0)
            total = total - dot(ZM[i], part)
        o_ref[lower, LANES * side:LANES * (side + 1)] = total

    for side in (1, 0):

        @pl.when(first_half)
        def _():
            t_far(side)

        @pl.when(core == 0)
        def _():
            net.wait((side, "partner"), TG.at[side])

        x21(side)

    for name in ("leaf", 0, 1, 2):
        net.wait(name, G.at[0, :, 0], "send")
    net.wait("link", U, "send")
    net.wait("rest", G.at[pl.ds(0, 3), 0, 0], "send")
    net.wait("share", G.at[pl.ds(0, 3), 0, 0], "send")
    net.wait("pair", U.at[0], "send")
    net.wait("c0", C0.at[0, pl.ds(0, 2)], "send")

    @pl.when(first_half)
    def _():
        net.wait("c0far", C0.at[0, pl.ds(0, 2)], "send")
        net.wait("t", G.at[:, pl.ds(0, 3), 0], "send")
        net.wait("tpair", TG, "send")
        net.wait("w", G.at[0, pl.ds(0, 3), 0, pl.ds(0, 2)], "send")

    @pl.when(core == 0)
    def _():
        net.wait("c0pair", C0.at[0, 0], "send")
        net.wait("z", ZM, "send")

    counts = [len([key for key in net.names if key[0] == side]) for side in ("send", "recv")]
    assert counts == [send.shape[0], recv.shape[0]], counts


def solution(mesh):
    rows, cols = mesh.shape["row"], mesh.shape["col"]
    block_spec = P(("batch", "row"), "col")

    def device_body(local_l):
        vmem = functools.partial(pltpu.VMEM, dtype=F32)
        return pl.pallas_call(
            functools.partial(kernel, rows, cols),
            out_shape=pltpu.VMEM(local_l.shape, F32),
            in_specs=[pl.BlockSpec(memory_space=pl.ANY)],
            out_specs=pl.BlockSpec(memory_space=pltpu.VMEM),
            scratch_shapes=[
                vmem(local_l.shape),
                vmem((2, GROUPS, TALL, BLK, LANES)),
                vmem((cols, GROUPS, 2, TALL, TALL, BLK, LANES)),
                vmem((CORES, cols, LANES, WIDE)),
                vmem((TALL, TALL * BLK, BLK, WIDE)),
                vmem((TALL, 2 * BLK, BLK, WIDE)),
                vmem((TALL, TALL * BLK, BLK, WIDE)),
                vmem((2, cols, 2, TALL, 2, BLK, LANES)),
                vmem((cols, 2, TALL, 2, BLK, LANES)),
                vmem((TALL, LANES, WIDE)),
                vmem((TALL, LANES, WIDE)),
                vmem((2, 2, TALL, TALL, TALL, BLK, LANES)),
                vmem((2, TALL, 2, TALL, BLK, LANES)),
                vmem((cols, LANES, LANES)),
                vmem((WIDE, 2 * WIDE)),
                vmem((2 * TALL * BLK, BLK, LANES)),
                vmem((WIDE, LANES)),
                pltpu.SemaphoreType.DMA((3,)),
                pltpu.SemaphoreType.DMA((15,)),
                pltpu.SemaphoreType.DMA((45,)),
            ],
            compiler_params=pltpu.CompilerParams(collective_id=0, has_side_effects=True),
        )(local_l)

    return jax.shard_map(device_body, mesh=mesh, in_specs=(block_spec,), out_specs=block_spec, check_vma=False)
```
